128 devices in a mesh: shard: 16 (over x_hi, z, core), rep: 8 (over x_lo, y).
Axes of the slice: x: 4 (x_hi: 2, x_lo: 2; x = x_hi * 2 + x_lo), y: 4, z: 4, core: 2. Of those that a mesh axis runs over, the one named last changes fastest.
Arguments:
- tokens: bfloat16 [49152, 5120], P(('shard', 'rep')), may hold values from -700 to 700
- norm_gain: float32 [5120], replicated, may hold values from 0.1 to 1.9
- key_bias: float32 [1024], replicated, may hold values from -4 to 4
- key_weight: bfloat16 [8192, 1024], P('shard'), may hold values from -0.078125 to 0.078125
- cotangent: bfloat16 [49152, 1024], P(('shard', 'rep')), may hold values from -40 to 40
- block_slot: int32 [40], replicated, may hold values from 0 to 63, as said below
Outputs:
- projected: bfloat16 [49152, 1024], P(('shard', 'rep'))
- token_grad: bfloat16 [49152, 5120], P(('shard', 'rep'))
- weight_grad: float32 [8192, 1024], P('shard')
- gain_grad: float32 [5120], replicated
- bias_grad: float32 [1024], replicated
The draws below stay inside these ranges and needn't reach their ends.
Inputs may be any that keep to these rules, and one draw needn't show every extreme that they name: Entries are distinct; block b lies on the device of shard with index block_slot[b] // 4, at its local slot block_slot[b] % 4; in every draw some device holds 4 blocks.
All inputs are finite; a program needn't handle non-finite values.
Results may differ from the reference program's by a relative error of at most 0.013.
Values may be sent and summed in bfloat16 or wider, within the bound.
A program may use at most 128 MiB of HBM per device.

```python
import math
import jax
import jax.numpy as jnp
from jax import lax

D = 5120
KVW = 1024
BLK = 128
TOK_DEV = 384
NBLK = 40
CAP = 4
SLOTS = 64
ALL_TOK = 49152
N_SHARD = 16


def draw_tokens(key, part):
    keys = jax.random.split(key, 3)
    row_scale = jnp.exp(jax.random.uniform(keys[0], (ALL_TOK, 1), minval=0.0, maxval=math.log(10.0)))
    col_scale = jnp.exp(jax.random.uniform(keys[1], (1, D), minval=0.0, maxval=math.log(10.0)))
    base = jnp.clip(jax.random.normal(keys[2], (ALL_TOK, D)), -6.0, 6.0)
    return (base * row_scale * col_scale).astype(jnp.bfloat16)


def draw_cotangent(key, part):
    keys = jax.random.split(key, 1)
    position = jnp.arange(ALL_TOK, dtype=jnp.float32)[:, None] / max(ALL_TOK - 1, 1)
    rising = 1.0 + 2.0 * position
    values = jnp.clip(jax.random.normal(keys[0], (ALL_TOK, KVW)), -6.0, 6.0) * rising
    return values.astype(jnp.bfloat16)


def draw_block_slot(key, part):
    keys = jax.random.split(key, 3)
    full_owner = jax.random.randint(keys[0], (), 0, N_SHARD)
    slot_ids = jnp.arange(SLOTS, dtype=jnp.int32)
    order_slots = jax.random.permutation(keys[1], SLOTS).astype(jnp.int32)
    scores = jnp.where(slot_ids // CAP == full_owner, 0, 1 + order_slots)
    chosen = jnp.argsort(scores, stable=True)[:NBLK].astype(jnp.int32)
    block_order = jax.random.permutation(keys[2], NBLK).astype(jnp.int32)
    return chosen[block_order]


def level_of(key, shape, cuts, low, top_value):
    def one(axis_at, shards_of):
        draws = jax.random.uniform(jax.random.fold_in(jax.random.fold_in(key, 6), axis_at), (shards_of,), jnp.float32, low / len(cuts), top_value / len(cuts))
        return jnp.repeat(jnp.exp(draws), shape[axis_at] // shards_of).reshape((-1,) + (1,) * (len(shape) - axis_at - 1))

    factor_of = one(*cuts[0])
    for cut in cuts[1:]:
        factor_of = factor_of * one(*cut)
    return factor_of


def noise(own_key, dims, deviation, bound, pieces=(), held_as=jnp.bfloat16):
    loudness = level_of(own_key, dims, pieces, -0.22, 0.18) if pieces else 1.0
    drawn = jax.random.normal(own_key, dims, jnp.float32) * deviation * loudness
    return jnp.minimum(jnp.maximum(drawn, -bound), bound).astype(held_as)


def setup_inputs(seed: int = 0) -> dict:
    streams_of = jax.random.split(jax.random.key(seed), 7)
    tokens = draw_tokens(jax.random.fold_in(streams_of[6], 71), 0)
    norm_gain = jnp.clip(1.0 + 0.18 * jax.random.normal(streams_of[1], (D,), jnp.float32), 0.1, 1.9)
    key_bias = noise(streams_of[2], (KVW,), 1.0, 4.0, (), jnp.float32)
    key_weight = noise(streams_of[3], (SLOTS * BLK, KVW), D ** -0.5, 0.078125, ((0, 16),))
    cotangent = draw_cotangent(jax.random.fold_in(streams_of[6], 71), 0)
    block_slot = draw_block_slot(jax.random.fold_in(streams_of[6], 71), 0)
    return dict(tokens=tokens, norm_gain=norm_gain, key_bias=key_bias, key_weight=key_weight, cotangent=cotangent, block_slot=block_slot)


EPS = 1e-06

def normalize(tokens, norm_gain):
    values = tokens.astype(jnp.float32)
    inv_rms = lax.rsqrt(lax.optimization_barrier(jnp.mean(values * values, axis=-1, keepdims=True)) + EPS)
    normed = (values * inv_rms * norm_gain).astype(jnp.bfloat16)
    return (values, inv_rms, normed)

def token_backward(values, inv_rms, grad_normed, norm_gain):
    scaled = grad_normed * norm_gain
    inner = lax.optimization_barrier(jnp.mean(scaled * values, axis=-1, keepdims=True))
    return (inv_rms * (scaled - values * inv_rms * inv_rms * inner)).astype(jnp.bfloat16)

def reference(tokens, norm_gain, key_bias, key_weight, cotangent, block_slot):
    whole_weight = key_weight.reshape(SLOTS, BLK, KVW)[block_slot.astype(jnp.int32)].reshape(D, KVW)
    grad_scale = float(ALL_TOK) ** (-0.5)
    device_count = ALL_TOK // TOK_DEV

    def per_device(totals, blocks):
        tok_rows, cot_rows = blocks
        values, inv_rms, normed = normalize(tok_rows, norm_gain)
        forward = jnp.dot(normed, whole_weight, preferred_element_type=jnp.float32)
        projected = (forward + key_bias).astype(jnp.bfloat16)
        grad_normed = lax.dot_general(cot_rows, whole_weight, (((1,), (1,)), ((), ())), preferred_element_type=jnp.float32)
        token_grad = token_backward(values, inv_rms, grad_normed, norm_gain)
        partial_grad = lax.dot_general(normed, cot_rows, (((0,), (0,)), ((), ())), preferred_element_type=jnp.float32) * grad_scale
        rounded = lax.optimization_barrier(partial_grad.astype(jnp.bfloat16)).astype(jnp.float32)
        gain_term = lax.optimization_barrier(jnp.sum(grad_normed * values * inv_rms, axis=0)) * grad_scale
        bias_term = lax.optimization_barrier(jnp.sum(cot_rows.astype(jnp.float32), axis=0)) * grad_scale
        return ((totals[0] + rounded, totals[1] + gain_term, totals[2] + bias_term), (projected, token_grad))
    start = (jnp.zeros((D, KVW), jnp.float32), jnp.zeros((D,), jnp.float32), jnp.zeros((KVW,), jnp.float32))
    totals, outputs = lax.scan(per_device, start, (tokens.reshape(device_count, TOK_DEV, D), cotangent.reshape(device_count, TOK_DEV, KVW)))
    weight_sum, gain_grad, bias_grad = totals
    projected = outputs[0].reshape(ALL_TOK, KVW)
    token_grad = outputs[1].reshape(ALL_TOK, D)
    weight_grad = jnp.zeros((SLOTS, BLK, KVW), jnp.float32).at[block_slot.astype(jnp.int32)].set(weight_sum.reshape(NBLK, BLK, KVW)).reshape(SLOTS * BLK, KVW)
    return (projected, token_grad, weight_grad, gain_grad, bias_grad)
```

```python
import functools

import jax
import jax.numpy as jnp
from jax import lax
from jax.experimental import pallas as pl
from jax.experimental.pallas import tpu as pltpu
from jax.sharding import PartitionSpec as P

MESH = pl.DeviceIdType.MESH
BLK = 128
EPS = 1e-06
HALF = 20
PARTS = (
    (0, 7, 4, (0, 1, 2)),
    (7, 7, 3, (1, 2, 0)),
    (14, 6, 3, (2, 0, 1)),
)
BF = jnp.bfloat16
F32 = jnp.float32


class Place:
    def __init__(self):
        big = lax.axis_index("shard")
        rep = lax.axis_index("rep")
        self.big, self.rep = big, rep
        self.c = lax.rem(big, 2)
        self.s = lax.div(big, 2)
        self.z = lax.rem(self.s, 4)
        xh = lax.div(big, 8)
        xl = lax.div(rep, 4)
        self.xl = xl
        self.x = xh * 2 + xl
        self.y = lax.rem(rep, 4)
        self.pos = (self.x, self.y, self.z)

    def at(self, axis, step):
        return lax.rem(self.pos[axis] + step, 4)

    def device(self, pos, c):
        x, y, z = pos
        big = (lax.div(x, 2) * 4 + z) * 2 + c
        return (big, lax.rem(x, 2) * 4 + y)

    def ring(self, axis, step):
        pos = list(self.pos)
        pos[axis] = self.at(axis, step)
        return self.device(pos, self.c)

    def partner(self):
        return (self.s * 2 + 1 - self.c, self.rep)

    def x_pair(self):
        return (self.big, (1 - self.xl) * 4 + self.y)

    def group(self):
        for k in range(8):
            for d in range(2):
                if k == 0 and d == 0:
                    continue
                core = self.c if d == 0 else 1 - self.c
                yield k, d, (lax.rem(self.s + k, 8) * 2 + core, self.rep)


class Wires:
    def __init__(self, send, recv, limit):
        self.send, self.recv, self.limit, self.n, self.open = send, recv, limit, 0, []

    def put(self, src, dst, device):
        i = self.n
        self.n += 1
        assert i < self.limit, "sems"
        copy = pltpu.make_async_remote_copy(
            src_ref=src, dst_ref=dst, send_sem=self.send.at[i], recv_sem=self.recv.at[i],
            device_id=device, device_id_type=MESH,
        )
        copy.start()
        self.open.append(copy)
        return copy

    def drain(self):
        for copy in self.open:
            copy.wait_send()
        self.open = []


def greet(place):
    barrier = pltpu.get_barrier_semaphore()
    peers = [device for _, _, device in place.group()]
    for axis in (0, 1):
        peers += [place.ring(axis, 1), place.ring(axis, 3)]
    peers.append(place.ring(1, 2))
    for device in peers:
        pl.semaphore_signal(barrier, inc=1, device_id=device, device_id_type=MESH)
    pl.semaphore_wait(barrier, len(peers))


def locate(place, order, k, v, done, later):
    out = [None] * 3
    for j, axis in enumerate(order):
        out[axis] = v if j == k else (done(axis) if j < k else later(axis))
    return tuple(out)


class Gather:
    def __init__(self, place, wires, w):
        self.place, self.wires, self.w = place, wires, w
        self.base = place.c * HALF
        self.stage = {}
        self.pair = []

    def view(self, p, k, v, first, count):
        off, nb, h, order = PARTS[p]
        pos = self.place.pos
        idx = locate(self.place, order, k, v, lambda a: slice(None), lambda a: pos[a])
        return self.w.at[idx + (pl.ds(self.base + off + first, count),)]

    def move(self, p, k, v, first, count, device):
        ref = self.view(p, k, v, first, count)
        return self.wires.put(ref, ref, device)

    def start(self, p, k):
        off, nb, h, order = PARTS[p]
        place, axis = self.place, order[k]
        me = place.pos[axis]
        up, down = place.ring(axis, 1), place.ring(axis, 3)
        u0 = self.move(p, k, me, 0, h, up)
        d1 = self.move(p, k, me, h, nb - h, down)
        u1 = self.move(p, k, me, h, nb - h, up)
        d0 = self.move(p, k, me, 0, h, down)
        self.stage[p, k] = [u0, d1, u1, d0]

    def share(self, p, k, v, first, count):
        if k == 2:
            self.pair.append(self.move(p, k, v, first, count, self.place.partner()))

    def forward(self, p, k):
        off, nb, h, order = PARTS[p]
        place, axis = self.place, order[k]
        u0, d1, u1, d0 = self.stage[p, k]
        below, above = place.at(axis, 3), place.at(axis, 1)
        u0.wait_recv()
        f0 = self.move(p, k, below, 0, h, place.ring(axis, 1))
        self.share(p, k, below, 0, h)
        d1.wait_recv()
        f1 = self.move(p, k, above, h, nb - h, place.ring(axis, 3))
        self.share(p, k, above, h, nb - h)
        self.stage[p, k] += [f0, f1]

    def finish(self, p, k):
        off, nb, h, order = PARTS[p]
        place, axis = self.place, order[k]
        u0, d1, u1, d0, f0, f1 = self.stage[p, k]
        below, above, across = place.at(axis, 3), place.at(axis, 1), place.at(axis, 2)
        u1.wait_recv()
        self.share(p, k, below, h, nb - h)
        d0.wait_recv()
        self.share(p, k, above, 0, h)
        f0.wait_recv()
        self.share(p, k, across, 0, h)
        f1.wait_recv()
        self.share(p, k, across, h, nb - h)
        if k == 1:
            self.share(p, 2, place.pos[order[2]], 0, nb)


def rest_of(t, count):
    if count == 2:
        return (lax.div(t, 4), lax.rem(t, 4))
    return (t,) if count == 1 else ()


class Scatter:
    def __init__(self, place, wires, g, bufs):
        self.place, self.wires, self.g, self.bufs = place, wires, g, bufs
        self.base = place.c * HALF
        self.stage = {}

    def index(self, p, k, v, later):
        order = PARTS[p][3]
        pos = self.place.pos
        return locate(self.place, order, k, v, lambda a: pos[a], later)

    def view(self, p, k, v, first, count):
        idx = self.index(p, k, v, lambda a: slice(None))
        return self.g.at[idx + (pl.ds(self.base + PARTS[p][0] + first, count),)]

    def tile(self, p, k, v, rest, first, count):
        order = PARTS[p][3]
        later = sorted(order[k + 1:])
        idx = self.index(p, k, v, lambda a: rest[later.index(a)])
        return idx + (pl.ds(self.base + PARTS[p][0] + first, count),)

    def buf(self, p, k, which):
        return self.bufs[p][k][which]

    def start(self, p, k):
        off, nb, h, order = PARTS[p]
        place, axis = self.place, order[k]
        put, full = self.wires.put, (slice(None),) * (2 - k)
        up, down = place.ring(axis, 1), place.ring(axis, 3)
        over, under = place.at(axis, 1), place.at(axis, 3)
        across = place.at(axis, 2)
        ta, tb, fm, fp = self.bufs[p][k]
        a = put(self.view(p, k, across, 0, h), ta, up)
        b = put(self.view(p, k, across, h, nb - h), tb, down)
        u = put(self.view(p, k, over, h, nb - h), fm.at[full + (pl.ds(h, nb - h),)], up)
        d = put(self.view(p, k, under, 0, h), fp.at[full + (pl.ds(0, h),)], down)
        self.stage[p, k] = [a, b, u, d]

    def forward(self, p, k):
        off, nb, h, order = PARTS[p]
        place, axis = self.place, order[k]
        put, full = self.wires.put, (slice(None),) * (2 - k)
        up, down = place.ring(axis, 1), place.ring(axis, 3)
        over, under = place.at(axis, 1), place.at(axis, 3)
        ta, tb, fm, fp = self.bufs[p][k]
        a, b, u, d = self.stage[p, k]
        g = self.g

        def add(t, v, buf, first, count):
            rest = rest_of(t, 2 - k)
            idx = self.tile(p, k, v, rest, first, count)
            g[idx] = g[idx] + buf[rest]

        a.wait_recv()
        pl.loop(0, 4 ** (2 - k))(lambda t: add(t, over, ta, 0, h))
        fa = put(self.view(p, k, over, 0, h), fm.at[full + (pl.ds(0, h),)], up)
        b.wait_recv()
        pl.loop(0, 4 ** (2 - k))(lambda t: add(t, under, tb, h, nb - h))
        fb = put(self.view(p, k, under, h, nb - h), fp.at[full + (pl.ds(h, nb - h),)], down)
        self.stage[p, k] += [fa, fb]

    def finish(self, p, k):
        off, nb, h, order = PARTS[p]
        me = self.place.pos[order[k]]
        ta, tb, fm, fp = self.bufs[p][k]
        a, b, u, d, fa, fb = self.stage[p, k]
        g = self.g
        for copy in (u, d, fa, fb):
            copy.wait_recv()

        def add(t):
            rest = rest_of(t, 2 - k)
            idx = self.tile(p, k, me, rest, 0, nb)
            total = g[idx].astype(F32) + fm[rest].astype(F32) + fp[rest].astype(F32)
            g[idx] = total.astype(BF)

        pl.loop(0, 4 ** (2 - k))(add)


def scatter_scratch():
    out = []
    for p in range(3):
        _, nb, h, _ = PARTS[p]
        for k in range(3):
            lead = (4,) * (2 - k)
            out += [pltpu.VMEM(lead + (n, 16, 128), BF) for n in (h, nb - h, nb, nb)]
    return out


def scatter_bufs(flat):
    return [[flat[(p * 3 + k) * 4:(p * 3 + k) * 4 + 4] for k in range(3)] for p in range(3)]


class Small:
    def __init__(self, place, wires, first, rest):
        self.place, self.wires, self.first, self.rest = place, wires, first, rest
        self.sent = []

    def start(self, k, value):
        place = self.place
        if k == 0:
            self.first[place.c] = value
            own = self.first.at[place.c]
            self.sent = [self.wires.put(own, own, place.partner())]
            return
        axis = k - 1
        self.rest[axis, place.pos[axis]] = value
        own = self.rest.at[axis, place.pos[axis]]
        self.sent = [self.wires.put(own, own, place.ring(axis, step)) for step in (1, 3, 2)]

    def finish(self, k):
        for copy in self.sent:
            copy.wait_recv()
        if k == 0:
            return self.first[0] + self.first[1]
        t = self.rest
        return (t[k - 1, 0] + t[k - 1, 1]) + (t[k - 1, 2] + t[k - 1, 3])


def gather_kernel(slots_ref, kw_ref, out_ref, w, kws, held, send, recv, local):
    place = Place()
    wires = Wires(send, recv, 100)
    loads = []
    for t in range(8):
        load = pltpu.make_async_copy(kw_ref.at[:, place.rep, :, pl.ds(t * 128, 128)], kws.at[t], local.at[t])
        load.start()
        loads.append(load)
    greet(place)
    for load in loads:
        load.wait()
    mine = held.at[pl.ds(place.big * 4, 4)]
    come = [wires.put(kws.at[lax.rem(place.s + k, 8)], mine, device) for k, _, device in place.group()]
    held[pl.ds(place.big * 4, 4)] = kws[place.s]
    for copy in come:
        copy.wait_recv()

    @pl.loop(0, HALF)
    def _(t):
        b = place.c * HALF + t
        w[place.x, place.y, place.z, b] = held[slots_ref[b]]

    gather = Gather(place, wires, w)
    for p in range(3):
        gather.start(p, 0)
    for k in range(3):
        for p in range(3):
            gather.forward(p, k)
        for p in range(3):
            gather.finish(p, k)
            if k < 2:
                gather.start(p, k + 1)
    for copy in gather.pair:
        copy.wait_recv()
    stores = []
    for i in range(64):
        x, y, z = i // 16, i // 4 % 4, i % 4
        store = pltpu.make_async_copy(
            w.at[x, y, z],
            out_ref.at[:, (x % 2) * 4 + y, :, pl.ds((x // 2 * 4 + z) * 128, 128)],
            local.at[i],
        )
        store.start()
        stores.append(store)
    for store in stores:
        store.wait()
    wires.drain()


def scatter_kernel(owner_ref, part_ref, small_ref, out_ref, total_ref, g, half, slot, seen, fin,
                   first, rest, send, recv, local, *flat):
    place = Place()
    wires = Wires(send, recv, 130)
    loads = []
    for i in range(64):
        x, y, z = i // 16, i // 4 % 4, i % 4
        load = pltpu.make_async_copy(
            part_ref.at[:, (x % 2) * 4 + y, :, pl.ds((x // 2 * 4 + z) * 128, 128)],
            g.at[x, y, z],
            local.at[i],
        )
        load.start()
        loads.append(load)
    greet(place)
    for load in loads:
        load.wait()
    small = Small(place, wires, first, rest)
    small.start(0, small_ref[...])
    other = (1 - place.c) * HALF
    full = (slice(None),) * 3
    swap = []
    for off, nb, _, _ in PARTS:
        swap.append(wires.put(
            g.at[full + (pl.ds(other + off, nb),)], half.at[full + (pl.ds(off, nb),)], place.partner()))
    scatter = Scatter(place, wires, g, scatter_bufs(flat))
    mine = place.c * HALF
    for p, (off, nb, _, _) in enumerate(PARTS):
        swap[p].wait_recv()

        @pl.loop(0, 64)
        def _(t):
            i = (lax.div(t, 16), lax.rem(lax.div(t, 4), 4), lax.rem(t, 4))
            own = i + (pl.ds(mine + off, nb),)
            g[own] = g[own] + half[i + (pl.ds(off, nb),)]

        scatter.start(p, 0)
    for k in range(3):
        small.start(k + 1, small.finish(k))
        for p in range(3):
            scatter.forward(p, k)
        for p in range(3):
            scatter.finish(p, k)
            if k < 2:
                scatter.start(p, k + 1)
    total_ref[...] = small.finish(3)

    @pl.loop(0, 64)
    def _(t):
        b = owner_ref[t]
        ours = jnp.logical_and(b >= mine, b < mine + HALF)
        value = g[place.x, place.y, place.z, jnp.maximum(b, 0)]
        slot[t] = jnp.where(ours, value, jnp.zeros_like(value))

    come = []
    for _, _, device in place.group():
        come.append(wires.put(slot.at[pl.ds(device[0] * 4, 4)], seen.at[place.c, place.s], device))
    seen[place.c, place.s] = slot[pl.ds(place.big * 4, 4)]
    for copy in come:
        copy.wait_recv()
    for t in range(8):
        fin[place.xl, place.y, :, t] = seen[0, t] + seen[1, t]
    lo, hi = pl.ds(0, 2), pl.ds(2, 2)
    yup, ydown = place.ring(1, 1), place.ring(1, 3)
    below, above = place.at(1, 3), place.at(1, 1)

    def move(x, y, part, device):
        ref = fin.at[x, y, part]
        return wires.put(ref, ref, device)

    xl, y = place.xl, place.y
    every = slice(None)
    px = move(xl, y, lo, place.x_pair())
    hu = move(xl, y, hi, yup)
    hd = move(xl, y, hi, ydown)
    px.wait_recv()
    lu = [move(every, y, pl.ds(i, 1), yup) for i in (0, 1)]
    ld = [move(every, y, pl.ds(i, 1), ydown) for i in (1, 0)]
    hu.wait_recv()
    hfu = move(xl, below, pl.ds(2, 1), yup)
    hd.wait_recv()
    hfd = move(xl, above, pl.ds(3, 1), ydown)
    hfu.wait_recv()
    hfd.wait_recv()
    qx = move(xl, every, hi, place.x_pair())
    lu[0].wait_recv()
    lfu = move(every, below, pl.ds(0, 1), yup)
    ld[0].wait_recv()
    lfd = move(every, above, pl.ds(1, 1), ydown)
    for copy in (lu[1], ld[1], lfu, lfd, qx):
        copy.wait_recv()

    @pl.loop(0, 32)
    def _(t):
        i, r = lax.div(t, 8), lax.rem(t, 8)
        for j in range(8):
            out_ref[i, r, :, j * 128:(j + 1) * 128] = fin[lax.div(r, 4), lax.rem(r, 4), i, j].astype(F32)

    wires.drain()


VM = pl.BlockSpec(memory_space=pltpu.VMEM)
SM = pl.BlockSpec(memory_space=pltpu.SMEM)
ANY = pl.BlockSpec(memory_space=pl.ANY)
LIMIT = 64 * 1024 * 1024 - 65536


def gather_weights(block_slot, key_weight):
    return pl.pallas_call(
        gather_kernel,
        out_shape=jax.ShapeDtypeStruct((40, 8, 16, 1024), BF),
        in_specs=[SM, ANY],
        out_specs=ANY,
        scratch_shapes=[
            pltpu.VMEM((4, 4, 4, 40, 16, 128), BF),
            pltpu.VMEM((8, 4, 16, 128), BF),
            pltpu.VMEM((64, 16, 128), BF),
            pltpu.SemaphoreType.DMA((100,)),
            pltpu.SemaphoreType.DMA((100,)),
            pltpu.SemaphoreType.DMA((64,)),
        ],
        compiler_params=pltpu.CompilerParams(collective_id=0, has_side_effects=True, vmem_limit_bytes=LIMIT),
        name="gather",
    )(block_slot, key_weight.reshape(4, 8, 16, 1024))


def scatter_grads(owner, part, small):
    return pl.pallas_call(
        scatter_kernel,
        out_shape=(
            jax.ShapeDtypeStruct((4, 8, 16, 1024), F32),
            jax.ShapeDtypeStruct((48, 128), F32),
        ),
        in_specs=[SM, ANY, VM],
        out_specs=(VM, VM),
        scratch_shapes=[
            pltpu.VMEM((4, 4, 4, 40, 16, 128), BF),
            pltpu.VMEM((4, 4, 4, 20, 16, 128), BF),
            pltpu.VMEM((64, 16, 128), BF),
            pltpu.VMEM((2, 8, 4, 16, 128), BF),
            pltpu.VMEM((2, 4, 4, 8, 16, 128), BF),
            pltpu.VMEM((2, 48, 128), F32),
            pltpu.VMEM((3, 4, 48, 128), F32),
            pltpu.SemaphoreType.DMA((130,)),
            pltpu.SemaphoreType.DMA((130,)),
            pltpu.SemaphoreType.DMA((64,)),
        ] + scatter_scratch(),
        compiler_params=pltpu.CompilerParams(collective_id=1, has_side_effects=True, vmem_limit_bytes=LIMIT),
        name="scatter",
    )(owner, part.reshape(40, 8, 16, 1024), small)


def local(tokens, norm_gain, key_bias, key_weight, cotangent, block_slot):
    row_count, width = tokens.shape
    grad_scale = float(row_count * lax.axis_size("shard") * lax.axis_size("rep")) ** (-0.5)
    slots = jnp.arange(64, dtype=jnp.int32)
    hit = block_slot[None, :] == slots[:, None]
    owner = jnp.max(jnp.where(hit, jnp.arange(40, dtype=jnp.int32)[None, :], -1), axis=1)
    weight = gather_weights(block_slot, key_weight).reshape(width, 1024)
    values = tokens.astype(F32)
    inv_rms = lax.rsqrt(jnp.mean(values * values, axis=-1, keepdims=True) + EPS)
    normed = (values * inv_rms * norm_gain).astype(BF)
    forward = jnp.dot(normed, weight, preferred_element_type=F32)
    projected = (forward + key_bias).astype(BF)
    grad_normed = lax.dot_general(cotangent, weight, (((1,), (1,)), ((), ())), preferred_element_type=F32)
    scaled = grad_normed * norm_gain
    inner = jnp.mean(scaled * values, axis=-1, keepdims=True)
    token_grad = (inv_rms * (scaled - values * inv_rms * inv_rms * inner)).astype(BF)
    part = (
        lax.dot_general(normed, cotangent, (((0,), (0,)), ((), ())), preferred_element_type=F32) * grad_scale
    ).astype(BF)
    gain_part = jnp.sum(grad_normed * values * inv_rms, axis=0) * grad_scale
    bias_part = jnp.sum(cotangent.astype(F32), axis=0) * grad_scale
    small = jnp.concatenate([gain_part, bias_part]).reshape(48, 128)
    sums, total = scatter_grads(owner, part, small)
    total = total.reshape(-1)
    return (projected, token_grad, sums.reshape(512, 1024), total[:width], total[width:])


def solution(mesh):
    return jax.shard_map(
        local,
        mesh=mesh,
        in_specs=(
            P(("shard", "rep"), None),
            P(),
            P(),
            P("shard", None),
            P(("shard", "rep"), None),
            P(),
        ),
        out_specs=(
            P(("shard", "rep"), None),
            P(("shard", "rep"), None),
            P("shard", None),
            P(),
            P(),
        ),
        check_vma=False,
    )
```

```python
import functools

import jax
import jax.numpy as jnp
from jax import lax
from jax.experimental import pallas as pl
from jax.experimental.pallas import tpu as pltpu
from jax.sharding import PartitionSpec as P

MESH = pl.DeviceIdType.MESH
BLK = 128
EPS = 1e-06
HALF = 20
PARTS = (
    (0, 7, 4, (0, 1, 2)),
    (7, 7, 3, (1, 2, 0)),
    (14, 6, 3, (2, 0, 1)),
)
BF = jnp.bfloat16
F32 = jnp.float32


class Place:
    def __init__(self):
        big = lax.axis_index("shard")
        rep = lax.axis_index("rep")
        self.big, self.rep = big, rep
        self.c = lax.rem(big, 2)
        self.s = lax.div(big, 2)
        self.z = lax.rem(self.s, 4)
        xh = lax.div(big, 8)
        xl = lax.div(rep, 4)
        self.xl = xl
        self.x = xh * 2 + xl
        self.y = lax.rem(rep, 4)
        self.pos = (self.x, self.y, self.z)

    def at(self, axis, step):
        return lax.rem(self.pos[axis] + step, 4)

    def device(self, pos, c):
        x, y, z = pos
        big = (lax.div(x, 2) * 4 + z) * 2 + c
        return (big, lax.rem(x, 2) * 4 + y)

    def ring(self, axis, step):
        pos = list(self.pos)
        pos[axis] = self.at(axis, step)
        return self.device(pos, self.c)

    def partner(self):
        return (self.s * 2 + 1 - self.c, self.rep)

    def x_pair(self):
        return (self.big, (1 - self.xl) * 4 + self.y)

    def group(self):
        for k in range(8):
            for d in range(2):
                if k == 0 and d == 0:
                    continue
                core = self.c if d == 0 else 1 - self.c
                yield k, d, (lax.rem(self.s + k, 8) * 2 + core, self.rep)


class Wires:
    def __init__(self, send, recv, limit):
        self.send, self.recv, self.limit, self.n, self.open = send, recv, limit, 0, []

    def put(self, src, dst, device):
        i = self.n
        self.n += 1
        assert i < self.limit, "sems"
        copy = pltpu.make_async_remote_copy(
            src_ref=src, dst_ref=dst, send_sem=self.send.at[i], recv_sem=self.recv.at[i],
            device_id=device, device_id_type=MESH,
        )
        copy.start()
        self.open.append(copy)
        return copy

    def drain(self):
        for copy in self.open:
            copy.wait_send()
        self.open = []


def greet(place):
    barrier = pltpu.get_barrier_semaphore()
    peers = [device for _, _, device in place.group()]
    for axis in (0, 1):
        peers += [place.ring(axis, 1), place.ring(axis, 3)]
    peers.append(place.ring(1, 2))
    for device in peers:
        pl.semaphore_signal(barrier, inc=1, device_id=device, device_id_type=MESH)
    pl.semaphore_wait(barrier, len(peers))


def locate(place, order, k, v, done, later):
    out = [None] * 3
    for j, axis in enumerate(order):
        out[axis] = v if j == k else (done(axis) if j < k else later(axis))
    return tuple(out)


class Gather:
    def __init__(self, place, wires, w):
        self.place, self.wires, self.w = place, wires, w
        self.base = place.c * HALF
        self.stage = {}
        self.pair = []

    def view(self, p, k, v, first, count):
        off, nb, h, order = PARTS[p]
        pos = self.place.pos
        idx = locate(self.place, order, k, v, lambda a: slice(None), lambda a: pos[a])
        return self.w.at[idx + (pl.ds(self.base + off + first, count),)]

    def move(self, p, k, v, first, count, device):
        ref = self.view(p, k, v, first, count)
        return self.wires.put(ref, ref, device)

    def start(self, p, k):
        off, nb, h, order = PARTS[p]
        place, axis = self.place, order[k]
        me = place.pos[axis]
        up, down = place.ring(axis, 1), place.ring(axis, 3)
        u0 = self.move(p, k, me, 0, h, up)
        d1 = self.move(p, k, me, h, nb - h, down)
        u1 = self.move(p, k, me, h, nb - h, up)
        d0 = self.move(p, k, me, 0, h, down)
        self.stage[p, k] = [u0, d1, u1, d0]

    def share(self, p, k, v, first, count):
        if k == 2:
            self.pair.append(self.move(p, k, v, first, count, self.place.partner()))

    def forward(self, p, k):
        off, nb, h, order = PARTS[p]
        place, axis = self.place, order[k]
        u0, d1, u1, d0 = self.stage[p, k]
        below, above = place.at(axis, 3), place.at(axis, 1)
        u0.wait_recv()
        f0 = self.move(p, k, below, 0, h, place.ring(axis, 1))
        self.share(p, k, below, 0, h)
        d1.wait_recv()
        f1 = self.move(p, k, above, h, nb - h, place.ring(axis, 3))
        self.share(p, k, above, h, nb - h)
        self.stage[p, k] += [f0, f1]

    def finish(self, p, k):
        off, nb, h, order = PARTS[p]
        place, axis = self.place, order[k]
        u0, d1, u1, d0, f0, f1 = self.stage[p, k]
        below, above, across = place.at(axis, 3), place.at(axis, 1), place.at(axis, 2)
        u1.wait_recv()
        self.share(p, k, below, h, nb - h)
        d0.wait_recv()
        self.share(p, k, above, 0, h)
        f0.wait_recv()
        self.share(p, k, across, 0, h)
        f1.wait_recv()
        self.share(p, k, across, h, nb - h)
        if k == 1:
            self.share(p, 2, place.pos[order[2]], 0, nb)


def rest_of(t, count):
    if count == 2:
        return (lax.div(t, 4), lax.rem(t, 4))
    return (t,) if count == 1 else ()


class Scatter:
    def __init__(self, place, wires, g, bufs):
        self.place, self.wires, self.g, self.bufs = place, wires, g, bufs
        self.base = place.c * HALF
        self.stage = {}

    def index(self, p, k, v, later):
        order = PARTS[p][3]
        pos = self.place.pos
        return locate(self.place, order, k, v, lambda a: pos[a], later)

    def view(self, p, k, v, first, count):
        idx = self.index(p, k, v, lambda a: slice(None))
        return self.g.at[idx + (pl.ds(self.base + PARTS[p][0] + first, count),)]

    def tile(self, p, k, v, rest, first, count):
        order = PARTS[p][3]
        later = sorted(order[k + 1:])
        idx = self.index(p, k, v, lambda a: rest[later.index(a)])
        return idx + (pl.ds(self.base + PARTS[p][0] + first, count),)

    def buf(self, p, k, which):
        return self.bufs[p][k][which]

    def start(self, p, k):
        off, nb, h, order = PARTS[p]
        place, axis = self.place, order[k]
        put, full = self.wires.put, (slice(None),) * (2 - k)
        up, down = place.ring(axis, 1), place.ring(axis, 3)
        over, under = place.at(axis, 1), place.at(axis, 3)
        across = place.at(axis, 2)
        ta, tb, fm, fp = self.bufs[p][k]
        a = put(self.view(p, k, across, 0, h), ta, up)
        b = put(self.view(p, k, across, h, nb - h), tb, down)
        u = put(self.view(p, k, over, h, nb - h), fm.at[full + (pl.ds(h, nb - h),)], up)
        d = put(self.view(p, k, under, 0, h), fp.at[full + (pl.ds(0, h),)], down)
        self.stage[p, k] = [a, b, u, d]

    def forward(self, p, k):
        off, nb, h, order = PARTS[p]
        place, axis = self.place, order[k]
        put, full = self.wires.put, (slice(None),) * (2 - k)
        up, down = place.ring(axis, 1), place.ring(axis, 3)
        over, under = place.at(axis, 1), place.at(axis, 3)
        ta, tb, fm, fp = self.bufs[p][k]
        a, b, u, d = self.stage[p, k]
        g = self.g

        def add(t, v, buf, first, count):
            rest = rest_of(t, 2 - k)
            idx = self.tile(p, k, v, rest, first, count)
            g[idx] = g[idx] + buf[rest]

        a.wait_recv()
        pl.loop(0, 4 ** (2 - k))(lambda t: add(t, over, ta, 0, h))
        fa = put(self.view(p, k, over, 0, h), fm.at[full + (pl.ds(0, h),)], up)
        b.wait_recv()
        pl.loop(0, 4 ** (2 - k))(lambda t: add(t, under, tb, h, nb - h))
        fb = put(self.view(p, k, under, h, nb - h), fp.at[full + (pl.ds(h, nb - h),)], down)
        self.stage[p, k] += [fa, fb]

    def finish(self, p, k):
        off, nb, h, order = PARTS[p]
        me = self.place.pos[order[k]]
        ta, tb, fm, fp = self.bufs[p][k]
        a, b, u, d, fa, fb = self.stage[p, k]
        g = self.g
        for copy in (u, d, fa, fb):
            copy.wait_recv()

        def add(t):
            rest = rest_of(t, 2 - k)
            idx = self.tile(p, k, me, rest, 0, nb)
            total = g[idx].astype(F32) + fm[rest].astype(F32) + fp[rest].astype(F32)
            g[idx] = total.astype(BF)

        pl.loop(0, 4 ** (2 - k))(add)


def scatter_scratch():
    out = []
    for p in range(3):
        _, nb, h, _ = PARTS[p]
        for k in range(3):
            lead = (4,) * (2 - k)
            out += [pltpu.VMEM(lead + (n, 16, 128), BF) for n in (h, nb - h, nb, nb)]
    return out


def scatter_bufs(flat):
    return [[flat[(p * 3 + k) * 4:(p * 3 + k) * 4 + 4] for k in range(3)] for p in range(3)]


class Small:
    def __init__(self, place, wires, first, rest):
        self.place, self.wires, self.first, self.rest = place, wires, first, rest
        self.sent = []

    def start(self, k, value):
        place = self.place
        if k == 0:
            self.first[place.c] = value
            own = self.first.at[place.c]
            self.sent = [self.wires.put(own, own, place.partner())]
            return
        axis = k - 1
        self.rest[axis, place.pos[axis]] = value
        own = self.rest.at[axis, place.pos[axis]]
        self.sent = [self.wires.put(own, own, place.ring(axis, step)) for step in (1, 3, 2)]

    def finish(self, k):
        for copy in self.sent:
            copy.wait_recv()
        if k == 0:
            return self.first[0] + self.first[1]
        t = self.rest
        return (t[k - 1, 0] + t[k - 1, 1]) + (t[k - 1, 2] + t[k - 1, 3])


WIDTH = 5120
KEYS = 1024
ROWS = 384


def fused_kernel(slots_ref, owner_ref, tok_ref, gain_ref, bias_ref, kw_ref, cot_ref,
                 proj_out, grad_out, slab_out, total_ref,
                 w, kws, held, g, half, slot, seen, fin, first, rest,
                 tok, normed, cot, proj, inv, coef, small_v, send, recv, local, *flat):
    place = Place()
    wires = Wires(send, recv, 200)
    grad_scale = float(ROWS * 128) ** (-0.5)
    loads = []

    def load(src, dst):
        copy = pltpu.make_async_copy(src, dst, local.at[len(loads)])
        copy.start()
        loads.append(copy)
        return copy

    slabs = [load(kw_ref.at[:, place.rep, :, pl.ds(t * 128, 128)], kws.at[t]) for t in range(8)]
    rows = [load(tok_ref.at[pl.ds(i * 64, 64)], tok.at[pl.ds(i * 64, 64)]) for i in range(6)]
    cots = load(cot_ref, cot)
    greet(place)
    for copy in slabs:
        copy.wait()
    mine = held.at[pl.ds(place.big * 4, 4)]
    come = [wires.put(kws.at[lax.rem(place.s + k, 8)], mine, device) for k, _, device in place.group()]
    held[pl.ds(place.big * 4, 4)] = kws[place.s]

    def norm(i):
        rows[i].wait()

        @pl.loop(i * 4, i * 4 + 4)
        def _(t):
            r = pl.ds(pl.multiple_of(t * 16, 16), 16)
            acc = [jnp.zeros((16, 128), F32)] * 4
            for j in range(40):
                v = tok[r, j * 128:(j + 1) * 128].astype(F32)
                acc[j % 4] = acc[j % 4] + v * v
            total = jnp.sum((acc[0] + acc[1]) + (acc[2] + acc[3]), axis=1, keepdims=True)
            scale = jnp.broadcast_to(lax.rsqrt(total * (1.0 / WIDTH) + EPS), (16, 128))
            inv[r, :] = scale
            for j in range(40):
                col = slice(j * 128, (j + 1) * 128)
                normed[r, col] = (tok[r, col].astype(F32) * scale * gain_ref[:, col]).astype(BF)

    gather = Gather(place, wires, w)
    for i in range(2):
        norm(i)
    for copy in come:
        copy.wait_recv()

    @pl.loop(0, HALF)
    def _(t):
        b = place.c * HALF + t
        w[place.x, place.y, place.z, b] = held[slots_ref[b]]

    for p in range(3):
        gather.start(p, 0)
    for i in range(2, 6):
        norm(i)
    for p in range(3):
        gather.forward(p, 0)
    cots.wait()
    for j in range(8):
        small_v[40 + j:41 + j, :] = jnp.sum(
            cot[:, j * 128:(j + 1) * 128].astype(F32), axis=0, keepdims=True) * grad_scale

    def partial(side, low, high):
        @pl.loop(low, high)
        def _(t):
            b = side * HALF + 2 * t
            left = normed[:, pl.ds(pl.multiple_of(b * 128, 128), 256)]
            value = lax.dot_general(left, cot[...], (((0,), (0,)), ((), ())), preferred_element_type=F32)
            value = (value * grad_scale).astype(BF)
            for i in range(2):
                for r in range(8):
                    for q in range(8):
                        g[q // 4 * 2 + r // 4, r % 4, q % 4, b + i] = value[
                            i * 128 + r * 16:i * 128 + r * 16 + 16, q * 128:(q + 1) * 128]

    pairs = ((0, 4), (4, 7), (7, 10))
    swap = []
    full = (slice(None),) * 3

    def exchange(p):
        off, nb = PARTS[p][:2]
        other = (1 - place.c) * HALF
        swap.append(wires.put(
            g.at[full + (pl.ds(other + off, nb),)], half.at[full + (pl.ds(off, nb),)], place.partner()))

    scatter = Scatter(place, wires, g, scatter_bufs(flat))
    own = place.c * HALF

    def merge(p):
        off, nb = PARTS[p][:2]
        swap[p].wait_recv()

        @pl.loop(0, 64)
        def _(t):
            i = (lax.div(t, 16), lax.rem(lax.div(t, 4), 4), lax.rem(t, 4))
            at = i + (pl.ds(own + off, nb),)
            g[at] = g[at] + half[i + (pl.ds(off, nb),)]

    partial(1 - place.c, *pairs[0])
    exchange(0)
    for p in range(3):
        gather.finish(p, 0)
        gather.start(p, 1)
    partial(1 - place.c, *pairs[1])
    exchange(1)
    for p in range(3):
        gather.forward(p, 1)
    partial(1 - place.c, *pairs[2])
    exchange(2)
    for p in range(3):
        gather.finish(p, 1)
        gather.start(p, 2)
    for p in range(3):
        partial(place.c, *pairs[p])
        merge(p)
        scatter.start(p, 0)
    for p in range(3):
        gather.forward(p, 2)
    for p in range(3):
        gather.finish(p, 2)
    for copy in gather.pair:
        copy.wait_recv()

    coef[...] = jnp.zeros_like(coef)

    @pl.loop(0, 4)
    def _(n):
        q = 2 * n
        x0, z0 = lax.div(q, 4) * 2, lax.rem(q, 4)
        right = jnp.concatenate(
            [jnp.concatenate([w[x0 + r // 4, r % 4, z0, b], w[x0 + r // 4, r % 4, z0 + 1, b]], axis=1)
             for b in range(40) for r in range(8)], axis=0)
        value = jnp.dot(normed[...], right, preferred_element_type=F32)
        col = pl.ds(pl.multiple_of(n * 256, 256), 256)
        proj[:, col] = (value + bias_ref[:, col]).astype(BF)
        both = value * cot[:, col].astype(F32)
        coef[...] += both[:, :128] + both[:, 128:]

    def store(src, dst):
        copy = load(src, dst)
        return copy

    stores = [store(proj, proj_out)]
    coef[...] = jnp.broadcast_to(
        jnp.sum(coef[...], axis=1, keepdims=True), (ROWS, 128)) * inv[...] * (1.0 / WIDTH)

    def backward(low, high):
        @pl.loop(low, high)
        def _(t):
            b = 2 * t
            right = jnp.concatenate(
                [jnp.concatenate([w[q // 4 * 2 + r // 4, r % 4, q % 4, b + i] for q in range(8)], axis=1)
                 for i in range(2) for r in range(8)], axis=0)
            grad = lax.dot_general(cot[...], right, (((1,), (1,)), ((), ())), preferred_element_type=F32)
            for i in range(2):
                col = pl.ds(pl.multiple_of((b + i) * 128, 128), 128)
                gn = grad[:, i * 128:(i + 1) * 128]
                scale = inv[...]
                unit = tok[:, col].astype(F32) * scale
                small_v[pl.ds(b + i, 1), :] = jnp.sum(gn * unit, axis=0, keepdims=True) * grad_scale
                tok[:, col] = (gn * gain_ref[:, col] * scale - unit * coef[...]).astype(BF)

        col = pl.ds(low * 256, (high - low) * 256)
        stores.append(store(tok.at[:, col], grad_out.at[:, col]))

    small = Small(place, wires, first, rest)
    for p in range(3):
        scatter.forward(p, 0)
    for i in range(4):
        backward(i * 5, i * 5 + 5)
    small.start(0, small_v[...])
    for k in range(3):
        if k:
            for p in range(3):
                scatter.forward(p, k)
        for p in range(3):
            scatter.finish(p, k)
            if k < 2:
                scatter.start(p, k + 1)
        small.start(k + 1, small.finish(k))

    @pl.loop(0, 64)
    def _(t):
        b = owner_ref[t]
        ours = jnp.logical_and(b >= own, b < own + HALF)
        value = g[place.x, place.y, place.z, jnp.maximum(b, 0)]
        slot[t] = jnp.where(ours, value, jnp.zeros_like(value))

    come = []
    for _, _, device in place.group():
        come.append(wires.put(slot.at[pl.ds(device[0] * 4, 4)], seen.at[place.c, place.s], device))
    seen[place.c, place.s] = slot[pl.ds(place.big * 4, 4)]
    total_ref[...] = small.finish(3)
    for copy in come:
        copy.wait_recv()
    for t in range(8):
        fin[place.xl, place.y, :, t] = seen[0, t] + seen[1, t]
    lo, hi = pl.ds(0, 2), pl.ds(2, 2)
    yup, ydown = place.ring(1, 1), place.ring(1, 3)
    below, above = place.at(1, 3), place.at(1, 1)

    def move(x, y, part, device):
        ref = fin.at[x, y, part]
        return wires.put(ref, ref, device)

    xl, y = place.xl, place.y
    every = slice(None)
    px = move(xl, y, lo, place.x_pair())
    hu = move(xl, y, hi, yup)
    hd = move(xl, y, hi, ydown)
    px.wait_recv()
    lu = [move(every, y, pl.ds(i, 1), yup) for i in (0, 1)]
    ld = [move(every, y, pl.ds(i, 1), ydown) for i in (1, 0)]
    hu.wait_recv()
    hfu = move(xl, below, pl.ds(2, 1), yup)
    hd.wait_recv()
    hfd = move(xl, above, pl.ds(3, 1), ydown)
    hfu.wait_recv()
    hfd.wait_recv()
    qx = move(xl, every, hi, place.x_pair())
    lu[0].wait_recv()
    lfu = move(every, below, pl.ds(0, 1), yup)
    ld[0].wait_recv()
    lfd = move(every, above, pl.ds(1, 1), ydown)
    for copy in (lu[1], ld[1], lfu, lfd, qx):
        copy.wait_recv()

    @pl.loop(0, 32)
    def _(t):
        i, r = lax.div(t, 8), lax.rem(t, 8)
        for j in range(8):
            slab_out[i, r, :, j * 128:(j + 1) * 128] = fin[lax.div(r, 4), lax.rem(r, 4), i, j]

    for copy in stores:
        copy.wait()
    wires.drain()


VM = pl.BlockSpec(memory_space=pltpu.VMEM)
SM = pl.BlockSpec(memory_space=pltpu.SMEM)
ANY = pl.BlockSpec(memory_space=pl.ANY)
LIMIT = 64 * 1024 * 1024 - 65536


def fused(block_slot, owner, tokens, gain, bias, key_weight, cotangent):
    return pl.pallas_call(
        fused_kernel,
        out_shape=(
            jax.ShapeDtypeStruct((ROWS, KEYS), BF),
            jax.ShapeDtypeStruct((ROWS, WIDTH), BF),
            jax.ShapeDtypeStruct((4, 8, 16, 1024), BF),
            jax.ShapeDtypeStruct((48, 128), F32),
        ),
        in_specs=[SM, SM, ANY, VM, VM, ANY, ANY],
        out_specs=(ANY, ANY, VM, VM),
        scratch_shapes=[
            pltpu.VMEM((4, 4, 4, 40, 16, 128), BF),
            pltpu.VMEM((8, 4, 16, 128), BF),
            pltpu.VMEM((64, 16, 128), BF),
            pltpu.VMEM((4, 4, 4, 40, 16, 128), BF),
            pltpu.VMEM((4, 4, 4, 20, 16, 128), BF),
            pltpu.VMEM((64, 16, 128), BF),
            pltpu.VMEM((2, 8, 4, 16, 128), BF),
            pltpu.VMEM((2, 4, 4, 8, 16, 128), BF),
            pltpu.VMEM((2, 48, 128), F32),
            pltpu.VMEM((3, 4, 48, 128), F32),
            pltpu.VMEM((ROWS, WIDTH), BF),
            pltpu.VMEM((ROWS, WIDTH), BF),
            pltpu.VMEM((ROWS, KEYS), BF),
            pltpu.VMEM((ROWS, KEYS), BF),
            pltpu.VMEM((ROWS, 128), F32),
            pltpu.VMEM((ROWS, 128), F32),
            pltpu.VMEM((48, 128), F32),
            pltpu.SemaphoreType.DMA((200,)),
            pltpu.SemaphoreType.DMA((200,)),
            pltpu.SemaphoreType.DMA((40,)),
        ] + scatter_scratch(),
        compiler_params=pltpu.CompilerParams(collective_id=0, has_side_effects=True, vmem_limit_bytes=LIMIT),
        name="fused",
    )(block_slot, owner, tokens, gain, bias, key_weight, cotangent)


def local(tokens, norm_gain, key_bias, key_weight, cotangent, block_slot):
    slots = jnp.arange(64, dtype=jnp.int32)
    hit = block_slot[None, :] == slots[:, None]
    owner = jnp.max(jnp.where(hit, jnp.arange(40, dtype=jnp.int32)[None, :], -1), axis=1)
    projected, token_grad, slab, total = fused(
        block_slot, owner, tokens, norm_gain.reshape(1, WIDTH), key_bias.reshape(1, KEYS),
        key_weight.reshape(4, 8, 16, KEYS), cotangent)
    total = total.reshape(-1)
    return (projected, token_grad, slab.reshape(512, KEYS).astype(F32), total[:WIDTH], total[WIDTH:])


def solution(mesh):
    return jax.shard_map(
        local,
        mesh=mesh,
        in_specs=(
            P(("shard", "rep"), None),
            P(),
            P(),
            P("shard", None),
            P(("shard", "rep"), None),
            P(),
        ),
        out_specs=(
            P(("shard", "rep"), None),
            P(("shard", "rep"), None),
            P("shard", None),
            P(),
            P(),
        ),
        check_vma=False,
    )
```

```python
import functools

import jax
import jax.numpy as jnp
from jax import lax
from jax.experimental import pallas as pl
from jax.experimental.pallas import tpu as pltpu
from jax.sharding import PartitionSpec as P

MESH = pl.DeviceIdType.MESH
BLK = 128
EPS = 1e-06
HALF = 20
PARTS = (
    (0, 7, 4, (0, 1, 2)),
    (7, 7, 3, (1, 2, 0)),
    (14, 6, 3, (2, 0, 1)),
)
BF = jnp.bfloat16
F32 = jnp.float32


class Place:
    def __init__(self):
        big = lax.axis_index("shard")
        rep = lax.axis_index("rep")
        self.big, self.rep = big, rep
        self.c = lax.rem(big, 2)
        self.s = lax.div(big, 2)
        self.z = lax.rem(self.s, 4)
        xh = lax.div(big, 8)
        xl = lax.div(rep, 4)
        self.xl = xl
        self.xh = xh
        self.pi = lax.rem(xl + xh, 2)
        self.x = xh * 2 + xl
        self.y = lax.rem(rep, 4)
        self.pos = (self.x, self.y, self.z)

    def at(self, axis, step):
        return lax.rem(self.pos[axis] + step, 4)

    def device(self, pos, c):
        x, y, z = pos
        big = (lax.div(x, 2) * 4 + z) * 2 + c
        return (big, lax.rem(x, 2) * 4 + y)

    def ring(self, axis, step):
        pos = list(self.pos)
        pos[axis] = self.at(axis, step)
        return self.device(pos, self.c)

    def partner(self):
        return (self.s * 2 + 1 - self.c, self.rep)

    def x_pair(self):
        return (self.big, (1 - self.xl) * 4 + self.y)

    def group(self):
        for i in range(2):
            for j in range(4):
                for d in range(2):
                    if i == j == d == 0:
                        continue
                    xh = self.xh if i == 0 else 1 - self.xh
                    xl = self.xl if i == 0 else 1 - self.xl
                    core = self.c if d == 0 else 1 - self.c
                    yield i, j, d, ((xh * 4 + self.at(2, j)) * 2 + core, xl * 4 + self.y)


class Wires:
    def __init__(self, send, recv, limit):
        self.send, self.recv, self.limit, self.n, self.open = send, recv, limit, 0, []

    def put(self, src, dst, device):
        i = self.n
        self.n += 1
        assert i < self.limit, "sems"
        copy = pltpu.make_async_remote_copy(
            src_ref=src, dst_ref=dst, send_sem=self.send.at[i], recv_sem=self.recv.at[i],
            device_id=device, device_id_type=MESH,
        )
        copy.start()
        self.open.append(copy)
        return copy

    def drain(self):
        for copy in self.open:
            copy.wait_send()
        self.open = []


def greet(place):
    barrier = pltpu.get_barrier_semaphore()
    peers = [device for _, _, _, device in place.group()]
    peers += [place.x_pair(), place.ring(0, 2)]
    peers += [place.ring(1, step) for step in (1, 2, 3)]
    for device in peers:
        pl.semaphore_signal(barrier, inc=1, device_id=device, device_id_type=MESH)
    return lambda: pl.semaphore_wait(barrier, len(peers))


def locate(place, order, k, v, done, later):
    out = [None] * 3
    for j, axis in enumerate(order):
        out[axis] = v if j == k else (done(axis) if j < k else later(axis))
    return tuple(out)


class Gather:
    def __init__(self, place, wires, w):
        self.place, self.wires, self.w = place, wires, w
        self.base = place.c * HALF
        self.stage = {}
        self.passed = {}
        self.pair = []

    def view(self, p, k, v, first, count):
        off, nb, h, order = PARTS[p]
        pos = self.place.pos
        idx = locate(self.place, order, k, v, lambda a: slice(None), lambda a: pos[a])
        return self.w.at[idx + (pl.ds(self.base + off + first, count),)]

    def move(self, p, k, v, first, count, device):
        ref = self.view(p, k, v, first, count)
        return self.wires.put(ref, ref, device)

    def start(self, p, k, part=None):
        off, nb, h, order = PARTS[p]
        place, axis = self.place, order[k]
        me = place.pos[axis]
        up, down = place.ring(axis, 1), place.ring(axis, 3)
        if k == 0:
            self.stage[p, k] = [
                self.move(p, k, me, 0, nb, device) for device in (place.ring(axis, 2), up, down)]
            return
        if part != 1:
            u0 = self.move(p, k, me, 0, h, up)
            d1 = self.move(p, k, me, h, nb - h, down)
            self.stage[p, k] = [u0, d1]
        if part != 0:
            u1 = self.move(p, k, me, h, nb - h, up)
            d0 = self.move(p, k, me, 0, h, down)
            self.stage[p, k] += [u1, d0]

    def share(self, p, k, v, first, count):
        if k == 2:
            self.pair.append(self.move(p, k, v, first, count, self.place.partner()))

    def forward(self, p, k):
        off, nb, h, order = PARTS[p]
        place, axis = self.place, order[k]
        u0, d1 = self.stage[p, k][:2]
        below, above = place.at(axis, 3), place.at(axis, 1)
        u0.wait_recv()
        f0 = self.move(p, k, below, 0, h, place.ring(axis, 1))
        d1.wait_recv()
        f1 = self.move(p, k, above, h, nb - h, place.ring(axis, 3))
        self.share(p, k, below, 0, h)
        self.share(p, k, above, h, nb - h)
        self.passed[p, k] = [f0, f1]

    def finish(self, p, k):
        off, nb, h, order = PARTS[p]
        place, axis = self.place, order[k]
        if k == 0:
            for copy in self.stage[p, k]:
                copy.wait_recv()
            return
        u0, d1, u1, d0 = self.stage[p, k]
        f0, f1 = self.passed[p, k]
        below, above, across = place.at(axis, 3), place.at(axis, 1), place.at(axis, 2)
        u1.wait_recv()
        self.share(p, k, below, h, nb - h)
        d0.wait_recv()
        self.share(p, k, above, 0, h)
        f0.wait_recv()
        self.share(p, k, across, 0, h)
        f1.wait_recv()
        self.share(p, k, across, h, nb - h)
        if k == 1:
            self.share(p, 2, place.pos[order[2]], 0, nb)


def rest_of(t, count):
    if count == 2:
        return (lax.div(t, 4), lax.rem(t, 4))
    return (t,) if count == 1 else ()


class Scatter:
    def __init__(self, place, wires, g, bufs):
        self.place, self.wires, self.g, self.bufs = place, wires, g, bufs
        self.base = place.c * HALF
        self.stage = {}
        self.passed = {}

    def index(self, p, k, v, later):
        order = PARTS[p][3]
        pos = self.place.pos
        return locate(self.place, order, k, v, lambda a: pos[a], later)

    def view(self, p, k, v, first, count):
        idx = self.index(p, k, v, lambda a: slice(None))
        return self.g.at[idx + (pl.ds(self.base + PARTS[p][0] + first, count),)]

    def tile(self, p, k, v, rest, first, count):
        order = PARTS[p][3]
        later = sorted(order[k + 1:])
        idx = self.index(p, k, v, lambda a: rest[later.index(a)])
        return idx + (pl.ds(self.base + PARTS[p][0] + first, count),)

    def buf(self, p, k, which):
        return self.bufs[p][k][which]

    def start(self, p, k, part=None):
        off, nb, h, order = PARTS[p]
        place, axis = self.place, order[k]
        put, full = self.wires.put, (slice(None),) * (2 - k)
        up, down = place.ring(axis, 1), place.ring(axis, 3)
        over, under = place.at(axis, 1), place.at(axis, 3)
        across = place.at(axis, 2)
        ta, tb, fm, fp = self.bufs[p][k]
        if k == 2:
            self.stage[p, k] = [
                put(self.view(p, k, across, 0, nb), ta, place.ring(axis, 2)),
                put(self.view(p, k, over, 0, nb), fm, up),
                put(self.view(p, k, under, 0, nb), fp, down)]
            return
        if part != 1:
            a = put(self.view(p, k, across, 0, h), ta, up)
            b = put(self.view(p, k, across, h, nb - h), tb, down)
            self.stage[p, k] = [a, b]
        if part != 0:
            u = put(self.view(p, k, over, h, nb - h), fm.at[full + (pl.ds(h, nb - h),)], up)
            d = put(self.view(p, k, under, 0, h), fp.at[full + (pl.ds(0, h),)], down)
            self.stage[p, k] += [u, d]

    def forward(self, p, k):
        off, nb, h, order = PARTS[p]
        place, axis = self.place, order[k]
        put, full = self.wires.put, (slice(None),) * (2 - k)
        up, down = place.ring(axis, 1), place.ring(axis, 3)
        over, under = place.at(axis, 1), place.at(axis, 3)
        ta, tb, fm, fp = self.bufs[p][k]
        a, b = self.stage[p, k][:2]
        g = self.g

        def add(t, v, buf, first, count):
            rest = rest_of(t, 2 - k)
            idx = self.tile(p, k, v, rest, first, count)
            g[idx] = g[idx] + buf[rest]

        a.wait_recv()
        pl.loop(0, 4 ** (2 - k))(lambda t: add(t, over, ta, 0, h))
        fa = put(self.view(p, k, over, 0, h), fm.at[full + (pl.ds(0, h),)], up)
        b.wait_recv()
        pl.loop(0, 4 ** (2 - k))(lambda t: add(t, under, tb, h, nb - h))
        fb = put(self.view(p, k, under, h, nb - h), fp.at[full + (pl.ds(h, nb - h),)], down)
        self.passed[p, k] = [fa, fb]

    def finish(self, p, k):
        off, nb, h, order = PARTS[p]
        me = self.place.pos[order[k]]
        ta, tb, fm, fp = self.bufs[p][k]
        g = self.g
        if k == 2:
            for copy in self.stage[p, k]:
                copy.wait_recv()
            idx = self.tile(p, k, me, (), 0, nb)
            total = (g[idx].astype(F32) + ta[...].astype(F32)) + (fm[...].astype(F32) + fp[...].astype(F32))
            g[idx] = total.astype(BF)
            return
        for copy in self.stage[p, k][2:] + self.passed[p, k]:
            copy.wait_recv()

        def add(t):
            rest = rest_of(t, 2 - k)
            idx = self.tile(p, k, me, rest, 0, nb)
            total = g[idx].astype(F32) + fm[rest].astype(F32) + fp[rest].astype(F32)
            g[idx] = total.astype(BF)

        pl.loop(0, 4 ** (2 - k))(add)


def scatter_scratch():
    out = []
    for p in range(3):
        _, nb, h, _ = PARTS[p]
        for k in range(3):
            lead = (4,) * (2 - k)
            sizes = (nb, 1, nb, nb) if k == 2 else (h, nb - h, nb, nb)
            out += [pltpu.VMEM(lead + (n, 16, 128), BF) for n in sizes]
    return out


def scatter_bufs(flat):
    return [[flat[(p * 3 + k) * 4:(p * 3 + k) * 4 + 4] for k in range(3)] for p in range(3)]


class Small:
    def __init__(self, place, wires, first, rest):
        self.place, self.wires, self.first, self.rest = place, wires, first, rest
        self.sent = []

    def start(self, k, value):
        place = self.place
        if k == 0:
            self.first[place.c] = value
            own = self.first.at[place.c]
            self.sent = [self.wires.put(own, own, place.partner())]
            return
        axis = k - 1
        self.rest[axis, place.pos[axis]] = value
        own = self.rest.at[axis, place.pos[axis]]
        self.sent = [self.wires.put(own, own, place.ring(axis, step)) for step in (1, 3, 2)]

    def finish(self, k):
        for copy in self.sent:
            copy.wait_recv()
        if k == 0:
            return self.first[0] + self.first[1]
        t = self.rest
        return (t[k - 1, 0] + t[k - 1, 1]) + (t[k - 1, 2] + t[k - 1, 3])


WIDTH = 5120
KEYS = 1024
ROWS = 384


def fused_kernel(slots_ref, owner_ref, tok_ref, gain_ref, bias_ref, kw_ref, cot_ref,
                 proj, grad_out, slab_out, gain_out, bias_out,
                 w, kws, held, g, half, slot, seen, fin, first, rest,
                 tok, normed, cot, inv, coef, small_v, even, odd, send, recv, local, *flat):
    place = Place()
    wires = Wires(send, recv, 220)
    grad_scale = float(ROWS * 128) ** (-0.5)
    loads = []

    def load(src, dst):
        copy = pltpu.make_async_copy(src, dst, local.at[len(loads)])
        copy.start()
        loads.append(copy)
        return copy

    wait_greet = greet(place)
    slabs = []
    for i in range(2):
        xh = place.xh if i == 0 else 1 - place.xh
        xl = place.xl if i == 0 else 1 - place.xl
        for t in range(4):
            col = pl.ds(pl.multiple_of((xh * 4 + t) * 128, 128), 128)
            slabs.append(load(kw_ref.at[:, xl * 4 + place.y, :, col], kws.at[i, t]))
    rows = [load(tok_ref.at[pl.ds(i * 64, 64)], tok.at[pl.ds(i * 64, 64)]) for i in range(6)]
    cots = load(cot_ref, cot)

    def norm(i):
        rows[i].wait()

        @pl.loop(i * 4, i * 4 + 4)
        def _(t):
            r = pl.ds(pl.multiple_of(t * 16, 16), 16)
            acc = [jnp.zeros((16, 128), F32)] * 4
            for j in range(40):
                v = tok[r, j * 128:(j + 1) * 128].astype(F32)
                acc[j % 4] = acc[j % 4] + v * v
            total = jnp.sum((acc[0] + acc[1]) + (acc[2] + acc[3]), axis=1, keepdims=True)
            scale = jnp.broadcast_to(lax.rsqrt(total * (1.0 / WIDTH) + EPS), (16, 128))
            inv[r, :] = scale
            for j in range(40):
                col = slice(j * 128, (j + 1) * 128)
                normed[r, col] = (tok[r, col].astype(F32) * scale * gain_ref[:, col]).astype(BF)

    own = place.c * HALF
    other = (1 - place.c) * HALF
    full = (slice(None),) * 3

    def blocks(side, first, count, add):
        b = side + first
        left = normed[:, pl.ds(pl.multiple_of(b * 128, 128), count * 128)]
        value = lax.dot_general(left, cot[...], (((0,), (0,)), ((), ())), preferred_element_type=F32)
        value = value * grad_scale
        for i in range(count):
            for r in range(8):
                for q in range(8):
                    at = (q // 4 * 2 + r // 4, r % 4, q % 4)
                    tile = value[i * 128 + r * 16:i * 128 + r * 16 + 16, q * 128:(q + 1) * 128]
                    if add:
                        tile = tile + half[at + (first + i,)].astype(F32)
                    g[at + (b + i,)] = tile.astype(BF)

    def partial(p, mine):
        off, nb = PARTS[p][:2]
        side = own if mine else other
        if mine:
            swap[p].wait_recv()

        @pl.loop(0, nb // 2)
        def _(t):
            blocks(side, off + 2 * t, 2, mine)

        if nb % 2:
            blocks(side, off + nb - 1, 1, mine)
        if not mine:
            swap.append(wires.put(
                g.at[full + (pl.ds(other + off, nb),)], half.at[full + (pl.ds(off, nb),)], place.partner()))

    swap = []
    gather = Gather(place, wires, w)
    scatter = Scatter(place, wires, g, scatter_bufs(flat))
    small = Small(place, wires, first, rest)
    come = []

    def trade_weights():
        for copy in slabs:
            copy.wait()
        mine = held.at[pl.ds(place.big * 4, 4)]
        for i, j, _, device in place.group():
            come.append(wires.put(kws.at[i, place.at(2, j)], mine, device))
        held[pl.ds(place.big * 4, 4)] = kws[0, place.z]

    def pick():
        for copy in come:
            copy.wait_recv()

        @pl.loop(0, HALF)
        def _(t):
            b = own + t
            w[place.x, place.y, place.z, b] = held[slots_ref[b]]

    def bias_sum():
        for j in range(8):
            small_v[40 + j:41 + j, :] = jnp.sum(
                cot[:, j * 128:(j + 1) * 128].astype(F32), axis=0, keepdims=True) * grad_scale

    def forward():
        for copy in gather.pair:
            copy.wait_recv()
        coef[...] = jnp.zeros_like(coef)

        @pl.loop(0, 4)
        def _(n):
            q = 2 * n
            x0, z0 = lax.div(q, 4) * 2, lax.rem(q, 4)
            right = jnp.concatenate(
                [jnp.concatenate([w[x0 + r // 4, r % 4, z0, b], w[x0 + r // 4, r % 4, z0 + 1, b]], axis=1)
                 for b in range(40) for r in range(8)], axis=0)
            value = jnp.dot(normed[...], right, preferred_element_type=F32)
            col = pl.ds(pl.multiple_of(n * 256, 256), 256)
            proj[:, col] = (value + bias_ref[:, col]).astype(BF)
            both = value * cot[:, col].astype(F32)
            coef[...] += both[:, :128] + both[:, 128:]

        coef[...] = jnp.broadcast_to(
            jnp.sum(coef[...], axis=1, keepdims=True), (ROWS, 128)) * inv[...] * (1.0 / WIDTH)

    def product(t, into):
        b = 2 * t
        right = jnp.concatenate(
            [jnp.concatenate([w[q // 4 * 2 + r // 4, r % 4, q % 4, b + i] for q in range(8)], axis=1)
             for i in range(2) for r in range(8)], axis=0)
        into[...] = lax.dot_general(cot[...], right, (((1,), (1,)), ((), ())), preferred_element_type=F32)

    def apply(t, grad):
        b = 2 * t
        for i in range(2):
            col = pl.ds(pl.multiple_of((b + i) * 128, 128), 128)
            gn = grad[:, i * 128:(i + 1) * 128]
            scale = inv[...]
            unit = tok[:, col].astype(F32) * scale
            small_v[pl.ds(b + i, 1), :] = jnp.sum(gn * unit, axis=0, keepdims=True) * grad_scale
            grad_out[:, col] = (gn * gain_ref[:, col] * scale - unit * coef[...]).astype(BF)

    def backward(low, high):
        if low == 0:
            product(0, even)

        @pl.loop(low, min(high, 9))
        def _(u):
            product(2 * u + 1, odd)
            apply(2 * u, even)
            product(2 * u + 2, even)
            apply(2 * u + 1, odd)

        if high == 10:
            product(19, odd)
            apply(18, even)
            apply(19, odd)

    def each(step, k, *part):
        for p in range(3):
            step(p, k, *part)

    def small_next(k):
        small.start(k + 1, small.finish(k))

    def small_end():
        total = small.finish(3)
        gain_out[...] = total[:40]
        bias_out[...] = total[40:]

    back = []

    def trade_grads():
        @pl.loop(0, 64)
        def _(t):
            b = owner_ref[t]
            ours = jnp.logical_and(b >= own, b < own + HALF)
            value = g[place.x, place.y, place.z, jnp.maximum(b, 0)]
            slot[t] = jnp.where(ours, value, jnp.zeros_like(value))

        for _, _, _, device in place.group():
            back.append(wires.put(
                slot.at[pl.ds(device[0] * 4, 4)], seen.at[place.c, place.xh, place.z], device))
        seen[place.c, place.xh, place.z] = slot[pl.ds(place.big * 4, 4)]

    pi, y = place.pi, place.y
    yup, ydown = place.ring(1, 1), place.ring(1, 3)
    below, above, across = place.at(1, 3), place.at(1, 1), place.at(1, 2)
    sent = {}

    def move(name, side, row, slot0, count, device):
        ref = fin.at[side, row, pl.ds(slot0, count)]
        sent[name] = wires.put(ref, ref, device)

    def ring(name, side, slot0):
        move(name + "u0", side, y, slot0, 1, yup)
        move(name + "d1", side, y, slot0 + 1, 1, ydown)
        move(name + "u1", side, y, slot0 + 1, 1, yup)
        move(name + "d0", side, y, slot0, 1, ydown)

    def ring_on(name, side, slot0):
        sent[name + "u0"].wait_recv()
        move(name + "f0", side, below, slot0, 1, yup)
        sent[name + "d1"].wait_recv()
        move(name + "f1", side, above, slot0 + 1, 1, ydown)

    def spread_start():
        for copy in back:
            copy.wait_recv()
        for q in range(8):
            fin[pi, y, :, q // 4, q % 4] = seen[0, q // 4, q % 4] + seen[1, q // 4, q % 4]
        move("px", pi, y, 0, 2, place.x_pair())
        ring("a", pi, 0)
        move("qx", pi, y, 2, 2, place.x_pair())
        ring("c", pi, 2)

    def spread_middle():
        sent["px"].wait_recv()
        ring("b", 1 - pi, 0)
        ring_on("a", pi, 0)
        ring_on("c", pi, 2)
        sent["cu1"].wait_recv()
        move("rx", pi, below, 2, 2, place.x_pair())
        sent["cd0"].wait_recv()
        move("sx", pi, above, 2, 2, place.x_pair())

    def spread_end():
        sent["cf0"].wait_recv()
        sent["cf1"].wait_recv()
        move("tx", pi, across, 2, 2, place.x_pair())
        ring_on("b", 1 - pi, 0)
        for name in ("au1", "ad0", "af0", "af1", "bu1", "bd0", "bf0", "bf1", "qx", "rx", "sx", "tx"):
            sent[name].wait_recv()

        @pl.loop(0, 32)
        def _(t):
            i, r = lax.div(t, 8), lax.rem(t, 8)
            for q in range(8):
                side = lax.rem(lax.div(r, 4) + q // 4, 2)
                slab_out[i, r, :, q * 128:(q + 1) * 128] = fin[side, lax.rem(r, 4), i, q // 4, q % 4].astype(F32)

    for i in range(3): norm(i)
    wait_greet()
    trade_weights()
    for i in range(3, 6): norm(i)
    cots.wait()
    partial(0, False)
    partial(1, False)
    pick()
    each(gather.start, 0)
    partial(2, False)
    partial(0, True)
    each(gather.finish, 0)
    each(gather.start, 1)
    partial(1, True)
    partial(2, True)
    each(gather.forward, 1)
    each(scatter.start, 0, 0)
    bias_sum()
    each(gather.finish, 1)
    each(gather.start, 2)
    each(scatter.start, 0, 1)
    each(gather.forward, 2)
    each(scatter.forward, 0)
    each(gather.finish, 2)
    forward()
    each(scatter.finish, 0)
    each(scatter.start, 1)
    backward(0, 4)
    each(scatter.forward, 1)
    backward(4, 8)
    each(scatter.finish, 1)
    each(scatter.start, 2)
    backward(8, 10)
    small.start(0, small_v[...])
    small_next(0)
    each(scatter.finish, 2)
    trade_grads()
    small_next(1)
    spread_start()
    small_next(2)
    spread_middle()
    small_end()
    spread_end()
    wires.drain()


def emit_kernel(*refs):
    sem = refs[-1]
    copies = [pltpu.make_async_copy(refs[i], refs[5 + i], sem.at[i]) for i in range(5)]
    for copy in copies:
        copy.start()
    for copy in copies:
        copy.wait()


VM = pl.BlockSpec(memory_space=pltpu.VMEM)
SM = pl.BlockSpec(memory_space=pltpu.SMEM)
ANY = pl.BlockSpec(memory_space=pl.ANY)
LIMIT = 56 * 1024 * 1024


OUTS = (
    ((ROWS, KEYS), BF),
    ((ROWS, WIDTH), BF),
    ((4, 8, 16, KEYS), F32),
    ((40, 128), F32),
    ((8, 128), F32),
)


def fused(block_slot, owner, tokens, gain, bias, key_weight, cotangent):
    outs = pl.pallas_call(
        fused_kernel,
        out_shape=tuple(pltpu.VMEM(*out) for out in OUTS),
        in_specs=[SM, SM, ANY, VM, VM, ANY, ANY],
        out_specs=(VM,) * 5,
        scratch_shapes=[
            pltpu.VMEM((4, 4, 4, 40, 16, 128), BF),
            pltpu.VMEM((2, 4, 4, 16, 128), BF),
            pltpu.VMEM((64, 16, 128), BF),
            pltpu.VMEM((4, 4, 4, 40, 16, 128), BF),
            pltpu.VMEM((4, 4, 4, 20, 16, 128), BF),
            pltpu.VMEM((64, 16, 128), BF),
            pltpu.VMEM((2, 2, 4, 4, 16, 128), BF),
            pltpu.VMEM((2, 4, 4, 2, 4, 16, 128), BF),
            pltpu.VMEM((2, 48, 128), F32),
            pltpu.VMEM((3, 4, 48, 128), F32),
            pltpu.VMEM((ROWS, WIDTH), BF),
            pltpu.VMEM((ROWS, WIDTH), BF),
            pltpu.VMEM((ROWS, KEYS), BF),
            pltpu.VMEM((ROWS, 128), F32),
            pltpu.VMEM((ROWS, 128), F32),
            pltpu.VMEM((48, 128), F32),
            pltpu.VMEM((ROWS, 256), F32),
            pltpu.VMEM((ROWS, 256), F32),
            pltpu.SemaphoreType.DMA((220,)),
            pltpu.SemaphoreType.DMA((220,)),
            pltpu.SemaphoreType.DMA((40,)),
        ] + scatter_scratch(),
        compiler_params=pltpu.CompilerParams(collective_id=0, has_side_effects=True, vmem_limit_bytes=LIMIT),
        name="fused",
    )(block_slot, owner, tokens, gain, bias, key_weight, cotangent)
    return pl.pallas_call(
        emit_kernel,
        out_shape=tuple(jax.ShapeDtypeStruct(*out) for out in OUTS),
        in_specs=[VM] * 5,
        out_specs=(ANY,) * 5,
        scratch_shapes=[pltpu.SemaphoreType.DMA((5,))],
        compiler_params=pltpu.CompilerParams(vmem_limit_bytes=1024 * 1024),
        name="emit",
    )(*(pltpu.with_memory_space_constraint(out, pltpu.VMEM) for out in outs))


def local(tokens, norm_gain, key_bias, key_weight, cotangent, block_slot):
    slots = jnp.arange(64, dtype=jnp.int32)
    hit = block_slot[None, :] == slots[:, None]
    owner = jnp.max(jnp.where(hit, jnp.arange(40, dtype=jnp.int32)[None, :], -1), axis=1)
    projected, token_grad, slab, gain, bias = fused(
        block_slot, owner, tokens, norm_gain.reshape(1, WIDTH), key_bias.reshape(1, KEYS),
        key_weight.reshape(4, 8, 16, KEYS), cotangent)
    return (projected, token_grad, slab.reshape(512, KEYS), gain.reshape(-1), bias.reshape(-1))


def solution(mesh):
    return jax.shard_map(
        local,
        mesh=mesh,
        in_specs=(
            P(("shard", "rep"), None),
            P(),
            P(),
            P("shard", None),
            P(("shard", "rep"), None),
            P(),
        ),
        out_specs=(
            P(("shard", "rep"), None),
            P(("shard", "rep"), None),
            P("shard", None),
            P(),
            P(),
        ),
        check_vma=False,
    )
```

```python
import functools

import jax
import jax.numpy as jnp
from jax import lax
from jax.experimental import pallas as pl
from jax.experimental.pallas import tpu as pltpu
from jax.sharding import PartitionSpec as P

MESH = pl.DeviceIdType.MESH
BLK = 128
EPS = 1e-06
HALF = 20
PARTS = (
    (0, 7, 4, (0, 1, 2)),
    (7, 7, 3, (1, 2, 0)),
    (14, 6, 3, (2, 0, 1)),
)
BF = jnp.bfloat16
F32 = jnp.float32


class Place:
    def __init__(self):
        big = lax.axis_index("shard")
        rep = lax.axis_index("rep")
        self.big, self.rep = big, rep
        self.c = lax.rem(big, 2)
        self.s = lax.div(big, 2)
        self.z = lax.rem(self.s, 4)
        xh = lax.div(big, 8)
        xl = lax.div(rep, 4)
        self.xl = xl
        self.xh = xh
        self.pi = lax.rem(xl + xh, 2)
        self.x = xh * 2 + xl
        self.y = lax.rem(rep, 4)
        self.pos = (self.x, self.y, self.z)

    def at(self, axis, step):
        return lax.rem(self.pos[axis] + step, 4)

    def device(self, pos, c):
        x, y, z = pos
        big = (lax.div(x, 2) * 4 + z) * 2 + c
        return (big, lax.rem(x, 2) * 4 + y)

    def ring(self, axis, step):
        pos = list(self.pos)
        pos[axis] = self.at(axis, step)
        return self.device(pos, self.c)

    def partner(self):
        return (self.s * 2 + 1 - self.c, self.rep)

    def x_pair(self):
        return (self.big, (1 - self.xl) * 4 + self.y)

    def group(self):
        for i in range(2):
            for j in range(4):
                for d in range(2):
                    if i == j == d == 0:
                        continue
                    xh = self.xh if i == 0 else 1 - self.xh
                    xl = self.xl if i == 0 else 1 - self.xl
                    core = self.c if d == 0 else 1 - self.c
                    yield i, j, d, ((xh * 4 + self.at(2, j)) * 2 + core, xl * 4 + self.y)


class Wires:
    def __init__(self, send, recv, limit):
        self.send, self.recv, self.limit, self.groups = send, recv, limit, []

    def group(self, total):
        i = len(self.groups)
        assert i < self.limit, "sems"
        self.groups.append(Group(self.send.at[i], self.recv.at[i], total))
        return self.groups[-1]

    def put(self, src, dst, device):
        return self.group(dst).put(src, dst, device)

    def drain(self):
        for group in self.groups:
            pltpu.make_async_copy(group.total, group.total, group.send).wait()


class Group:
    def __init__(self, send, recv, total):
        self.send, self.recv, self.total = send, recv, total

    def put(self, src, dst, device):
        pltpu.make_async_remote_copy(
            src_ref=src, dst_ref=dst, send_sem=self.send, recv_sem=self.recv,
            device_id=device, device_id_type=MESH,
        ).start()
        return self

    def wait(self):
        pltpu.make_async_copy(self.total, self.total, self.recv).wait()


def greet(place):
    barrier = pltpu.get_barrier_semaphore()
    peers = [device for _, _, _, device in place.group()]
    peers += [place.x_pair(), place.ring(0, 2)]
    peers += [place.ring(1, step) for step in (1, 2, 3)]
    for device in peers:
        pl.semaphore_signal(barrier, inc=1, device_id=device, device_id_type=MESH)
    return lambda: pl.semaphore_wait(barrier, len(peers))


def locate(place, order, k, v, done, later):
    out = [None] * 3
    for j, axis in enumerate(order):
        out[axis] = v if j == k else (done(axis) if j < k else later(axis))
    return tuple(out)


class Gather:
    def __init__(self, place, wires, w):
        self.place, self.wires, self.w = place, wires, w
        self.base = place.c * HALF
        self.stage = {}
        self.pair = wires.group(w.at[:, :, :, pl.ds(0, HALF)])

    def view(self, p, k, v, first, count):
        off, nb, h, order = PARTS[p]
        pos = self.place.pos
        idx = locate(self.place, order, k, v, lambda a: slice(None), lambda a: pos[a])
        return self.w.at[idx + (pl.ds(self.base + off + first, count),)]

    def move(self, group, p, k, v, first, count, device):
        ref = self.view(p, k, v, first, count)
        (group or self.wires.group(ref)).put(ref, ref, device)
        return group or self.wires.groups[-1]

    def start(self, p, k, part=None):
        off, nb, h, order = PARTS[p]
        place, axis, group = self.place, order[k], self.wires.group
        me = place.pos[axis]
        up, down = place.ring(axis, 1), place.ring(axis, 3)
        if k == 0:
            both = group(self.w.at[0, 0, 0, pl.ds(0, 3 * nb)])
            for device in (place.ring(axis, 2), up, down):
                self.move(both, p, k, me, 0, nb, device)
            self.stage[p, k] = both
            return
        if part != 1:
            u0 = self.move(None, p, k, me, 0, h, up)
            d1 = self.move(None, p, k, me, h, nb - h, down)
            self.stage[p, k] = [u0, d1]
        if part != 0:
            one = self.w.at[0, :, :, pl.ds(0, nb)]
            two = self.w.at[0, pl.ds(0, 2), :, pl.ds(0, nb)]
            late = group(one if k == 2 else two)
            self.move(late, p, k, me, h, nb - h, up)
            self.move(late, p, k, me, 0, h, down)
            self.stage[p, k] += [late, group(one) if k == 2 else late]

    def share(self, p, k, v, first, count):
        if k == 2:
            self.move(self.pair, p, k, v, first, count, self.place.partner())

    def forward(self, p, k):
        off, nb, h, order = PARTS[p]
        place, axis = self.place, order[k]
        u0, d1, late, last = self.stage[p, k]
        below, above = place.at(axis, 3), place.at(axis, 1)
        u0.wait()
        self.move(last, p, k, below, 0, h, place.ring(axis, 1))
        d1.wait()
        self.move(last, p, k, above, h, nb - h, place.ring(axis, 3))
        self.share(p, k, below, 0, h)
        self.share(p, k, above, h, nb - h)

    def arrive(self, p, k):
        off, nb, h, order = PARTS[p]
        place, axis = self.place, order[k]
        self.stage[p, k][2].wait()
        self.share(p, k, place.at(axis, 3), h, nb - h)
        self.share(p, k, place.at(axis, 1), 0, h)

    def finish(self, p, k):
        off, nb, h, order = PARTS[p]
        place, axis = self.place, order[k]
        if k == 0:
            self.stage[p, k].wait()
            return
        self.stage[p, k][3].wait()
        across = place.at(axis, 2)
        self.share(p, k, across, 0, h)
        self.share(p, k, across, h, nb - h)
        if k == 1:
            self.share(p, 2, place.pos[order[2]], 0, nb)


def rest_of(t, count):
    if count == 2:
        return (lax.div(t, 4), lax.rem(t, 4))
    return (t,) if count == 1 else ()


class Scatter:
    def __init__(self, place, wires, g, bufs):
        self.place, self.wires, self.g, self.bufs = place, wires, g, bufs
        self.base = place.c * HALF
        self.stage = {}

    def index(self, p, k, v, later):
        order = PARTS[p][3]
        pos = self.place.pos
        return locate(self.place, order, k, v, lambda a: pos[a], later)

    def view(self, p, k, v, first, count):
        idx = self.index(p, k, v, lambda a: slice(None))
        return self.g.at[idx + (pl.ds(self.base + PARTS[p][0] + first, count),)]

    def tile(self, p, k, v, rest, first, count):
        order = PARTS[p][3]
        later = sorted(order[k + 1:])
        idx = self.index(p, k, v, lambda a: rest[later.index(a)])
        return idx + (pl.ds(self.base + PARTS[p][0] + first, count),)

    def buf(self, p, k, which):
        return self.bufs[p][k][which]

    def start(self, p, k, part=None):
        off, nb, h, order = PARTS[p]
        place, axis = self.place, order[k]
        put, full = self.wires.put, (slice(None),) * (2 - k)
        up, down = place.ring(axis, 1), place.ring(axis, 3)
        over, under = place.at(axis, 1), place.at(axis, 3)
        across = place.at(axis, 2)
        ta, tb, fm, fp = self.bufs[p][k]
        if k == 2:
            both = self.wires.group(self.g.at[0, 0, 0, pl.ds(0, 3 * nb)])
            both.put(self.view(p, k, across, 0, nb), ta, place.ring(axis, 2))
            both.put(self.view(p, k, over, 0, nb), fm, up)
            both.put(self.view(p, k, under, 0, nb), fp, down)
            self.stage[p, k] = both
            return
        if part != 1:
            a = put(self.view(p, k, across, 0, h), ta, up)
            b = put(self.view(p, k, across, h, nb - h), tb, down)
            lead = (pl.ds(0, 2), slice(None), slice(None)) if k == 0 else (0, pl.ds(0, 2), slice(None))
            self.stage[p, k] = [a, b, self.wires.group(self.g.at[lead + (pl.ds(0, nb),)])]
        if part != 0:
            rest = self.stage[p, k][2]
            rest.put(self.view(p, k, over, h, nb - h), fm.at[full + (pl.ds(h, nb - h),)], up)
            rest.put(self.view(p, k, under, 0, h), fp.at[full + (pl.ds(0, h),)], down)

    def forward(self, p, k):
        off, nb, h, order = PARTS[p]
        place, axis = self.place, order[k]
        full = (slice(None),) * (2 - k)
        up, down = place.ring(axis, 1), place.ring(axis, 3)
        over, under = place.at(axis, 1), place.at(axis, 3)
        ta, tb, fm, fp = self.bufs[p][k]
        a, b, last = self.stage[p, k]
        g = self.g

        def add(t, v, buf, first, count):
            rest = rest_of(t, 2 - k)
            idx = self.tile(p, k, v, rest, first, count)
            g[idx] = g[idx] + buf[rest]

        a.wait()
        pl.loop(0, 4 ** (2 - k))(lambda t: add(t, over, ta, 0, h))
        last.put(self.view(p, k, over, 0, h), fm.at[full + (pl.ds(0, h),)], up)
        b.wait()
        pl.loop(0, 4 ** (2 - k))(lambda t: add(t, under, tb, h, nb - h))
        last.put(self.view(p, k, under, h, nb - h), fp.at[full + (pl.ds(h, nb - h),)], down)

    def finish(self, p, k):
        off, nb, h, order = PARTS[p]
        me = self.place.pos[order[k]]
        ta, tb, fm, fp = self.bufs[p][k]
        g = self.g
        if k == 2:
            self.stage[p, k].wait()
            idx = self.tile(p, k, me, (), 0, nb)
            total = (g[idx].astype(F32) + ta[...].astype(F32)) + (fm[...].astype(F32) + fp[...].astype(F32))
            g[idx] = total.astype(BF)
            return
        self.stage[p, k][2].wait()

        def add(t):
            rest = rest_of(t, 2 - k)
            idx = self.tile(p, k, me, rest, 0, nb)
            total = g[idx].astype(F32) + fm[rest].astype(F32) + fp[rest].astype(F32)
            g[idx] = total.astype(BF)

        pl.loop(0, 4 ** (2 - k))(add)


def scatter_scratch():
    out = []
    for p in range(3):
        _, nb, h, _ = PARTS[p]
        for k in range(3):
            lead = (4,) * (2 - k)
            sizes = (nb, 1, nb, nb) if k == 2 else (h, nb - h, nb, nb)
            out += [pltpu.VMEM(lead + (n, 16, 128), BF) for n in sizes]
    return out


def scatter_bufs(flat):
    return [[flat[(p * 3 + k) * 4:(p * 3 + k) * 4 + 4] for k in range(3)] for p in range(3)]


class Small:
    def __init__(self, place, wires, first, rest):
        self.place, self.wires, self.first, self.rest = place, wires, first, rest
        self.sent = []

    def start(self, k, value):
        place = self.place
        if k == 0:
            self.first[place.c] = value
            own = self.first.at[place.c]
            self.sent = self.wires.put(own, own, place.partner())
            return
        axis = k - 1
        self.rest[axis, place.pos[axis]] = value
        own = self.rest.at[axis, place.pos[axis]]
        self.sent = self.wires.group(self.rest.at[0, pl.ds(0, 3)])
        for step in (2, 1, 3):
            self.sent.put(own, own, place.ring(axis, step))

    def finish(self, k):
        self.sent.wait()
        if k == 0:
            return self.first[0] + self.first[1]
        t = self.rest
        return (t[k - 1, 0] + t[k - 1, 1]) + (t[k - 1, 2] + t[k - 1, 3])


WIDTH = 5120
KEYS = 1024
ROWS = 384


def fused_kernel(slots_ref, tok_ref, gain_ref, bias_ref, kw_ref, cot_ref,
                 proj, grad_out, slab_out, gain_out, bias_out,
                 w, kws, held, g, half, slot, seen, fin, first, rest,
                 tok, normed, cot, inv, coef, small_v, even, odd, owner, send, recv, local, *flat):
    place = Place()
    wires = Wires(send, recv, SEMS)
    grad_scale = float(ROWS * 128) ** (-0.5)

    def load(src, dst, i):
        copy = pltpu.make_async_copy(src, dst, local.at[i])
        copy.start()
        return copy

    wait_greet = greet(place)
    for i in range(2):
        xh = place.xh if i == 0 else 1 - place.xh
        xl = place.xl if i == 0 else 1 - place.xl
        for t in range(4):
            col = pl.ds(pl.multiple_of((xh * 4 + t) * 128, 128), 128)
            load(kw_ref.at[:, xl * 4 + place.y, :, col], kws.at[i, t], 0)
    rows = [load(tok_ref.at[pl.ds(i * 64, 64)], tok.at[pl.ds(i * 64, 64)], i + 1) for i in range(6)]
    cots = load(cot_ref, cot, 7)

    def norm(i):
        rows[i].wait()

        @pl.loop(i * 4, i * 4 + 4, unroll=2)
        def _(t):
            r = pl.ds(pl.multiple_of(t * 16, 16), 16)
            acc = [jnp.zeros((16, 128), F32)] * 4
            for j in range(40):
                v = tok[r, j * 128:(j + 1) * 128].astype(F32)
                acc[j % 4] = acc[j % 4] + v * v
            total = jnp.sum((acc[0] + acc[1]) + (acc[2] + acc[3]), axis=1, keepdims=True)
            scale = jnp.broadcast_to(lax.rsqrt(total * (1.0 / WIDTH) + EPS), (16, 128))
            inv[r, :] = scale
            for j in range(40):
                col = slice(j * 128, (j + 1) * 128)
                normed[r, col] = (tok[r, col].astype(F32) * scale * gain_ref[:, col]).astype(BF)

    own = place.c * HALF
    other = (1 - place.c) * HALF
    full = (slice(None),) * 3

    def blocks(side, first, count, add):
        b = side + first
        left = normed[:, pl.ds(pl.multiple_of(b * 128, 128), count * 128)]
        value = lax.dot_general(left, cot[...], (((0,), (0,)), ((), ())), preferred_element_type=F32)
        value = value * grad_scale
        for i in range(count):
            for r in range(8):
                for q in range(8):
                    at = (q // 4 * 2 + r // 4, r % 4, q % 4)
                    tile = value[i * 128 + r * 16:i * 128 + r * 16 + 16, q * 128:(q + 1) * 128]
                    if add:
                        tile = tile + half[at + (first + i,)].astype(F32)
                    g[at + (b + i,)] = tile.astype(BF)

    def partial(p, mine):
        off, nb = PARTS[p][:2]
        side = own if mine else other
        if mine:
            swap[p].wait()

        for t in range(nb // 2):
            blocks(side, off + 2 * t, 2, mine)

        if nb % 2:
            blocks(side, off + nb - 1, 1, mine)
        if not mine:
            swap.append(wires.put(
                g.at[full + (pl.ds(other + off, nb),)], half.at[full + (pl.ds(off, nb),)], place.partner()))

    swap = []
    gather = Gather(place, wires, w)
    scatter = Scatter(place, wires, g, scatter_bufs(flat))
    small = Small(place, wires, first, rest)
    come = wires.group(held.at[pl.ds(0, 60)])

    def trade_weights():
        pltpu.make_async_copy(kws, kws, local.at[0]).wait()
        mine = held.at[pl.ds(place.big * 4, 4)]
        for i, j, _, device in place.group():
            come.put(kws.at[i, place.at(2, j)], mine, device)
        held[pl.ds(place.big * 4, 4)] = kws[0, place.z]

    def pick():
        come.wait()

        @pl.loop(0, HALF)
        def _(t):
            b = own + t
            w[place.x, place.y, place.z, b] = held[slots_ref[b]]

    def bias_sum():
        for j in range(8):
            small_v[40 + j:41 + j, :] = jnp.sum(
                cot[:, j * 128:(j + 1) * 128].astype(F32), axis=0, keepdims=True) * grad_scale

    def forward(low, high):
        if low == 0:
            coef[...] = jnp.zeros_like(coef)

        @pl.loop(low, high)
        def _(n):
            q = 2 * n
            x0, z0 = lax.div(q, 4) * 2, lax.rem(q, 4)
            right = jnp.concatenate(
                [jnp.concatenate([w[x0 + r // 4, r % 4, z0, b], w[x0 + r // 4, r % 4, z0 + 1, b]], axis=1)
                 for b in range(40) for r in range(8)], axis=0)
            value = jnp.dot(normed[...], right, preferred_element_type=F32)
            col = pl.ds(pl.multiple_of(n * 256, 256), 256)
            proj[:, col] = (value + bias_ref[:, col]).astype(BF)
            both = value * cot[:, col].astype(F32)
            coef[...] += both[:, :128] + both[:, 128:]

        if high == 4:
            coef[...] = jnp.broadcast_to(
                jnp.sum(coef[...], axis=1, keepdims=True), (ROWS, 128)) * inv[...] * (1.0 / WIDTH)

    def product(t, into):
        b = 2 * t
        right = jnp.concatenate(
            [jnp.concatenate([w[q // 4 * 2 + r // 4, r % 4, q % 4, b + i] for q in range(8)], axis=1)
             for i in range(2) for r in range(8)], axis=0)
        into[...] = lax.dot_general(cot[...], right, (((1,), (1,)), ((), ())), preferred_element_type=F32)

    def apply(t, grad):
        b = 2 * t
        for i in range(2):
            col = pl.ds(pl.multiple_of((b + i) * 128, 128), 128)
            gn = grad[:, i * 128:(i + 1) * 128] * inv[...]
            small_v[pl.ds(b + i, 1), :] = jnp.sum(gn * tok[:, col].astype(F32), axis=0, keepdims=True) * grad_scale
            grad_out[:, col] = (gn * gain_ref[:, col]).astype(BF)

    def backward(mine, part):
        t0 = (place.c if mine else 1 - place.c) * (HALF // 2)
        if part == 0:
            if not mine:
                gather.pair.wait()
            product(t0, even)

        @pl.loop(2 * part, 2 * part + 2)
        def _(u):
            t = t0 + 2 * u
            product(t + 1, odd)
            apply(t, even)
            product(t + 2, even)
            apply(t + 1, odd)

        if part == 1:
            product(t0 + 9, odd)
            apply(t0 + 8, even)
            apply(t0 + 9, odd)

    def project_out(low, high):
        @pl.loop(low, high)
        def _(t):
            col = pl.ds(pl.multiple_of(t * 256, 256), 256)
            along = coef[...] * inv[...]
            along = jnp.concatenate([along, along], axis=1)
            grad_out[:, col] = (grad_out[:, col].astype(F32) - tok[:, col].astype(F32) * along).astype(BF)

    def each(step, k, *part):
        for p in range(3):
            step(p, k, *part)

    def small_next(k):
        small.start(k + 1, small.finish(k))

    def small_end():
        total = small.finish(3)
        gain_out[...] = total[:40]
        bias_out[...] = total[40:]

    back = wires.group(slot.at[pl.ds(0, 60)])

    def invert():
        @pl.loop(0, 64)
        def _(t):
            found = jnp.int32(-1)
            for b in range(40):
                found = jnp.where(slots_ref[b] == t, b, found)
            owner[t] = found

    def trade_grads():
        @pl.loop(0, 64)
        def _(t):
            b = owner[t]
            ours = jnp.logical_and(b >= own, b < own + HALF)
            value = g[place.x, place.y, place.z, jnp.maximum(b, 0)]
            slot[t] = jnp.where(ours, value, jnp.zeros_like(value))

        for _, _, _, device in place.group():
            back.put(slot.at[pl.ds(device[0] * 4, 4)], seen.at[place.c, place.xh, place.z], device)
        seen[place.c, place.xh, place.z] = slot[pl.ds(place.big * 4, 4)]

    pi, y = place.pi, place.y
    yup, ydown = place.ring(1, 1), place.ring(1, 3)
    below, above, across = place.at(1, 3), place.at(1, 1), place.at(1, 2)
    sent = {}
    last = wires.group(fin.at[0])

    def move(name, side, row, slot0, count, device):
        ref = fin.at[side, row, pl.ds(slot0, count)]
        if name in sent:
            sent[name].put(ref, ref, device)
        elif name:
            sent[name] = wires.put(ref, ref, device)
        else:
            last.put(ref, ref, device)

    def ring(name, side, slot0, late):
        move(name + "u", side, y, slot0, 1, yup)
        move(name + "d", side, y, slot0 + 1, 1, ydown)
        move(late, side, y, slot0 + 1, 1, yup)
        move(late, side, y, slot0, 1, ydown)

    def ring_on(name, side, slot0, late):
        sent[name + "u"].wait()
        move(late, side, below, slot0, 1, yup)
        sent[name + "d"].wait()
        move(late, side, above, slot0 + 1, 1, ydown)

    def spread_start():
        back.wait()
        for q in range(8):
            fin[pi, y, :, q // 4, q % 4] = seen[0, q // 4, q % 4] + seen[1, q // 4, q % 4]
        sent["c1"] = wires.group(fin.at[0, 0, pl.ds(0, 2)])
        sent["c2"] = wires.group(fin.at[0, 0, pl.ds(0, 2)])
        move("px", pi, y, 0, 2, place.x_pair())
        ring("a", pi, 0, "")
        move("", pi, y, 2, 2, place.x_pair())
        ring("c", pi, 2, "c1")

    def spread_middle():
        sent["px"].wait()
        ring("b", 1 - pi, 0, "")
        ring_on("a", pi, 0, "")
        ring_on("c", pi, 2, "c2")
        sent["c1"].wait()
        move("", pi, below, 2, 2, place.x_pair())
        move("", pi, above, 2, 2, place.x_pair())

    def spread_late():
        ring_on("b", 1 - pi, 0, "")
        sent["c2"].wait()
        move("", pi, across, 2, 2, place.x_pair())

    def spread_end():
        last.wait()

        @pl.loop(0, 32)
        def _(t):
            i, r = lax.div(t, 8), lax.rem(t, 8)
            for q in range(8):
                side = lax.rem(lax.div(r, 4) + q // 4, 2)
                slab_out[i, r, :, q * 128:(q + 1) * 128] = fin[side, lax.rem(r, 4), i, q // 4, q % 4].astype(F32)

    wait_greet()
    trade_weights()
    for i in range(6): norm(i)
    cots.wait()
    partial(0, False)
    partial(1, False)
    pick()
    each(gather.start, 0)
    partial(2, False)
    partial(0, True)
    each(gather.finish, 0)
    each(gather.start, 1)
    scatter.start(0, 0, 0)
    partial(1, True)
    scatter.start(1, 0, 0)
    partial(2, True)
    scatter.start(2, 0, 0)
    each(gather.forward, 1)
    each(scatter.start, 0, 1)
    bias_sum()
    invert()
    each(scatter.forward, 0)
    each(gather.finish, 1)
    each(gather.start, 2, 0)
    each(scatter.finish, 0)
    each(scatter.start, 1)
    each(gather.start, 2, 1)
    each(scatter.forward, 1)
    each(gather.forward, 2)
    each(scatter.finish, 1)
    each(scatter.start, 2)
    each(gather.arrive, 2)
    each(gather.finish, 2)
    backward(True, 0)
    each(scatter.finish, 2)
    trade_grads()
    backward(True, 1)
    backward(False, 0)
    spread_start()
    backward(False, 1)
    small.start(0, small_v[...])
    small_next(0)
    spread_middle()
    forward(0, 1)
    small_next(1)
    forward(1, 3)
    spread_late()
    small_next(2)
    forward(3, 4)
    project_out(0, 20)
    spread_end()
    small_end()
    wires.drain()


def emit_kernel(*refs):
    sem = refs[-1]
    copies = [pltpu.make_async_copy(refs[i], refs[5 + i], sem.at[i]) for i in range(5)]
    for copy in copies:
        copy.start()
    for copy in copies:
        copy.wait()


VM = pl.BlockSpec(memory_space=pltpu.VMEM)
SM = pl.BlockSpec(memory_space=pltpu.SMEM)
ANY = pl.BlockSpec(memory_space=pl.ANY)
LIMIT = 56 * 1024 * 1024


SEMS = 65
OUTS = (
    ((ROWS, KEYS), BF),
    ((ROWS, WIDTH), BF),
    ((4, 8, 16, KEYS), F32),
    ((40, 128), F32),
    ((8, 128), F32),
)


def fused(block_slot, tokens, gain, bias, key_weight, cotangent):
    outs = pl.pallas_call(
        fused_kernel,
        out_shape=tuple(pltpu.VMEM(*out) for out in OUTS),
        in_specs=[SM, ANY, VM, VM, ANY, ANY],
        out_specs=(VM,) * 5,
        scratch_shapes=[
            pltpu.VMEM((4, 4, 4, 40, 16, 128), BF),
            pltpu.VMEM((2, 4, 4, 16, 128), BF),
            pltpu.VMEM((64, 16, 128), BF),
            pltpu.VMEM((4, 4, 4, 40, 16, 128), BF),
            pltpu.VMEM((4, 4, 4, 20, 16, 128), BF),
            pltpu.VMEM((64, 16, 128), BF),
            pltpu.VMEM((2, 2, 4, 4, 16, 128), BF),
            pltpu.VMEM((2, 4, 4, 2, 4, 16, 128), BF),
            pltpu.VMEM((2, 48, 128), F32),
            pltpu.VMEM((3, 4, 48, 128), F32),
            pltpu.VMEM((ROWS, WIDTH), BF),
            pltpu.VMEM((ROWS, WIDTH), BF),
            pltpu.VMEM((ROWS, KEYS), BF),
            pltpu.VMEM((ROWS, 128), F32),
            pltpu.VMEM((ROWS, 128), F32),
            pltpu.VMEM((48, 128), F32),
            pltpu.VMEM((ROWS, 256), F32),
            pltpu.VMEM((ROWS, 256), F32),
            pltpu.SMEM((64,), jnp.int32),
            pltpu.SemaphoreType.DMA((SEMS,)),
            pltpu.SemaphoreType.DMA((SEMS,)),
            pltpu.SemaphoreType.DMA((8,)),
        ] + scatter_scratch(),
        compiler_params=pltpu.CompilerParams(collective_id=0, has_side_effects=True, vmem_limit_bytes=LIMIT),
        name="fused",
    )(block_slot, tokens, gain, bias, key_weight, cotangent)
    return pl.pallas_call(
        emit_kernel,
        out_shape=tuple(jax.ShapeDtypeStruct(*out) for out in OUTS),
        in_specs=[VM] * 5,
        out_specs=(ANY,) * 5,
        scratch_shapes=[pltpu.SemaphoreType.DMA((5,))],
        compiler_params=pltpu.CompilerParams(vmem_limit_bytes=1024 * 1024),
        name="emit",
    )(*(pltpu.with_memory_space_constraint(out, pltpu.VMEM) for out in outs))


def local(tokens, norm_gain, key_bias, key_weight, cotangent, block_slot):
    projected, token_grad, slab, gain, bias = fused(
        block_slot, tokens, norm_gain.reshape(1, WIDTH), key_bias.reshape(1, KEYS),
        key_weight.reshape(4, 8, 16, KEYS), cotangent)
    return (projected, token_grad, slab.reshape(512, KEYS), gain.reshape(-1), bias.reshape(-1))


def solution(mesh):
    return jax.shard_map(
        local,
        mesh=mesh,
        in_specs=(
            P(("shard", "rep"), None),
            P(),
            P(),
            P("shard", None),
            P(("shard", "rep"), None),
            P(),
        ),
        out_specs=(
            P(("shard", "rep"), None),
            P(("shard", "rep"), None),
            P("shard", None),
            P(),
            P(),
        ),
        check_vma=False,
    )
```

```python
import functools

import jax
import jax.numpy as jnp
from jax import lax
from jax.experimental import pallas as pl
from jax.experimental.pallas import tpu as pltpu
from jax.sharding import PartitionSpec as P

MESH = pl.DeviceIdType.MESH
BLK = 128
EPS = 1e-06
HALF = 20
PARTS = (
    (0, 7, 4, (0, 1, 2)),
    (7, 7, 3, (1, 2, 0)),
    (14, 6, 3, (2, 0, 1)),
)
BF = jnp.bfloat16
F32 = jnp.float32


class Place:
    def __init__(self):
        big = lax.axis_index("shard")
        rep = lax.axis_index("rep")
        self.big, self.rep = big, rep
        self.c = lax.rem(big, 2)
        self.s = lax.div(big, 2)
        self.z = lax.rem(self.s, 4)
        xh = lax.div(big, 8)
        xl = lax.div(rep, 4)
        self.xl = xl
        self.xh = xh
        self.pi = lax.rem(xl + xh, 2)
        self.x = xh * 2 + xl
        self.y = lax.rem(rep, 4)
        self.pos = (self.x, self.y, self.z)

    def at(self, axis, step):
        return lax.rem(self.pos[axis] + step, 4)

    def device(self, pos, c):
        x, y, z = pos
        big = (lax.div(x, 2) * 4 + z) * 2 + c
        return (big, lax.rem(x, 2) * 4 + y)

    def ring(self, axis, step):
        pos = list(self.pos)
        pos[axis] = self.at(axis, step)
        return self.device(pos, self.c)

    def partner(self):
        return (self.s * 2 + 1 - self.c, self.rep)

    def x_pair(self):
        return (self.big, (1 - self.xl) * 4 + self.y)

    def group(self):
        for i in range(2):
            for j in range(4):
                for d in range(2):
                    if i == j == d == 0:
                        continue
                    xh = self.xh if i == 0 else 1 - self.xh
                    xl = self.xl if i == 0 else 1 - self.xl
                    core = self.c if d == 0 else 1 - self.c
                    yield i, j, d, ((xh * 4 + self.at(2, j)) * 2 + core, xl * 4 + self.y)


class Wires:
    def __init__(self, send, recv, limit):
        self.send, self.recv, self.limit, self.groups = send, recv, limit, []

    def group(self, total):
        i = len(self.groups)
        assert i < self.limit, "sems"
        self.groups.append(Group(self.send.at[i], self.recv.at[i], total))
        return self.groups[-1]

    def put(self, src, dst, device):
        return self.group(dst).put(src, dst, device)

    def drain(self):
        for group in self.groups:
            pltpu.make_async_copy(group.total, group.total, group.send).wait()


class Group:
    def __init__(self, send, recv, total):
        self.send, self.recv, self.total = send, recv, total

    def put(self, src, dst, device):
        pltpu.make_async_remote_copy(
            src_ref=src, dst_ref=dst, send_sem=self.send, recv_sem=self.recv,
            device_id=device, device_id_type=MESH,
        ).start()
        return self

    def wait(self):
        pltpu.make_async_copy(self.total, self.total, self.recv).wait()


def greet(place):
    barrier = pltpu.get_barrier_semaphore()
    peers = [device for _, _, _, device in place.group()]
    peers += [place.x_pair(), place.ring(0, 2)]
    peers += [place.ring(1, step) for step in (1, 2, 3)]
    for device in peers:
        pl.semaphore_signal(barrier, inc=1, device_id=device, device_id_type=MESH)
    return lambda: pl.semaphore_wait(barrier, len(peers))


def locate(place, order, k, v, done, later):
    out = [None] * 3
    for j, axis in enumerate(order):
        out[axis] = v if j == k else (done(axis) if j < k else later(axis))
    return tuple(out)


BATCHES = (
    ((0, 4, 2), (4, 3, 2)),
    ((0, 4, 2), (4, 3, 1)),
    ((0, 2, 1), (2, 4, 2)),
)


class Gather:
    def __init__(self, place, wires, w):
        self.place, self.wires, self.w = place, wires, w
        self.base = place.c * HALF
        self.stage = {}
        half = HALF // 2
        self.pair = [wires.group(w.at[:, :, :, pl.ds(0, half)]) for _ in range(2)]

    def view(self, p, k, v, first, count):
        off, nb, h, order = PARTS[p]
        pos = self.place.pos
        idx = locate(self.place, order, k, v, lambda a: slice(None), lambda a: pos[a])
        return self.w.at[idx + (pl.ds(self.base + off + first, count),)]

    def move(self, group, p, k, v, first, count, device):
        ref = self.view(p, k, v, first, count)
        group = group or self.wires.group(ref)
        group.put(ref, ref, device)
        return group

    def span(self, p, k, batch):
        first, n, h = (0,) + PARTS[p][1:3] if k < 2 else BATCHES[p][batch]
        return first, h, n - h

    def start(self, p, k, batch=0, part=None):
        place, axis, group = self.place, PARTS[p][3][k], self.wires.group
        first, lo, hi = self.span(p, k, batch)
        mid = first + lo
        me = place.pos[axis]
        up, down = place.ring(axis, 1), place.ring(axis, 3)
        if k == 0:
            both = group(self.w.at[0, 0, 0, pl.ds(0, 3 * (lo + hi))])
            for device in (place.ring(axis, 2), up, down):
                self.move(both, p, k, me, 0, lo + hi, device)
            self.stage[p, k, 0] = both
            return
        if part != 1:
            u0 = self.move(None, p, k, me, first, lo, up)
            d1 = self.move(None, p, k, me, mid, hi, down)
            self.stage[p, k, batch] = [u0, d1]
        if part != 0:
            one = self.w.at[0, :, :, pl.ds(0, lo + hi)]
            two = self.w.at[0, pl.ds(0, 2), :, pl.ds(0, lo + hi)]
            late = group(one if k == 2 else two)
            self.move(late, p, k, me, mid, hi, up)
            self.move(late, p, k, me, first, lo, down)
            self.stage[p, k, batch] += [late, group(one) if k == 2 else late]

    def share(self, p, k, v, first, count, batch):
        if k == 2:
            self.move(self.pair[batch], p, k, v, first, count, self.place.partner())

    def forward(self, p, k, batch=0):
        place, axis = self.place, PARTS[p][3][k]
        first, lo, hi = self.span(p, k, batch)
        u0, d1, late, last = self.stage[p, k, batch]
        below, above = place.at(axis, 3), place.at(axis, 1)
        u0.wait()
        self.move(last, p, k, below, first, lo, place.ring(axis, 1))
        d1.wait()
        self.move(last, p, k, above, first + lo, hi, place.ring(axis, 3))
        self.share(p, k, below, first, lo, batch)
        self.share(p, k, above, first + lo, hi, batch)

    def arrive(self, p, k, batch=0):
        place, axis = self.place, PARTS[p][3][k]
        first, lo, hi = self.span(p, k, batch)
        self.stage[p, k, batch][2].wait()
        self.share(p, k, place.at(axis, 3), first + lo, hi, batch)
        self.share(p, k, place.at(axis, 1), first, lo, batch)

    def finish(self, p, k, batch=0):
        order = PARTS[p][3]
        place, axis = self.place, order[k]
        first, lo, hi = self.span(p, k, batch)
        if k == 0:
            self.stage[p, k, 0].wait()
            return
        self.stage[p, k, batch][3].wait()
        self.share(p, k, place.at(axis, 2), first, lo + hi, batch)
        if k == 1:
            for i, (start, n, _) in enumerate(BATCHES[p]):
                self.share(p, 2, place.pos[order[2]], start, n, i)


def rest_of(t, count):
    if count == 2:
        return (lax.div(t, 4), lax.rem(t, 4))
    return (t,) if count == 1 else ()


class Scatter:
    def __init__(self, place, wires, g, bufs):
        self.place, self.wires, self.g, self.bufs = place, wires, g, bufs
        self.base = place.c * HALF
        self.stage = {}

    def index(self, p, k, v, later):
        order = PARTS[p][3]
        pos = self.place.pos
        return locate(self.place, order, k, v, lambda a: pos[a], later)

    def view(self, p, k, v, first, count):
        idx = self.index(p, k, v, lambda a: slice(None))
        return self.g.at[idx + (pl.ds(self.base + PARTS[p][0] + first, count),)]

    def tile(self, p, k, v, rest, first, count):
        order = PARTS[p][3]
        later = sorted(order[k + 1:])
        idx = self.index(p, k, v, lambda a: rest[later.index(a)])
        return idx + (pl.ds(self.base + PARTS[p][0] + first, count),)

    def buf(self, p, k, which):
        return self.bufs[p][k][which]

    def start(self, p, k, part=None):
        off, nb, h, order = PARTS[p]
        place, axis = self.place, order[k]
        put, full = self.wires.put, (slice(None),) * (2 - k)
        up, down = place.ring(axis, 1), place.ring(axis, 3)
        over, under = place.at(axis, 1), place.at(axis, 3)
        across = place.at(axis, 2)
        ta, tb, fm, fp = self.bufs[p][k]
        if k == 2:
            both = self.wires.group(self.g.at[0, 0, 0, pl.ds(0, 3 * nb)])
            both.put(self.view(p, k, across, 0, nb), ta, place.ring(axis, 2))
            both.put(self.view(p, k, over, 0, nb), fm, up)
            both.put(self.view(p, k, under, 0, nb), fp, down)
            self.stage[p, k] = both
            return
        if part != 1:
            a = put(self.view(p, k, across, 0, h), ta, up)
            b = put(self.view(p, k, across, h, nb - h), tb, down)
            lead = (pl.ds(0, 2), slice(None), slice(None)) if k == 0 else (0, pl.ds(0, 2), slice(None))
            self.stage[p, k] = [a, b, self.wires.group(self.g.at[lead + (pl.ds(0, nb),)])]
        if part != 0:
            rest = self.stage[p, k][2]
            rest.put(self.view(p, k, over, h, nb - h), fm.at[full + (pl.ds(h, nb - h),)], up)
            rest.put(self.view(p, k, under, 0, h), fp.at[full + (pl.ds(0, h),)], down)

    def forward(self, p, k):
        off, nb, h, order = PARTS[p]
        place, axis = self.place, order[k]
        full = (slice(None),) * (2 - k)
        up, down = place.ring(axis, 1), place.ring(axis, 3)
        over, under = place.at(axis, 1), place.at(axis, 3)
        ta, tb, fm, fp = self.bufs[p][k]
        a, b, last = self.stage[p, k]
        g = self.g

        def add(t, v, buf, first, count):
            rest = rest_of(t, 2 - k)
            idx = self.tile(p, k, v, rest, first, count)
            g[idx] = g[idx] + buf[rest]

        a.wait()
        pl.loop(0, 4 ** (2 - k))(lambda t: add(t, over, ta, 0, h))
        last.put(self.view(p, k, over, 0, h), fm.at[full + (pl.ds(0, h),)], up)
        b.wait()
        pl.loop(0, 4 ** (2 - k))(lambda t: add(t, under, tb, h, nb - h))
        last.put(self.view(p, k, under, h, nb - h), fp.at[full + (pl.ds(h, nb - h),)], down)

    def finish(self, p, k):
        off, nb, h, order = PARTS[p]
        me = self.place.pos[order[k]]
        ta, tb, fm, fp = self.bufs[p][k]
        g = self.g
        if k == 2:
            self.stage[p, k].wait()
            idx = self.tile(p, k, me, (), 0, nb)
            total = (g[idx].astype(F32) + ta[...].astype(F32)) + (fm[...].astype(F32) + fp[...].astype(F32))
            g[idx] = total.astype(BF)
            return
        self.stage[p, k][2].wait()

        def add(t):
            rest = rest_of(t, 2 - k)
            idx = self.tile(p, k, me, rest, 0, nb)
            total = g[idx].astype(F32) + fm[rest].astype(F32) + fp[rest].astype(F32)
            g[idx] = total.astype(BF)

        pl.loop(0, 4 ** (2 - k))(add)


def scatter_scratch():
    out = []
    for p in range(3):
        _, nb, h, _ = PARTS[p]
        for k in range(3):
            lead = (4,) * (2 - k)
            sizes = (nb, 1, nb, nb) if k == 2 else (h, nb - h, nb, nb)
            out += [pltpu.VMEM(lead + (n, 16, 128), BF) for n in sizes]
    return out


def scatter_bufs(flat):
    return [[flat[(p * 3 + k) * 4:(p * 3 + k) * 4 + 4] for k in range(3)] for p in range(3)]


class Small:
    def __init__(self, place, wires, first, rest):
        self.place, self.wires, self.first, self.rest = place, wires, first, rest
        self.sent = []

    def start(self, k, value):
        place = self.place
        if k == 0:
            self.first[place.c] = value
            own = self.first.at[place.c]
            self.sent = self.wires.put(own, own, place.partner())
            return
        axis = 3 - k
        self.rest[k - 1, place.pos[axis]] = value
        own = self.rest.at[k - 1, place.pos[axis]]
        self.sent = self.wires.group(self.rest.at[0, pl.ds(0, 3)])
        for step in (2, 1, 3):
            self.sent.put(own, own, place.ring(axis, step))

    def finish(self, k):
        self.sent.wait()
        if k == 0:
            return self.first[0] + self.first[1]
        t = self.rest
        return (t[k - 1, 0] + t[k - 1, 1]) + (t[k - 1, 2] + t[k - 1, 3])


WIDTH = 5120
KEYS = 1024
ROWS = 384


def fused_kernel(slots_hbm, tok_ref, gain_hbm, bias_hbm, kw_ref, cot_ref,
                 proj, grad_out, slab_out, gain_out, bias_out,
                 w, kws, held, g, half, slot, seen, fin, first, rest,
                 tok, normed, cot, inv, coef, small_v, even, odd, keys, owner, slots_ref, gain_ref, bias_ref, send, recv, local, *flat):
    place = Place()
    wires = Wires(send, recv, SEMS)
    grad_scale = float(ROWS * 128) ** (-0.5)

    def load(src, dst, i):
        copy = pltpu.make_async_copy(src, dst, local.at[i])
        copy.start()
        return copy

    gains = load(gain_hbm, gain_ref, 8)
    wait_greet = greet(place)
    for i in range(2):
        xh = place.xh if i == 0 else 1 - place.xh
        xl = place.xl if i == 0 else 1 - place.xl
        for t in range(4):
            col = pl.ds(pl.multiple_of((xh * 4 + t) * 128, 128), 128)
            load(kw_ref.at[:, xl * 4 + place.y, :, col], kws.at[i, t], 0)
    rows = [load(tok_ref.at[pl.ds(i * 64, 64)], tok.at[pl.ds(i * 64, 64)], i + 1) for i in range(6)]
    cots = load(cot_ref, cot, 7)
    slot_list = load(slots_hbm, slots_ref, 9)
    biases = load(bias_hbm, bias_ref, 10)

    def norm(i):
        rows[i].wait()
        if i == 0:
            gains.wait()

        @pl.loop(i * 4, i * 4 + 4, unroll=2)
        def _(t):
            r = pl.ds(pl.multiple_of(t * 16, 16), 16)
            acc = [jnp.zeros((16, 128), F32)] * 4
            for j in range(40):
                v = tok[r, j * 128:(j + 1) * 128].astype(F32)
                acc[j % 4] = acc[j % 4] + v * v
            total = jnp.sum((acc[0] + acc[1]) + (acc[2] + acc[3]), axis=1, keepdims=True)
            scale = jnp.broadcast_to(lax.rsqrt(total * (1.0 / WIDTH) + EPS), (16, 128))
            inv[r, :] = scale
            for j in range(40):
                col = slice(j * 128, (j + 1) * 128)
                normed[r, col] = (tok[r, col].astype(F32) * scale * gain_ref[:, col]).astype(BF)

    own = place.c * HALF
    other = (1 - place.c) * HALF
    full = (slice(None),) * 3

    def blocks(side, first, count):
        b = side + first
        left = normed[:, pl.ds(pl.multiple_of(b * 128, 128), count * 128)]
        value = lax.dot_general(left, cot[...], (((0,), (0,)), ((), ())), preferred_element_type=F32)
        value = (value * grad_scale).astype(BF)
        for i in range(count):
            for r in range(8):
                for q in range(8):
                    g[q // 4 * 2 + r // 4, r % 4, q % 4, b + i] = value[
                        i * 128 + r * 16:i * 128 + r * 16 + 16, q * 128:(q + 1) * 128]

    def partial(p, mine):
        off, nb = PARTS[p][:2]
        side = own if mine else other
        for t in range(nb // 2):
            blocks(side, off + 2 * t, 2)
        if nb % 2:
            blocks(side, off + nb - 1, 1)

    def plane(p, step):
        axis = PARTS[p][3][0]
        at = [slice(None)] * 3
        at[axis] = place.at(axis, step)
        return axis, tuple(at)

    def swap(p, step, group=None):
        off, nb = PARTS[p][:2]
        _, at = plane(p, step)
        dst = half.at[at + (pl.ds(off, nb),)]
        group = group or wires.group(dst)
        group.put(g.at[at + (pl.ds(other + off, nb),)], dst, place.partner())
        return group

    def swap_rest(p):
        group = wires.group(half.at[pl.ds(0, 3), :, :, pl.ds(0, PARTS[p][1])])
        for step in (1, 3, 0):
            swap(p, step, group)
        return group

    def merge(p, *steps):
        off, nb = PARTS[p][:2]
        for step in steps:
            axis, at = plane(p, step)

            @pl.loop(0, 16, unroll=2)
            def _(t):
                rest = [lax.div(t, 4), lax.rem(t, 4)]
                rest.insert(axis, at[axis])
                here = tuple(rest) + (pl.ds(own + off, nb),)
                g[here] = g[here] + half[tuple(rest) + (pl.ds(off, nb),)]

    def merge_far(p):
        far[p].wait()
        merge(p, 2)

    def merge_near(p):
        near[p].wait()
        merge(p, 1, 3, 0)

    far, near = [], []
    gather = Gather(place, wires, w)
    scatter = Scatter(place, wires, g, scatter_bufs(flat))
    small = Small(place, wires, first, rest)
    come = wires.group(held.at[pl.ds(0, 60)])

    def trade_weights():
        pltpu.make_async_copy(kws, kws, local.at[0]).wait()
        mine = held.at[pl.ds(place.big * 4, 4)]
        for i, j, _, device in place.group():
            come.put(kws.at[i, place.at(2, j)], mine, device)
        held[pl.ds(place.big * 4, 4)] = kws[0, place.z]

    def pick():
        come.wait()
        slot_list.wait()

        @pl.loop(0, HALF)
        def _(t):
            b = own + t
            w[place.x, place.y, place.z, b] = held[slots_ref[b]]

    def bias_sum():
        biases.wait()
        for j in range(8):
            small_v[40 + j:41 + j, :] = jnp.sum(
                cot[:, j * 128:(j + 1) * 128].astype(F32), axis=0, keepdims=True) * grad_scale

    def early(batch):
        return [PARTS[p][0] + BATCHES[p][batch][0] + i for p in range(3) for i in range(BATCHES[p][batch][1])]

    def forward(batch, low, high):
        some = [side * HALF + b for side in range(2) for b in early(batch)]

        @pl.loop(low, high)
        def _(n):
            q = 2 * n
            x0, z0 = lax.div(q, 4) * 2, lax.rem(q, 4)
            left = jnp.concatenate([normed[:, b * 128:(b + 1) * 128] for b in some], axis=1)
            right = jnp.concatenate(
                [jnp.concatenate([w[x0 + r // 4, r % 4, z0, b], w[x0 + r // 4, r % 4, z0 + 1, b]], axis=1)
                 for b in some for r in range(8)], axis=0)
            value = jnp.dot(left, right, preferred_element_type=F32)
            col = pl.ds(pl.multiple_of(n * 256, 256), 256)
            if batch == 0:
                keys[:, col] = value
                return
            value = value + keys[:, col]
            proj[:, col] = (value + bias_ref[:, col]).astype(BF)
            both = value * cot[:, col].astype(F32)
            both = both[:, :128] + both[:, 128:]
            if low == 0:
                both = jnp.where(n == 0, 0.0, coef[...]) + both
            else:
                both = coef[...] + both
            coef[...] = both

        if batch == 1 and high == 4:
            coef[...] = jnp.broadcast_to(
                jnp.sum(coef[...], axis=1, keepdims=True), (ROWS, 128)) * inv[...] * inv[...] * (1.0 / WIDTH)

    def product(side, pair, into):
        right = jnp.concatenate(
            [jnp.concatenate([w[q // 4 * 2 + r // 4, r % 4, q % 4, side + b] for q in range(8)], axis=1)
             for b in pair for r in range(8)], axis=0)
        into[...] = lax.dot_general(cot[...], right, (((1,), (1,)), ((), ())), preferred_element_type=F32)

    def apply(side, pair, grad):
        for i, b in enumerate(pair):
            col = pl.ds(pl.multiple_of((side + b) * 128, 128), 128)
            gn = grad[:, i * 128:(i + 1) * 128] * inv[...]
            small_v[pl.ds(side + b, 1), :] = jnp.sum(
                gn * tok[:, col].astype(F32), axis=0, keepdims=True) * grad_scale
            grad_out[:, col] = (gn * gain_ref[:, col]).astype(BF)

    def backward(batch, side):
        some = early(batch)
        pairs = [some[i:i + 2] for i in range(0, len(some), 2)]
        product(side, pairs[0], even)
        for i, pair in enumerate(pairs):
            here, there = (even, odd) if i % 2 == 0 else (odd, even)
            if i + 1 < len(pairs):
                product(side, pairs[i + 1], there)
            apply(side, pair, here)

    def backward_early(mine):
        if not mine:
            gather.pair[0].wait()
        backward(0, own if mine else other)

    def backward_late(mine):
        if not mine:
            gather.pair[1].wait()
        backward(1, own if mine else other)

    def project_out(low, high):
        @pl.loop(low, high)
        def _(t):
            col = pl.ds(pl.multiple_of(t * 256, 256), 256)
            along = jnp.concatenate([coef[...], coef[...]], axis=1)
            grad_out[:, col] = (grad_out[:, col].astype(F32) - tok[:, col].astype(F32) * along).astype(BF)

    def each(step, k, *part):
        for p in range(3):
            step(p, k, *part)

    def small_next(k):
        small.start(k + 1, small.finish(k))

    def small_end():
        total = small.finish(3)
        gain_out[...] = total[:40]
        bias_out[...] = total[40:]

    back = wires.group(slot.at[pl.ds(0, 60)])

    def invert():
        @pl.loop(0, 64)
        def _(t):
            found = jnp.int32(-1)
            for b in range(40):
                found = jnp.where(slots_ref[b] == t, b, found)
            owner[t] = found

    def trade_grads():
        @pl.loop(0, 64, unroll=4)
        def _(t):
            b = owner[t]
            ours = jnp.logical_and(b >= own, b < own + HALF)
            value = g[place.x, place.y, place.z, jnp.maximum(b, 0)]
            slot[t] = jnp.where(ours, value, jnp.zeros_like(value))

        for _, _, _, device in place.group():
            back.put(slot.at[pl.ds(device[0] * 4, 4)], seen.at[place.c, place.xh, place.z], device)
        seen[place.c, place.xh, place.z] = slot[pl.ds(place.big * 4, 4)]

    pi, y = place.pi, place.y
    yup, ydown = place.ring(1, 1), place.ring(1, 3)
    below, above, across = place.at(1, 3), place.at(1, 1), place.at(1, 2)
    sent = {}
    last = wires.group(fin.at[0])

    def move(name, side, row, slot0, count, device):
        ref = fin.at[side, row, pl.ds(slot0, count)]
        if name in sent:
            sent[name].put(ref, ref, device)
        elif name:
            sent[name] = wires.put(ref, ref, device)
        else:
            last.put(ref, ref, device)

    def ring(name, side, slot0, late):
        move(name + "u", side, y, slot0, 1, yup)
        move(name + "d", side, y, slot0 + 1, 1, ydown)
        move(late, side, y, slot0 + 1, 1, yup)
        move(late, side, y, slot0, 1, ydown)

    def ring_on(name, side, slot0, late):
        sent[name + "u"].wait()
        move(late, side, below, slot0, 1, yup)
        sent[name + "d"].wait()
        move(late, side, above, slot0 + 1, 1, ydown)

    def spread_start():
        back.wait()
        for q in range(8):
            fin[pi, y, :, q // 4, q % 4] = seen[0, q // 4, q % 4] + seen[1, q // 4, q % 4]
        sent["c1"] = wires.group(fin.at[0, 0, pl.ds(0, 2)])
        sent["c2"] = wires.group(fin.at[0, 0, pl.ds(0, 2)])
        move("px", pi, y, 0, 2, place.x_pair())
        ring("c", pi, 2, "c1")
        ring("a", pi, 0, "")
        move("", pi, y, 2, 2, place.x_pair())

    def spread_on():
        ring_on("c", pi, 2, "c2")

    def spread_middle():
        sent["px"].wait()
        ring("b", 1 - pi, 0, "")
        sent["c1"].wait()
        move("", pi, below, 2, 2, place.x_pair())
        move("", pi, above, 2, 2, place.x_pair())
        ring_on("a", pi, 0, "")

    def spread_late():
        sent["c2"].wait()
        move("", pi, across, 2, 2, place.x_pair())
        ring_on("b", 1 - pi, 0, "")

    def spread_end():
        last.wait()

        @pl.loop(0, 32)
        def _(t):
            i, r = lax.div(t, 8), lax.rem(t, 8)
            for q in range(8):
                side = lax.rem(lax.div(r, 4) + q // 4, 2)
                slab_out[i, r, :, q * 128:(q + 1) * 128] = fin[side, lax.rem(r, 4), i, q // 4, q % 4].astype(F32)

    for i in range(3): norm(i)
    wait_greet()
    trade_weights()
    for i in range(3, 6): norm(i)
    cots.wait()
    partial(0, False)
    far.append(swap(0, 2))
    partial(1, False)
    far.append(swap(1, 2))
    partial(2, False)
    far.append(swap(2, 2))
    near.extend(swap_rest(p) for p in range(3))
    partial(0, True)
    pick()
    each(gather.start, 0)
    merge_far(0)
    scatter.start(0, 0, 0)
    partial(1, True)
    merge_far(1)
    scatter.start(1, 0, 0)
    partial(2, True)
    each(gather.finish, 0)
    each(gather.start, 1)
    merge_far(2)
    scatter.start(2, 0, 0)
    for p in range(3): merge_near(p); scatter.start(p, 0, 1)
    for p in (1, 2): gather.forward(p, 1)
    scatter.forward(0, 0)
    gather.forward(0, 1)
    scatter.forward(1, 0)
    bias_sum()
    invert()
    scatter.forward(2, 0)
    for p in (2, 0, 1): gather.finish(p, 1); gather.start(p, 2, 0, 0)
    for p in range(3): scatter.finish(p, 0); scatter.start(p, 1)
    each(gather.start, 2, 0, 1)
    each(scatter.forward, 1)
    each(gather.forward, 2, 0)
    each(gather.start, 2, 1, 0)
    each(scatter.finish, 1)
    each(scatter.start, 2)
    each(gather.start, 2, 1, 1)
    each(gather.arrive, 2, 0)
    each(gather.finish, 2, 0)
    backward_early(True)
    each(gather.forward, 2, 1)
    each(scatter.finish, 2)
    trade_grads()
    each(gather.arrive, 2, 1)
    backward_early(False)
    each(gather.finish, 2, 1)
    backward_late(True)
    spread_start()
    backward_late(False)
    small.start(0, small_v[...])
    forward(0, 0, 2)
    small_next(0)
    spread_on()
    forward(0, 2, 3)
    spread_middle()
    forward(0, 3, 4)
    forward(1, 0, 1)
    small_next(1)
    forward(1, 1, 2)
    spread_late()
    forward(1, 2, 4)
    small_next(2)
    project_out(0, 20)
    spread_end()
    small_end()
    wires.drain()


def emit_kernel(*refs):
    sem = refs[-1]
    copies = [pltpu.make_async_copy(refs[i], refs[5 + i], sem.at[i]) for i in range(5)]
    for copy in copies:
        copy.start()
    for copy in copies:
        copy.wait()


VM = pl.BlockSpec(memory_space=pltpu.VMEM)
SM = pl.BlockSpec(memory_space=pltpu.SMEM)
ANY = pl.BlockSpec(memory_space=pl.ANY)
LIMIT = 56 * 1024 * 1024


SEMS = 81
OUTS = (
    ((ROWS, KEYS), BF),
    ((ROWS, WIDTH), BF),
    ((4, 8, 16, KEYS), F32),
    ((40, 128), F32),
    ((8, 128), F32),
)


def fused(block_slot, tokens, gain, bias, key_weight, cotangent):
    outs = pl.pallas_call(
        fused_kernel,
        out_shape=tuple(pltpu.VMEM(*out) for out in OUTS),
        in_specs=[ANY] * 6,
        out_specs=(VM,) * 5,
        scratch_shapes=[
            pltpu.VMEM((4, 4, 4, 40, 16, 128), BF),
            pltpu.VMEM((2, 4, 4, 16, 128), BF),
            pltpu.VMEM((64, 16, 128), BF),
            pltpu.VMEM((4, 4, 4, 40, 16, 128), BF),
            pltpu.VMEM((4, 4, 4, 20, 16, 128), BF),
            pltpu.VMEM((64, 16, 128), BF),
            pltpu.VMEM((2, 2, 4, 4, 16, 128), BF),
            pltpu.VMEM((2, 4, 4, 2, 4, 16, 128), BF),
            pltpu.VMEM((2, 48, 128), F32),
            pltpu.VMEM((3, 4, 48, 128), F32),
            pltpu.VMEM((ROWS, WIDTH), BF),
            pltpu.VMEM((ROWS, WIDTH), BF),
            pltpu.VMEM((ROWS, KEYS), BF),
            pltpu.VMEM((ROWS, 128), F32),
            pltpu.VMEM((ROWS, 128), F32),
            pltpu.VMEM((48, 128), F32),
            pltpu.VMEM((ROWS, 256), F32),
            pltpu.VMEM((ROWS, 256), F32),
            pltpu.VMEM((ROWS, KEYS), F32),
            pltpu.SMEM((64,), jnp.int32),
            pltpu.SMEM((40,), jnp.int32),
            pltpu.VMEM((1, WIDTH), F32),
            pltpu.VMEM((1, KEYS), F32),
            pltpu.SemaphoreType.DMA((SEMS,)),
            pltpu.SemaphoreType.DMA((SEMS,)),
            pltpu.SemaphoreType.DMA((11,)),
        ] + scatter_scratch(),
        compiler_params=pltpu.CompilerParams(collective_id=0, has_side_effects=True, vmem_limit_bytes=LIMIT),
        name="fused",
    )(block_slot, tokens, gain, bias, key_weight, cotangent)
    return pl.pallas_call(
        emit_kernel,
        out_shape=tuple(jax.ShapeDtypeStruct(*out) for out in OUTS),
        in_specs=[VM] * 5,
        out_specs=(ANY,) * 5,
        scratch_shapes=[pltpu.SemaphoreType.DMA((5,))],
        compiler_params=pltpu.CompilerParams(vmem_limit_bytes=1024 * 1024),
        name="emit",
    )(*(pltpu.with_memory_space_constraint(out, pltpu.VMEM) for out in outs))


def local(tokens, norm_gain, key_bias, key_weight, cotangent, block_slot):
    projected, token_grad, slab, gain, bias = fused(
        block_slot, tokens, norm_gain.reshape(1, WIDTH), key_bias.reshape(1, KEYS),
        key_weight.reshape(4, 8, 16, KEYS), cotangent)
    return (projected, token_grad, slab.reshape(512, KEYS), gain.reshape(-1), bias.reshape(-1))


def solution(mesh):
    return jax.shard_map(
        local,
        mesh=mesh,
        in_specs=(
            P(("shard", "rep"), None),
            P(),
            P(),
            P("shard", None),
            P(("shard", "rep"), None),
            P(),
        ),
        out_specs=(
            P(("shard", "rep"), None),
            P(("shard", "rep"), None),
            P("shard", None),
            P(),
            P(),
        ),
        check_vma=False,
    )
```

```python
import functools

import jax
import jax.numpy as jnp
from jax import lax
from jax.experimental import pallas as pl
from jax.experimental.pallas import tpu as pltpu
from jax.sharding import PartitionSpec as P

MESH = pl.DeviceIdType.MESH
BLK = 128
EPS = 1e-06
HALF = 20
PARTS = (
    (0, 7, 4, (0, 1, 2)),
    (7, 7, 3, (1, 2, 0)),
    (14, 6, 3, (2, 0, 1)),
)
BF = jnp.bfloat16
F32 = jnp.float32


class Place:
    def __init__(self):
        big = lax.axis_index("shard")
        rep = lax.axis_index("rep")
        self.big, self.rep = big, rep
        self.c = lax.rem(big, 2)
        self.s = lax.div(big, 2)
        self.z = lax.rem(self.s, 4)
        xh = lax.div(big, 8)
        xl = lax.div(rep, 4)
        self.xl = xl
        self.xh = xh
        self.pi = lax.rem(xl + xh, 2)
        self.x = xh * 2 + xl
        self.y = lax.rem(rep, 4)
        self.pos = (self.x, self.y, self.z)

    def at(self, axis, step):
        return lax.rem(self.pos[axis] + step, 4)

    def device(self, pos, c):
        x, y, z = pos
        big = (lax.div(x, 2) * 4 + z) * 2 + c
        return (big, lax.rem(x, 2) * 4 + y)

    def ring(self, axis, step):
        pos = list(self.pos)
        pos[axis] = self.at(axis, step)
        return self.device(pos, self.c)

    def partner(self):
        return (self.s * 2 + 1 - self.c, self.rep)

    def x_pair(self):
        return (self.big, (1 - self.xl) * 4 + self.y)

    def group(self):
        for i in range(2):
            for j in range(4):
                for d in range(2):
                    if i == j == d == 0:
                        continue
                    xh = self.xh if i == 0 else 1 - self.xh
                    xl = self.xl if i == 0 else 1 - self.xl
                    core = self.c if d == 0 else 1 - self.c
                    yield i, j, d, ((xh * 4 + self.at(2, j)) * 2 + core, xl * 4 + self.y)


class Wires:
    def __init__(self, send, recv, limit):
        self.send, self.recv, self.limit = send, recv, limit
        self.count, self.lanes = 0, []

    def lane(self, total):
        self.lanes.append((self.send.at[len(self.lanes)], total))
        return self.lanes[-1][0]

    def group(self, total, lane=None):
        i = self.count
        self.count += 1
        assert i < self.limit, "sems"
        return Group(self.lane(total) if lane is None else lane, self.recv.at[i], total)

    def put(self, src, dst, device, lane=None):
        return self.group(dst, lane).put(src, dst, device)

    def drain(self):
        for sem, total in self.lanes:
            pltpu.make_async_copy(total, total, sem).wait()


def thirds(wires, ref):
    blocks = pl.ds(0, HALF)
    return [
        wires.lane(ref.at[0, 0, pl.ds(0, 3), blocks]),
        wires.lane(ref.at[0, pl.ds(0, 3), :, blocks]),
        wires.lane(ref.at[pl.ds(0, 3), :, :, blocks]),
    ]


class Group:
    def __init__(self, send, recv, total):
        self.send, self.recv, self.total = send, recv, total

    def put(self, src, dst, device):
        pltpu.make_async_remote_copy(
            src_ref=src, dst_ref=dst, send_sem=self.send, recv_sem=self.recv,
            device_id=device, device_id_type=MESH,
        ).start()
        return self

    def wait(self):
        pltpu.make_async_copy(self.total, self.total, self.recv).wait()


def greet(place):
    barrier = pltpu.get_barrier_semaphore()
    peers = [device for _, _, _, device in place.group()]
    peers += [place.x_pair(), place.ring(0, 2)]
    peers += [place.ring(1, step) for step in (1, 2, 3)]
    for device in peers:
        pl.semaphore_signal(barrier, inc=1, device_id=device, device_id_type=MESH)
    return lambda: pl.semaphore_wait(barrier, len(peers))


def locate(place, order, k, v, done, later):
    out = [None] * 3
    for j, axis in enumerate(order):
        out[axis] = v if j == k else (done(axis) if j < k else later(axis))
    return tuple(out)


BATCHES = (
    ((0, 4, 2), (4, 3, 2)),
    ((0, 4, 2), (4, 3, 1)),
    ((0, 2, 1), (2, 4, 2)),
)


class Gather:
    def __init__(self, place, wires, w):
        self.place, self.wires, self.w = place, wires, w
        self.base = place.c * HALF
        self.stage = {}
        half = HALF // 2
        self.lanes = thirds(wires, w)
        across = wires.lane(w.at[:, :, :, pl.ds(0, HALF)])
        self.pair = [wires.group(w.at[:, :, :, pl.ds(0, half)], across) for _ in range(2)]

    def view(self, p, k, v, first, count):
        off, nb, h, order = PARTS[p]
        pos = self.place.pos
        idx = locate(self.place, order, k, v, lambda a: slice(None), lambda a: pos[a])
        return self.w.at[idx + (pl.ds(self.base + off + first, count),)]

    def move(self, group, p, k, v, first, count, device):
        ref = self.view(p, k, v, first, count)
        group = group or self.wires.group(ref, self.lanes[k])
        group.put(ref, ref, device)
        return group

    def span(self, p, k, batch):
        first, n, h = (0,) + PARTS[p][1:3] if k < 2 else BATCHES[p][batch]
        return first, h, n - h

    def start(self, p, k, batch=0, part=None):
        place, axis = self.place, PARTS[p][3][k]
        group = functools.partial(self.wires.group, lane=self.lanes[k])
        first, lo, hi = self.span(p, k, batch)
        mid = first + lo
        me = place.pos[axis]
        up, down = place.ring(axis, 1), place.ring(axis, 3)
        if k == 0:
            both = group(self.w.at[0, 0, 0, pl.ds(0, 3 * (lo + hi))])
            for device in (place.ring(axis, 2), up, down):
                self.move(both, p, k, me, 0, lo + hi, device)
            self.stage[p, k, 0] = both
            return
        if part != 1:
            u0 = self.move(None, p, k, me, first, lo, up)
            d1 = self.move(None, p, k, me, mid, hi, down)
            self.stage[p, k, batch] = [u0, d1]
        if part != 0:
            one = self.w.at[0, :, :, pl.ds(0, lo + hi)]
            two = self.w.at[0, pl.ds(0, 2), :, pl.ds(0, lo + hi)]
            late = group(one if k == 2 else two)
            self.move(late, p, k, me, mid, hi, up)
            self.move(late, p, k, me, first, lo, down)
            self.stage[p, k, batch] += [late, group(one) if k == 2 else late]

    def share(self, p, k, v, first, count, batch):
        if k == 2:
            self.move(self.pair[batch], p, k, v, first, count, self.place.partner())

    def forward(self, p, k, batch=0):
        place, axis = self.place, PARTS[p][3][k]
        first, lo, hi = self.span(p, k, batch)
        u0, d1, late, last = self.stage[p, k, batch]
        below, above = place.at(axis, 3), place.at(axis, 1)
        u0.wait()
        self.move(last, p, k, below, first, lo, place.ring(axis, 1))
        d1.wait()
        self.move(last, p, k, above, first + lo, hi, place.ring(axis, 3))
        self.share(p, k, below, first, lo, batch)
        self.share(p, k, above, first + lo, hi, batch)

    def arrive(self, p, k, batch=0):
        place, axis = self.place, PARTS[p][3][k]
        first, lo, hi = self.span(p, k, batch)
        self.stage[p, k, batch][2].wait()
        self.share(p, k, place.at(axis, 3), first + lo, hi, batch)
        self.share(p, k, place.at(axis, 1), first, lo, batch)

    def finish(self, p, k, batch=0):
        order = PARTS[p][3]
        place, axis = self.place, order[k]
        first, lo, hi = self.span(p, k, batch)
        if k == 0:
            self.stage[p, k, 0].wait()
            return
        self.stage[p, k, batch][3].wait()
        self.share(p, k, place.at(axis, 2), first, lo + hi, batch)
        if k == 1:
            for i, (start, n, _) in enumerate(BATCHES[p]):
                self.share(p, 2, place.pos[order[2]], start, n, i)


def rest_of(t, count):
    if count == 2:
        return (lax.div(t, 4), lax.rem(t, 4))
    return (t,) if count == 1 else ()


class Scatter:
    def __init__(self, place, wires, g, bufs):
        self.place, self.wires, self.g, self.bufs = place, wires, g, bufs
        self.base = place.c * HALF
        self.stage = {}
        self.lanes = thirds(wires, g)[::-1]

    def index(self, p, k, v, later):
        order = PARTS[p][3]
        pos = self.place.pos
        return locate(self.place, order, k, v, lambda a: pos[a], later)

    def view(self, p, k, v, first, count):
        idx = self.index(p, k, v, lambda a: slice(None))
        return self.g.at[idx + (pl.ds(self.base + PARTS[p][0] + first, count),)]

    def tile(self, p, k, v, rest, first, count):
        order = PARTS[p][3]
        later = sorted(order[k + 1:])
        idx = self.index(p, k, v, lambda a: rest[later.index(a)])
        return idx + (pl.ds(self.base + PARTS[p][0] + first, count),)

    def buf(self, p, k, which):
        return self.bufs[p][k][which]

    def start(self, p, k, part=None):
        off, nb, h, order = PARTS[p]
        place, axis = self.place, order[k]
        full = (slice(None),) * (2 - k)
        put = functools.partial(self.wires.put, lane=self.lanes[k])
        up, down = place.ring(axis, 1), place.ring(axis, 3)
        over, under = place.at(axis, 1), place.at(axis, 3)
        across = place.at(axis, 2)
        ta, tb, fm, fp = self.bufs[p][k]
        if k == 2:
            both = self.wires.group(self.g.at[0, 0, 0, pl.ds(0, 3 * nb)], self.lanes[k])
            both.put(self.view(p, k, across, 0, nb), ta, place.ring(axis, 2))
            both.put(self.view(p, k, over, 0, nb), fm, up)
            both.put(self.view(p, k, under, 0, nb), fp, down)
            self.stage[p, k] = both
            return
        if part != 1:
            a = put(self.view(p, k, across, 0, h), ta, up)
            b = put(self.view(p, k, across, h, nb - h), tb, down)
            lead = (pl.ds(0, 2), slice(None), slice(None)) if k == 0 else (0, pl.ds(0, 2), slice(None))
            self.stage[p, k] = [a, b, self.wires.group(self.g.at[lead + (pl.ds(0, nb),)], self.lanes[k])]
        if part != 0:
            rest = self.stage[p, k][2]
            rest.put(self.view(p, k, over, h, nb - h), fm.at[full + (pl.ds(h, nb - h),)], up)
            rest.put(self.view(p, k, under, 0, h), fp.at[full + (pl.ds(0, h),)], down)

    def forward(self, p, k):
        off, nb, h, order = PARTS[p]
        place, axis = self.place, order[k]
        full = (slice(None),) * (2 - k)
        up, down = place.ring(axis, 1), place.ring(axis, 3)
        over, under = place.at(axis, 1), place.at(axis, 3)
        ta, tb, fm, fp = self.bufs[p][k]
        a, b, last = self.stage[p, k]
        g = self.g

        def add(t, v, buf, first, count):
            rest = rest_of(t, 2 - k)
            idx = self.tile(p, k, v, rest, first, count)
            g[idx] = g[idx] + buf[rest]

        a.wait()
        pl.loop(0, 4 ** (2 - k))(lambda t: add(t, over, ta, 0, h))
        last.put(self.view(p, k, over, 0, h), fm.at[full + (pl.ds(0, h),)], up)
        b.wait()
        pl.loop(0, 4 ** (2 - k))(lambda t: add(t, under, tb, h, nb - h))
        last.put(self.view(p, k, under, h, nb - h), fp.at[full + (pl.ds(h, nb - h),)], down)

    def finish(self, p, k):
        off, nb, h, order = PARTS[p]
        me = self.place.pos[order[k]]
        ta, tb, fm, fp = self.bufs[p][k]
        g = self.g
        if k == 2:
            self.stage[p, k].wait()
            idx = self.tile(p, k, me, (), 0, nb)
            total = (g[idx].astype(F32) + ta[...].astype(F32)) + (fm[...].astype(F32) + fp[...].astype(F32))
            g[idx] = total.astype(BF)
            return
        self.stage[p, k][2].wait()

        def add(t):
            rest = rest_of(t, 2 - k)
            idx = self.tile(p, k, me, rest, 0, nb)
            total = g[idx].astype(F32) + fm[rest].astype(F32) + fp[rest].astype(F32)
            g[idx] = total.astype(BF)

        pl.loop(0, 4 ** (2 - k))(add)


def scatter_scratch():
    out = []
    for p in range(3):
        _, nb, h, _ = PARTS[p]
        for k in range(3):
            lead = (4,) * (2 - k)
            sizes = (nb, 1, nb, nb) if k == 2 else (h, nb - h, nb, nb)
            out += [pltpu.VMEM(lead + (n, 16, 128), BF) for n in sizes]
    return out


def scatter_bufs(flat):
    return [[flat[(p * 3 + k) * 4:(p * 3 + k) * 4 + 4] for k in range(3)] for p in range(3)]


class Small:
    def __init__(self, place, wires, first, rest):
        self.place, self.wires, self.first, self.rest = place, wires, first, rest
        self.sent = []

    def start(self, k, value):
        place = self.place
        if k == 0:
            self.first[place.c] = value
            own = self.first.at[place.c]
            self.sent = self.wires.put(own, own, place.partner())
            return
        axis = 3 - k
        self.rest[k - 1, place.pos[axis]] = value
        own = self.rest.at[k - 1, place.pos[axis]]
        self.sent = self.wires.group(self.rest.at[0, pl.ds(0, 3)])
        for step in (2, 1, 3):
            self.sent.put(own, own, place.ring(axis, step))

    def finish(self, k):
        self.sent.wait()
        if k == 0:
            return self.first[0] + self.first[1]
        t = self.rest
        return (t[k - 1, 0] + t[k - 1, 1]) + (t[k - 1, 2] + t[k - 1, 3])


WIDTH = 5120
KEYS = 1024
ROWS = 384


def fused_kernel(slots_hbm, tok_ref, gain_hbm, bias_hbm, kw_ref, cot_ref,
                 proj, grad_out, slab_out, gain_out, bias_out,
                 w, kws, held, g, half, slot, seen, fin, first, rest,
                 tok, normed, cot, inv, coef, small_v, even, odd, keys, owner, slots_ref, gain_ref, bias_ref, send, recv, local, *flat):
    place = Place()
    wires = Wires(send, recv, SEMS)
    grad_scale = float(ROWS * 128) ** (-0.5)

    def load(src, dst, i):
        copy = pltpu.make_async_copy(src, dst, local.at[i])
        copy.start()
        return copy

    gains = load(gain_hbm, gain_ref, 8)
    wait_greet = greet(place)
    for i in range(2):
        xh = place.xh if i == 0 else 1 - place.xh
        xl = place.xl if i == 0 else 1 - place.xl
        for t in range(4):
            col = pl.ds(pl.multiple_of((xh * 4 + t) * 128, 128), 128)
            load(kw_ref.at[:, xl * 4 + place.y, :, col], kws.at[i, t], 0)
    rows = [load(tok_ref.at[pl.ds(i * 64, 64)], tok.at[pl.ds(i * 64, 64)], i + 1) for i in range(6)]
    cots = load(cot_ref, cot, 7)
    slot_list = load(slots_hbm, slots_ref, 9)
    biases = load(bias_hbm, bias_ref, 10)

    def norm(i):
        rows[i].wait()
        if i == 0:
            gains.wait()

        @pl.loop(i * 4, i * 4 + 4, unroll=2)
        def _(t):
            r = pl.ds(pl.multiple_of(t * 16, 16), 16)
            acc = [jnp.zeros((16, 128), F32)] * 4
            for j in range(40):
                v = tok[r, j * 128:(j + 1) * 128].astype(F32)
                acc[j % 4] = acc[j % 4] + v * v
            total = jnp.sum((acc[0] + acc[1]) + (acc[2] + acc[3]), axis=1, keepdims=True)
            scale = jnp.broadcast_to(lax.rsqrt(total * (1.0 / WIDTH) + EPS), (16, 128))
            inv[r, :] = scale
            for j in range(40):
                col = slice(j * 128, (j + 1) * 128)
                normed[r, col] = (tok[r, col].astype(F32) * scale * gain_ref[:, col]).astype(BF)

    own = place.c * HALF
    other = (1 - place.c) * HALF
    full = (slice(None),) * 3

    def blocks(side, first, count):
        b = side + first
        left = normed[:, pl.ds(pl.multiple_of(b * 128, 128), count * 128)]
        value = lax.dot_general(left, cot[...], (((0,), (0,)), ((), ())), preferred_element_type=F32)
        value = (value * grad_scale).astype(BF)
        for i in range(count):
            for r in range(8):
                for q in range(8):
                    g[q // 4 * 2 + r // 4, r % 4, q % 4, b + i] = value[
                        i * 128 + r * 16:i * 128 + r * 16 + 16, q * 128:(q + 1) * 128]

    def partial(p, mine):
        off, nb = PARTS[p][:2]
        side = own if mine else other
        for t in range(nb // 2):
            blocks(side, off + 2 * t, 2)
        if nb % 2:
            blocks(side, off + nb - 1, 1)

    def plane(p, step):
        axis = PARTS[p][3][0]
        at = [slice(None)] * 3
        at[axis] = place.at(axis, step)
        return axis, tuple(at)

    def swap(p, step, group=None):
        off, nb = PARTS[p][:2]
        _, at = plane(p, step)
        dst = half.at[at + (pl.ds(off, nb),)]
        group = group or wires.group(dst, swaps)
        group.put(g.at[at + (pl.ds(other + off, nb),)], dst, place.partner())
        return group

    def swap_rest(p):
        group = wires.group(half.at[pl.ds(0, 3), :, :, pl.ds(0, PARTS[p][1])], swaps)
        for step in (1, 3, 0):
            swap(p, step, group)
        return group

    def merge(p, *steps):
        off, nb = PARTS[p][:2]
        for step in steps:
            axis, at = plane(p, step)

            @pl.loop(0, 16, unroll=2)
            def _(t):
                rest = [lax.div(t, 4), lax.rem(t, 4)]
                rest.insert(axis, at[axis])
                here = tuple(rest) + (pl.ds(own + off, nb),)
                g[here] = g[here] + half[tuple(rest) + (pl.ds(off, nb),)]

    def merge_far(p):
        far[p].wait()
        merge(p, 2)

    def merge_near(p):
        near[p].wait()
        merge(p, 1, 3, 0)

    far, near = [], []
    swaps = wires.lane(half)
    gather = Gather(place, wires, w)
    scatter = Scatter(place, wires, g, scatter_bufs(flat))
    small = Small(place, wires, first, rest)
    come = wires.group(held.at[pl.ds(0, 60)])

    def trade_weights():
        pltpu.make_async_copy(kws, kws, local.at[0]).wait()
        mine = held.at[pl.ds(place.big * 4, 4)]
        for i, j, _, device in place.group():
            come.put(kws.at[i, place.at(2, j)], mine, device)
        held[pl.ds(place.big * 4, 4)] = kws[0, place.z]

    def pick():
        come.wait()
        slot_list.wait()

        @pl.loop(0, HALF)
        def _(t):
            b = own + t
            w[place.x, place.y, place.z, b] = held[slots_ref[b]]

    def bias_sum():
        biases.wait()
        for j in range(8):
            small_v[40 + j:41 + j, :] = jnp.sum(
                cot[:, j * 128:(j + 1) * 128].astype(F32), axis=0, keepdims=True) * grad_scale

    def early(batch):
        return [PARTS[p][0] + BATCHES[p][batch][0] + i for p in range(3) for i in range(BATCHES[p][batch][1])]

    def forward(batch, low, high):
        some = [side * HALF + b for side in range(2) for b in early(batch)]

        @pl.loop(low, high)
        def _(n):
            q = 2 * n
            x0, z0 = lax.div(q, 4) * 2, lax.rem(q, 4)
            left = jnp.concatenate([normed[:, b * 128:(b + 1) * 128] for b in some], axis=1)
            right = jnp.concatenate(
                [jnp.concatenate([w[x0 + r // 4, r % 4, z0, b], w[x0 + r // 4, r % 4, z0 + 1, b]], axis=1)
                 for b in some for r in range(8)], axis=0)
            value = jnp.dot(left, right, preferred_element_type=F32)
            col = pl.ds(pl.multiple_of(n * 256, 256), 256)
            if batch == 0:
                keys[:, col] = value
                return
            value = value + keys[:, col]
            proj[:, col] = (value + bias_ref[:, col]).astype(BF)
            both = value * cot[:, col].astype(F32)
            both = both[:, :128] + both[:, 128:]
            if low == 0:
                both = jnp.where(n == 0, 0.0, coef[...]) + both
            else:
                both = coef[...] + both
            coef[...] = both

        if batch == 1 and high == 4:
            coef[...] = jnp.broadcast_to(
                jnp.sum(coef[...], axis=1, keepdims=True), (ROWS, 128)) * inv[...] * inv[...] * (1.0 / WIDTH)

    def product(side, pair, into):
        right = jnp.concatenate(
            [jnp.concatenate([w[q // 4 * 2 + r // 4, r % 4, q % 4, side + b] for q in range(8)], axis=1)
             for b in pair for r in range(8)], axis=0)
        into[...] = lax.dot_general(cot[...], right, (((1,), (1,)), ((), ())), preferred_element_type=F32)

    def apply(side, pair, grad):
        for i, b in enumerate(pair):
            col = pl.ds(pl.multiple_of((side + b) * 128, 128), 128)
            gn = grad[:, i * 128:(i + 1) * 128] * inv[...]
            small_v[pl.ds(side + b, 1), :] = jnp.sum(
                gn * tok[:, col].astype(F32), axis=0, keepdims=True) * grad_scale
            grad_out[:, col] = (gn * gain_ref[:, col]).astype(BF)

    def backward(batch, side):
        some = early(batch)
        pairs = [some[i:i + 2] for i in range(0, len(some), 2)]
        product(side, pairs[0], even)
        for i, pair in enumerate(pairs):
            here, there = (even, odd) if i % 2 == 0 else (odd, even)
            if i + 1 < len(pairs):
                product(side, pairs[i + 1], there)
            apply(side, pair, here)

    def backward_early(mine):
        if not mine:
            gather.pair[0].wait()
        backward(0, own if mine else other)

    def backward_late(mine):
        if not mine:
            gather.pair[1].wait()
        backward(1, own if mine else other)

    def project_out(low, high):
        @pl.loop(low, high)
        def _(t):
            col = pl.ds(pl.multiple_of(t * 256, 256), 256)
            along = jnp.concatenate([coef[...], coef[...]], axis=1)
            grad_out[:, col] = (grad_out[:, col].astype(F32) - tok[:, col].astype(F32) * along).astype(BF)

    def each(step, k, *part):
        for p in range(3):
            step(p, k, *part)

    def small_next(k):
        small.start(k + 1, small.finish(k))

    def small_end():
        total = small.finish(3)
        gain_out[...] = total[:40]
        bias_out[...] = total[40:]

    back = wires.group(slot.at[pl.ds(0, 60)])

    def invert():
        @pl.loop(0, 64)
        def _(t):
            found = jnp.int32(-1)
            for b in range(40):
                found = jnp.where(slots_ref[b] == t, b, found)
            owner[t] = found

    def trade_grads():
        @pl.loop(0, 64, unroll=4)
        def _(t):
            b = owner[t]
            ours = jnp.logical_and(b >= own, b < own + HALF)
            value = g[place.x, place.y, place.z, jnp.maximum(b, 0)]
            slot[t] = jnp.where(ours, value, jnp.zeros_like(value))

        for _, _, _, device in place.group():
            back.put(slot.at[pl.ds(device[0] * 4, 4)], seen.at[place.c, place.xh, place.z], device)
        seen[place.c, place.xh, place.z] = slot[pl.ds(place.big * 4, 4)]

    pi, y = place.pi, place.y
    yup, ydown = place.ring(1, 1), place.ring(1, 3)
    below, above, across = place.at(1, 3), place.at(1, 1), place.at(1, 2)
    sent = {}
    last = wires.group(fin.at[0])

    def move(name, side, row, slot0, count, device):
        ref = fin.at[side, row, pl.ds(slot0, count)]
        if name in sent:
            sent[name].put(ref, ref, device)
        elif name:
            sent[name] = wires.put(ref, ref, device)
        else:
            last.put(ref, ref, device)

    def ring(name, side, slot0, late):
        move(name + "u", side, y, slot0, 1, yup)
        move(name + "d", side, y, slot0 + 1, 1, ydown)
        move(late, side, y, slot0 + 1, 1, yup)
        move(late, side, y, slot0, 1, ydown)

    def ring_on(name, side, slot0, late):
        sent[name + "u"].wait()
        move(late, side, below, slot0, 1, yup)
        sent[name + "d"].wait()
        move(late, side, above, slot0 + 1, 1, ydown)

    def spread_start():
        back.wait()
        for q in range(8):
            fin[pi, y, :, q // 4, q % 4] = seen[0, q // 4, q % 4] + seen[1, q // 4, q % 4]
        sent["c1"] = wires.group(fin.at[0, 0, pl.ds(0, 2)])
        sent["c2"] = wires.group(fin.at[0, 0, pl.ds(0, 2)])
        move("px", pi, y, 0, 2, place.x_pair())
        ring("c", pi, 2, "c1")
        ring("a", pi, 0, "")
        move("", pi, y, 2, 2, place.x_pair())

    def spread_on():
        ring_on("c", pi, 2, "c2")

    def spread_middle():
        sent["px"].wait()
        ring("b", 1 - pi, 0, "")
        sent["c1"].wait()
        move("", pi, below, 2, 2, place.x_pair())
        move("", pi, above, 2, 2, place.x_pair())
        ring_on("a", pi, 0, "")

    def spread_late():
        sent["c2"].wait()
        move("", pi, across, 2, 2, place.x_pair())
        ring_on("b", 1 - pi, 0, "")

    def spread_end():
        last.wait()

        @pl.loop(0, 32)
        def _(t):
            i, r = lax.div(t, 8), lax.rem(t, 8)
            for q in range(8):
                side = lax.rem(lax.div(r, 4) + q // 4, 2)
                slab_out[i, r, :, q * 128:(q + 1) * 128] = fin[side, lax.rem(r, 4), i, q // 4, q % 4].astype(F32)

    for i in range(3): norm(i)
    wait_greet()
    trade_weights()
    for i in range(3, 6): norm(i)
    cots.wait()
    partial(0, False)
    far.append(swap(0, 2))
    partial(1, False)
    far.append(swap(1, 2))
    partial(2, False)
    far.append(swap(2, 2))
    near.extend(swap_rest(p) for p in range(3))
    partial(0, True)
    pick()
    each(gather.start, 0)
    merge_far(0)
    scatter.start(0, 0, 0)
    partial(1, True)
    merge_far(1)
    scatter.start(1, 0, 0)
    partial(2, True)
    each(gather.finish, 0)
    each(gather.start, 1)
    merge_far(2)
    scatter.start(2, 0, 0)
    for p in range(3): merge_near(p); scatter.start(p, 0, 1)
    for p in (1, 2): gather.forward(p, 1)
    scatter.forward(0, 0)
    gather.forward(0, 1)
    scatter.forward(1, 0)
    bias_sum()
    invert()
    scatter.forward(2, 0)
    for p in (2, 0, 1): gather.finish(p, 1); gather.start(p, 2, 0, 0)
    for p in range(3): scatter.finish(p, 0); scatter.start(p, 1)
    each(gather.start, 2, 0, 1)
    each(scatter.forward, 1)
    each(gather.forward, 2, 0)
    each(gather.start, 2, 1, 0)
    each(scatter.finish, 1)
    each(scatter.start, 2)
    each(gather.start, 2, 1, 1)
    each(gather.arrive, 2, 0)
    each(gather.finish, 2, 0)
    backward_early(True)
    each(gather.forward, 2, 1)
    each(scatter.finish, 2)
    trade_grads()
    each(gather.arrive, 2, 1)
    backward_early(False)
    each(gather.finish, 2, 1)
    backward_late(True)
    spread_start()
    backward_late(False)
    small.start(0, small_v[...])
    forward(0, 0, 2)
    small_next(0)
    spread_on()
    forward(0, 2, 4)
    spread_middle()
    forward(1, 0, 2)
    small_next(1)
    spread_late()
    forward(1, 2, 4)
    small_next(2)
    project_out(0, 20)
    spread_end()
    small_end()
    wires.drain()


def emit_kernel(*refs):
    sem = refs[-1]
    copies = [pltpu.make_async_copy(refs[i], refs[5 + i], sem.at[i]) for i in range(5)]
    for copy in copies:
        copy.start()
    for copy in copies:
        copy.wait()


VM = pl.BlockSpec(memory_space=pltpu.VMEM)
SM = pl.BlockSpec(memory_space=pltpu.SMEM)
ANY = pl.BlockSpec(memory_space=pl.ANY)
LIMIT = 56 * 1024 * 1024


SEMS = 81
LANES = 24
OUTS = (
    ((ROWS, KEYS), BF),
    ((ROWS, WIDTH), BF),
    ((4, 8, 16, KEYS), F32),
    ((40, 128), F32),
    ((8, 128), F32),
)


def fused(block_slot, tokens, gain, bias, key_weight, cotangent):
    outs = pl.pallas_call(
        fused_kernel,
        out_shape=tuple(pltpu.VMEM(*out) for out in OUTS),
        in_specs=[ANY] * 6,
        out_specs=(VM,) * 5,
        scratch_shapes=[
            pltpu.VMEM((4, 4, 4, 40, 16, 128), BF),
            pltpu.VMEM((2, 4, 4, 16, 128), BF),
            pltpu.VMEM((64, 16, 128), BF),
            pltpu.VMEM((4, 4, 4, 40, 16, 128), BF),
            pltpu.VMEM((4, 4, 4, 20, 16, 128), BF),
            pltpu.VMEM((64, 16, 128), BF),
            pltpu.VMEM((2, 2, 4, 4, 16, 128), BF),
            pltpu.VMEM((2, 4, 4, 2, 4, 16, 128), BF),
            pltpu.VMEM((2, 48, 128), F32),
            pltpu.VMEM((3, 4, 48, 128), F32),
            pltpu.VMEM((ROWS, WIDTH), BF),
            pltpu.VMEM((ROWS, WIDTH), BF),
            pltpu.VMEM((ROWS, KEYS), BF),
            pltpu.VMEM((ROWS, 128), F32),
            pltpu.VMEM((ROWS, 128), F32),
            pltpu.VMEM((48, 128), F32),
            pltpu.VMEM((ROWS, 256), F32),
            pltpu.VMEM((ROWS, 256), F32),
            pltpu.VMEM((ROWS, KEYS), F32),
            pltpu.SMEM((64,), jnp.int32),
            pltpu.SMEM((40,), jnp.int32),
            pltpu.VMEM((1, WIDTH), F32),
            pltpu.VMEM((1, KEYS), F32),
            pltpu.SemaphoreType.DMA((LANES,)),
            pltpu.SemaphoreType.DMA((SEMS,)),
            pltpu.SemaphoreType.DMA((11,)),
        ] + scatter_scratch(),
        compiler_params=pltpu.CompilerParams(collective_id=0, has_side_effects=True, vmem_limit_bytes=LIMIT),
        name="fused",
    )(block_slot, tokens, gain, bias, key_weight, cotangent)
    return pl.pallas_call(
        emit_kernel,
        out_shape=tuple(jax.ShapeDtypeStruct(*out) for out in OUTS),
        in_specs=[VM] * 5,
        out_specs=(ANY,) * 5,
        scratch_shapes=[pltpu.SemaphoreType.DMA((5,))],
        compiler_params=pltpu.CompilerParams(vmem_limit_bytes=1024 * 1024),
        name="emit",
    )(*(pltpu.with_memory_space_constraint(out, pltpu.VMEM) for out in outs))


def local(tokens, norm_gain, key_bias, key_weight, cotangent, block_slot):
    projected, token_grad, slab, gain, bias = fused(
        block_slot, tokens, norm_gain.reshape(1, WIDTH), key_bias.reshape(1, KEYS),
        key_weight.reshape(4, 8, 16, KEYS), cotangent)
    return (projected, token_grad, slab.reshape(512, KEYS), gain.reshape(-1), bias.reshape(-1))


def solution(mesh):
    return jax.shard_map(
        local,
        mesh=mesh,
        in_specs=(
            P(("shard", "rep"), None),
            P(),
            P(),
            P("shard", None),
            P(("shard", "rep"), None),
            P(),
        ),
        out_specs=(
            P(("shard", "rep"), None),
            P(("shard", "rep"), None),
            P("shard", None),
            P(),
            P(),
        ),
        check_vma=False,
    )
```

```python
import functools

import jax
import jax.numpy as jnp
from jax import lax
from jax.experimental import pallas as pl
from jax.experimental.pallas import tpu as pltpu
from jax.sharding import PartitionSpec as P

MESH = pl.DeviceIdType.MESH
BLK = 128
EPS = 1e-06
HALF = 20
PARTS = (
    (0, 7, 4, (0, 1, 2)),
    (7, 7, 3, (1, 2, 0)),
    (14, 6, 3, (2, 0, 1)),
)
BF = jnp.bfloat16
F32 = jnp.float32


class Place:
    def __init__(self):
        big = lax.axis_index("shard")
        rep = lax.axis_index("rep")
        self.big, self.rep = big, rep
        self.c = lax.rem(big, 2)
        self.s = lax.div(big, 2)
        self.z = lax.rem(self.s, 4)
        xh = lax.div(big, 8)
        xl = lax.div(rep, 4)
        self.xl = xl
        self.xh = xh
        self.pi = lax.rem(xl + xh, 2)
        self.x = xh * 2 + xl
        self.y = lax.rem(rep, 4)
        self.pos = (self.x, self.y, self.z)

    def at(self, axis, step):
        return lax.rem(self.pos[axis] + step, 4)

    def device(self, pos, c):
        x, y, z = pos
        big = (lax.div(x, 2) * 4 + z) * 2 + c
        return (big, lax.rem(x, 2) * 4 + y)

    def ring(self, axis, step):
        pos = list(self.pos)
        pos[axis] = self.at(axis, step)
        return self.device(pos, self.c)

    def partner(self):
        return (self.s * 2 + 1 - self.c, self.rep)

    def x_pair(self):
        return (self.big, (1 - self.xl) * 4 + self.y)

    def group(self):
        for i in range(2):
            for j in range(4):
                for d in range(2):
                    if i == j == d == 0:
                        continue
                    xh = self.xh if i == 0 else 1 - self.xh
                    xl = self.xl if i == 0 else 1 - self.xl
                    core = self.c if d == 0 else 1 - self.c
                    yield i, j, d, ((xh * 4 + self.at(2, j)) * 2 + core, xl * 4 + self.y)


class Wires:
    def __init__(self, send, recv, limit):
        self.send, self.recv, self.limit = send, recv, limit
        self.count, self.lanes = 0, []

    def lane(self, total):
        self.lanes.append((self.send.at[len(self.lanes)], total))
        return self.lanes[-1][0]

    def group(self, total, lane=None):
        i = self.count
        self.count += 1
        assert i < self.limit, "sems"
        return Group(self.lane(total) if lane is None else lane, self.recv.at[i], total)

    def put(self, src, dst, device, lane=None):
        return self.group(dst, lane).put(src, dst, device)

    def drain(self):
        for sem, total in self.lanes:
            pltpu.make_async_copy(total, total, sem).wait()


def thirds(wires, ref):
    blocks = pl.ds(0, HALF)
    return [
        wires.lane(ref.at[0, 0, pl.ds(0, 3), blocks]),
        wires.lane(ref.at[0, pl.ds(0, 3), :, blocks]),
        wires.lane(ref.at[pl.ds(0, 3), :, :, blocks]),
    ]


class Group:
    def __init__(self, send, recv, total):
        self.send, self.recv, self.total = send, recv, total

    def put(self, src, dst, device):
        pltpu.make_async_remote_copy(
            src_ref=src, dst_ref=dst, send_sem=self.send, recv_sem=self.recv,
            device_id=device, device_id_type=MESH,
        ).start()
        return self

    def wait(self):
        pltpu.make_async_copy(self.total, self.total, self.recv).wait()


def greet(place):
    barrier = pltpu.get_barrier_semaphore()
    peers = [device for _, _, _, device in place.group()]
    peers += [place.x_pair(), place.ring(0, 2)]
    peers += [place.ring(1, step) for step in (1, 2, 3)]
    for device in peers:
        pl.semaphore_signal(barrier, inc=1, device_id=device, device_id_type=MESH)
    return lambda: pl.semaphore_wait(barrier, len(peers))


def locate(place, order, k, v, done, later):
    out = [None] * 3
    for j, axis in enumerate(order):
        out[axis] = v if j == k else (done(axis) if j < k else later(axis))
    return tuple(out)


BATCHES = (
    ((0, 4, 2), (4, 3, 2)),
    ((0, 4, 2), (4, 3, 1)),
    ((0, 2, 1), (2, 4, 2)),
)


class Gather:
    def __init__(self, place, wires, w):
        self.place, self.wires, self.w = place, wires, w
        self.base = place.c * HALF
        self.stage = {}
        half = HALF // 2
        self.lanes = thirds(wires, w)
        across = wires.lane(w.at[:, :, :, pl.ds(0, HALF)])
        self.pair = [wires.group(w.at[:, :, :, pl.ds(0, half)], across) for _ in range(2)]

    def view(self, p, k, v, first, count):
        off, nb, h, order = PARTS[p]
        pos = self.place.pos
        idx = locate(self.place, order, k, v, lambda a: slice(None), lambda a: pos[a])
        return self.w.at[idx + (pl.ds(self.base + off + first, count),)]

    def move(self, group, p, k, v, first, count, device):
        ref = self.view(p, k, v, first, count)
        group = group or self.wires.group(ref, self.lanes[k])
        group.put(ref, ref, device)
        return group

    def span(self, p, k, batch):
        first, n, h = (0,) + PARTS[p][1:3] if k < 2 else BATCHES[p][batch]
        return first, h, n - h

    def start(self, p, k, batch=0, part=None):
        place, axis = self.place, PARTS[p][3][k]
        group = functools.partial(self.wires.group, lane=self.lanes[k])
        first, lo, hi = self.span(p, k, batch)
        mid = first + lo
        me = place.pos[axis]
        up, down = place.ring(axis, 1), place.ring(axis, 3)
        if k == 0:
            if p == 0:
                self.joint = group(self.w.at[0, 0, pl.ds(0, 3), pl.ds(0, HALF)])
            both = self.joint
            for device in (place.ring(axis, 2), up, down):
                self.move(both, p, k, me, 0, lo + hi, device)
            self.stage[p, k, 0] = both
            return
        if part != 1:
            u0 = self.move(None, p, k, me, first, lo, up)
            d1 = self.move(None, p, k, me, mid, hi, down)
            self.stage[p, k, batch] = [u0, d1]
        if part != 0:
            one = self.w.at[0, :, :, pl.ds(0, lo + hi)]
            two = self.w.at[0, pl.ds(0, 2), :, pl.ds(0, lo + hi)]
            late = group(one if k == 2 else two)
            self.move(late, p, k, me, mid, hi, up)
            self.move(late, p, k, me, first, lo, down)
            self.stage[p, k, batch] += [late, group(one) if k == 2 else late]

    def share(self, p, k, v, first, count, batch):
        if k == 2:
            self.move(self.pair[batch], p, k, v, first, count, self.place.partner())

    def forward(self, p, k, batch=0):
        place, axis = self.place, PARTS[p][3][k]
        first, lo, hi = self.span(p, k, batch)
        u0, d1, late, last = self.stage[p, k, batch]
        below, above = place.at(axis, 3), place.at(axis, 1)
        u0.wait()
        self.move(last, p, k, below, first, lo, place.ring(axis, 1))
        d1.wait()
        self.move(last, p, k, above, first + lo, hi, place.ring(axis, 3))
        self.share(p, k, below, first, lo, batch)
        self.share(p, k, above, first + lo, hi, batch)

    def arrive(self, p, k, batch=0):
        place, axis = self.place, PARTS[p][3][k]
        first, lo, hi = self.span(p, k, batch)
        self.stage[p, k, batch][2].wait()
        self.share(p, k, place.at(axis, 3), first + lo, hi, batch)
        self.share(p, k, place.at(axis, 1), first, lo, batch)

    def finish(self, p, k, batch=0):
        order = PARTS[p][3]
        place, axis = self.place, order[k]
        first, lo, hi = self.span(p, k, batch)
        if k == 0:
            if p == 0:
                self.joint.wait()
            return
        self.stage[p, k, batch][3].wait()
        self.share(p, k, place.at(axis, 2), first, lo + hi, batch)
        if k == 1:
            for i, (start, n, _) in enumerate(BATCHES[p]):
                self.share(p, 2, place.pos[order[2]], start, n, i)


def rest_of(t, count):
    if count == 2:
        return (lax.div(t, 4), lax.rem(t, 4))
    return (t,) if count == 1 else ()


class Scatter:
    def __init__(self, place, wires, g, bufs):
        self.place, self.wires, self.g, self.bufs = place, wires, g, bufs
        self.base = place.c * HALF
        self.stage = {}
        self.lanes = thirds(wires, g)[::-1]

    def index(self, p, k, v, later):
        order = PARTS[p][3]
        pos = self.place.pos
        return locate(self.place, order, k, v, lambda a: pos[a], later)

    def view(self, p, k, v, first, count):
        idx = self.index(p, k, v, lambda a: slice(None))
        return self.g.at[idx + (pl.ds(self.base + PARTS[p][0] + first, count),)]

    def tile(self, p, k, v, rest, first, count):
        order = PARTS[p][3]
        later = sorted(order[k + 1:])
        idx = self.index(p, k, v, lambda a: rest[later.index(a)])
        return idx + (pl.ds(self.base + PARTS[p][0] + first, count),)

    def buf(self, p, k, which):
        return self.bufs[p][k][which]

    def start(self, p, k, part=None):
        off, nb, h, order = PARTS[p]
        place, axis = self.place, order[k]
        full = (slice(None),) * (2 - k)
        put = functools.partial(self.wires.put, lane=self.lanes[k])
        up, down = place.ring(axis, 1), place.ring(axis, 3)
        over, under = place.at(axis, 1), place.at(axis, 3)
        across = place.at(axis, 2)
        ta, tb, fm, fp = self.bufs[p][k]
        if k == 2:
            if p == 0:
                self.joint = self.wires.group(self.g.at[0, 0, pl.ds(0, 3), pl.ds(0, HALF)], self.lanes[k])
            both = self.joint
            both.put(self.view(p, k, across, 0, nb), ta, place.ring(axis, 2))
            both.put(self.view(p, k, over, 0, nb), fm, up)
            both.put(self.view(p, k, under, 0, nb), fp, down)
            self.stage[p, k] = both
            return
        if part != 1:
            a = put(self.view(p, k, across, 0, h), ta, up)
            b = put(self.view(p, k, across, h, nb - h), tb, down)
            lead = (pl.ds(0, 2), slice(None), slice(None)) if k == 0 else (0, pl.ds(0, 2), slice(None))
            self.stage[p, k] = [a, b, self.wires.group(self.g.at[lead + (pl.ds(0, nb),)], self.lanes[k])]
        if part != 0:
            rest = self.stage[p, k][2]
            rest.put(self.view(p, k, over, h, nb - h), fm.at[full + (pl.ds(h, nb - h),)], up)
            rest.put(self.view(p, k, under, 0, h), fp.at[full + (pl.ds(0, h),)], down)

    def forward(self, p, k):
        off, nb, h, order = PARTS[p]
        place, axis = self.place, order[k]
        full = (slice(None),) * (2 - k)
        up, down = place.ring(axis, 1), place.ring(axis, 3)
        over, under = place.at(axis, 1), place.at(axis, 3)
        ta, tb, fm, fp = self.bufs[p][k]
        a, b, last = self.stage[p, k]
        g = self.g

        def add(t, v, buf, first, count):
            rest = rest_of(t, 2 - k)
            idx = self.tile(p, k, v, rest, first, count)
            g[idx] = g[idx] + buf[rest]

        a.wait()
        pl.loop(0, 4 ** (2 - k))(lambda t: add(t, over, ta, 0, h))
        last.put(self.view(p, k, over, 0, h), fm.at[full + (pl.ds(0, h),)], up)
        b.wait()
        pl.loop(0, 4 ** (2 - k))(lambda t: add(t, under, tb, h, nb - h))
        last.put(self.view(p, k, under, h, nb - h), fp.at[full + (pl.ds(h, nb - h),)], down)

    def finish(self, p, k):
        off, nb, h, order = PARTS[p]
        me = self.place.pos[order[k]]
        ta, tb, fm, fp = self.bufs[p][k]
        g = self.g
        if k == 2:
            if p == 0:
                self.joint.wait()
            idx = self.tile(p, k, me, (), 0, nb)
            total = (g[idx].astype(F32) + ta[...].astype(F32)) + (fm[...].astype(F32) + fp[...].astype(F32))
            g[idx] = total.astype(BF)
            return
        self.stage[p, k][2].wait()

        def add(t):
            rest = rest_of(t, 2 - k)
            idx = self.tile(p, k, me, rest, 0, nb)
            total = g[idx].astype(F32) + fm[rest].astype(F32) + fp[rest].astype(F32)
            g[idx] = total.astype(BF)

        pl.loop(0, 4 ** (2 - k))(add)


def scatter_scratch():
    out = []
    for p in range(3):
        _, nb, h, _ = PARTS[p]
        for k in range(3):
            lead = (4,) * (2 - k)
            sizes = (nb, 1, nb, nb) if k == 2 else (h, nb - h, nb, nb)
            out += [pltpu.VMEM(lead + (n, 16, 128), BF) for n in sizes]
    return out


def scatter_bufs(flat):
    return [[flat[(p * 3 + k) * 4:(p * 3 + k) * 4 + 4] for k in range(3)] for p in range(3)]


class Small:
    def __init__(self, place, wires, first, rest):
        self.place, self.wires, self.first, self.rest = place, wires, first, rest
        self.sent = []

    def start(self, k, value):
        place = self.place
        if k == 0:
            self.first[place.c] = value
            own = self.first.at[place.c]
            self.sent = self.wires.put(own, own, place.partner())
            return
        axis = 3 - k
        self.rest[k - 1, place.pos[axis]] = value
        own = self.rest.at[k - 1, place.pos[axis]]
        self.sent = self.wires.group(self.rest.at[0, pl.ds(0, 3)])
        for step in (2, 1, 3):
            self.sent.put(own, own, place.ring(axis, step))

    def finish(self, k):
        self.sent.wait()
        if k == 0:
            return self.first[0] + self.first[1]
        t = self.rest
        return (t[k - 1, 0] + t[k - 1, 1]) + (t[k - 1, 2] + t[k - 1, 3])


WIDTH = 5120
KEYS = 1024
ROWS = 384


def fused_kernel(slots_hbm, tok_ref, gain_hbm, bias_hbm, kw_ref, cot_ref,
                 proj, grad_out, slab_out, gain_out, bias_out,
                 w, kws, held, g, half, slot, seen, fin, first, rest,
                 tok, normed, cot, inv, coef, small_v, even, odd, keys, owner, slots_ref, gain_ref, bias_ref, send, recv, local, *flat):
    place = Place()
    wires = Wires(send, recv, SEMS)
    grad_scale = float(ROWS * 128) ** (-0.5)

    def load(src, dst, i):
        copy = pltpu.make_async_copy(src, dst, local.at[i])
        copy.start()
        return copy

    gains = load(gain_hbm, gain_ref, 8)
    wait_greet = greet(place)
    for i in range(2):
        xh = place.xh if i == 0 else 1 - place.xh
        xl = place.xl if i == 0 else 1 - place.xl
        for t in range(4):
            col = pl.ds(pl.multiple_of((xh * 4 + t) * 128, 128), 128)
            load(kw_ref.at[:, xl * 4 + place.y, :, col], kws.at[i, t], 0)
    rows = [load(tok_ref.at[pl.ds(i * 64, 64)], tok.at[pl.ds(i * 64, 64)], i + 1) for i in range(6)]
    cots = load(cot_ref, cot, 7)
    slot_list = load(slots_hbm, slots_ref, 9)
    biases = load(bias_hbm, bias_ref, 10)

    def norm(i):
        rows[i].wait()
        if i == 0:
            gains.wait()

        @pl.loop(i * 4, i * 4 + 4, unroll=2)
        def _(t):
            r = pl.ds(pl.multiple_of(t * 16, 16), 16)
            acc = [jnp.zeros((16, 128), F32)] * 4
            for j in range(40):
                v = tok[r, j * 128:(j + 1) * 128].astype(F32)
                acc[j % 4] = acc[j % 4] + v * v
            total = jnp.sum((acc[0] + acc[1]) + (acc[2] + acc[3]), axis=1, keepdims=True)
            scale = jnp.broadcast_to(lax.rsqrt(total * (1.0 / WIDTH) + EPS), (16, 128))
            inv[r, :] = scale
            for j in range(40):
                col = slice(j * 128, (j + 1) * 128)
                normed[r, col] = (tok[r, col].astype(F32) * scale * gain_ref[:, col]).astype(BF)

    own = place.c * HALF
    other = (1 - place.c) * HALF
    full = (slice(None),) * 3

    def blocks(side, first, count):
        b = side + first
        left = normed[:, pl.ds(pl.multiple_of(b * 128, 128), count * 128)]
        value = lax.dot_general(left, cot[...], (((0,), (0,)), ((), ())), preferred_element_type=F32)
        value = (value * grad_scale).astype(BF)
        for i in range(count):
            for r in range(8):
                for q in range(8):
                    g[q // 4 * 2 + r // 4, r % 4, q % 4, b + i] = value[
                        i * 128 + r * 16:i * 128 + r * 16 + 16, q * 128:(q + 1) * 128]

    def partial(p, mine):
        off, nb = PARTS[p][:2]
        side = own if mine else other
        for t in range(nb // 2):
            blocks(side, off + 2 * t, 2)
        if nb % 2:
            blocks(side, off + nb - 1, 1)

    def plane(p, step):
        axis = PARTS[p][3][0]
        at = [slice(None)] * 3
        at[axis] = place.at(axis, step)
        return axis, tuple(at)

    def swap(p, step, group=None):
        off, nb = PARTS[p][:2]
        _, at = plane(p, step)
        dst = half.at[at + (pl.ds(off, nb),)]
        group = group or wires.group(dst, swaps)
        group.put(g.at[at + (pl.ds(other + off, nb),)], dst, place.partner())
        return group

    def swap_rest(p):
        group = wires.group(half.at[pl.ds(0, 3), :, :, pl.ds(0, PARTS[p][1])], swaps)
        for step in (1, 3, 0):
            swap(p, step, group)
        return group

    def merge(p, *steps):
        off, nb = PARTS[p][:2]
        for step in steps:
            axis, at = plane(p, step)

            @pl.loop(0, 16, unroll=2)
            def _(t):
                rest = [lax.div(t, 4), lax.rem(t, 4)]
                rest.insert(axis, at[axis])
                here = tuple(rest) + (pl.ds(own + off, nb),)
                g[here] = g[here] + half[tuple(rest) + (pl.ds(off, nb),)]

    def merge_far(p):
        far[p].wait()
        merge(p, 2)

    def merge_near(p):
        near[p].wait()
        merge(p, 1, 3, 0)

    far, near = [], []
    swaps = wires.lane(half)
    gather = Gather(place, wires, w)
    scatter = Scatter(place, wires, g, scatter_bufs(flat))
    small = Small(place, wires, first, rest)
    come = wires.group(held.at[pl.ds(0, 60)])

    def trade_weights():
        pltpu.make_async_copy(kws, kws, local.at[0]).wait()
        mine = held.at[pl.ds(place.big * 4, 4)]
        for i, j, _, device in place.group():
            come.put(kws.at[i, place.at(2, j)], mine, device)
        held[pl.ds(place.big * 4, 4)] = kws[0, place.z]

    def pick():
        come.wait()
        slot_list.wait()

        @pl.loop(0, HALF)
        def _(t):
            b = own + t
            w[place.x, place.y, place.z, b] = held[slots_ref[b]]

    def bias_sum():
        biases.wait()
        for j in range(8):
            small_v[40 + j:41 + j, :] = jnp.sum(
                cot[:, j * 128:(j + 1) * 128].astype(F32), axis=0, keepdims=True) * grad_scale

    def early(batch):
        return [PARTS[p][0] + BATCHES[p][batch][0] + i for p in range(3) for i in range(BATCHES[p][batch][1])]

    def forward(batch, low, high):
        some = [side * HALF + b for side in range(2) for b in early(batch)]

        @pl.loop(low, high)
        def _(n):
            q = 2 * n
            x0, z0 = lax.div(q, 4) * 2, lax.rem(q, 4)
            left = jnp.concatenate([normed[:, b * 128:(b + 1) * 128] for b in some], axis=1)
            right = jnp.concatenate(
                [jnp.concatenate([w[x0 + r // 4, r % 4, z0, b], w[x0 + r // 4, r % 4, z0 + 1, b]], axis=1)
                 for b in some for r in range(8)], axis=0)
            value = jnp.dot(left, right, preferred_element_type=F32)
            col = pl.ds(pl.multiple_of(n * 256, 256), 256)
            if batch == 0:
                keys[:, col] = value
                return
            value = value + keys[:, col]
            proj[:, col] = (value + bias_ref[:, col]).astype(BF)
            both = value * cot[:, col].astype(F32)
            both = both[:, :128] + both[:, 128:]
            if low == 0:
                both = jnp.where(n == 0, 0.0, coef[...]) + both
            else:
                both = coef[...] + both
            coef[...] = both

        if batch == 1 and high == 4:
            coef[...] = jnp.broadcast_to(
                jnp.sum(coef[...], axis=1, keepdims=True), (ROWS, 128)) * inv[...] * inv[...] * (1.0 / WIDTH)

    def product(side, pair, into):
        right = jnp.concatenate(
            [jnp.concatenate([w[q // 4 * 2 + r // 4, r % 4, q % 4, side + b] for q in range(8)], axis=1)
             for b in pair for r in range(8)], axis=0)
        into[...] = lax.dot_general(cot[...], right, (((1,), (1,)), ((), ())), preferred_element_type=F32)

    def apply(side, pair, grad):
        for i, b in enumerate(pair):
            col = pl.ds(pl.multiple_of((side + b) * 128, 128), 128)
            gn = grad[:, i * 128:(i + 1) * 128] * inv[...]
            small_v[pl.ds(side + b, 1), :] = jnp.sum(
                gn * tok[:, col].astype(F32), axis=0, keepdims=True) * grad_scale
            grad_out[:, col] = (gn * gain_ref[:, col]).astype(BF)

    def backward(batch, side):
        some = early(batch)
        pairs = [some[i:i + 2] for i in range(0, len(some), 2)]
        product(side, pairs[0], even)
        for i, pair in enumerate(pairs):
            here, there = (even, odd) if i % 2 == 0 else (odd, even)
            if i + 1 < len(pairs):
                product(side, pairs[i + 1], there)
            apply(side, pair, here)

    def backward_early(mine):
        if not mine:
            gather.pair[0].wait()
        backward(0, own if mine else other)

    def backward_late(mine):
        if not mine:
            gather.pair[1].wait()
        backward(1, own if mine else other)

    def project_out(low, high):
        @pl.loop(low, high)
        def _(t):
            col = pl.ds(pl.multiple_of(t * 256, 256), 256)
            along = jnp.concatenate([coef[...], coef[...]], axis=1)
            grad_out[:, col] = (grad_out[:, col].astype(F32) - tok[:, col].astype(F32) * along).astype(BF)

    def each(step, k, *part):
        for p in range(3):
            step(p, k, *part)

    def small_next(k):
        small.start(k + 1, small.finish(k))

    def small_end():
        total = small.finish(3)
        gain_out[...] = total[:40]
        bias_out[...] = total[40:]

    back = wires.group(slot.at[pl.ds(0, 60)])

    def invert():
        @pl.loop(0, 64)
        def _(t):
            found = jnp.int32(-1)
            for b in range(40):
                found = jnp.where(slots_ref[b] == t, b, found)
            owner[t] = found

    def trade_grads():
        @pl.loop(0, 64, unroll=4)
        def _(t):
            b = owner[t]
            ours = jnp.logical_and(b >= own, b < own + HALF)
            value = g[place.x, place.y, place.z, jnp.maximum(b, 0)]
            slot[t] = jnp.where(ours, value, jnp.zeros_like(value))

        for _, _, _, device in place.group():
            back.put(slot.at[pl.ds(device[0] * 4, 4)], seen.at[place.c, place.xh, place.z], device)
        seen[place.c, place.xh, place.z] = slot[pl.ds(place.big * 4, 4)]

    pi, y = place.pi, place.y
    yup, ydown = place.ring(1, 1), place.ring(1, 3)
    below, above, across = place.at(1, 3), place.at(1, 1), place.at(1, 2)
    sent = {}
    last = wires.group(fin.at[0])

    def move(name, side, row, slot0, count, device):
        ref = fin.at[side, row, pl.ds(slot0, count)]
        if name in sent:
            sent[name].put(ref, ref, device)
        elif name:
            sent[name] = wires.put(ref, ref, device)
        else:
            last.put(ref, ref, device)

    def ring(name, side, slot0, late):
        move(name + "u", side, y, slot0, 1, yup)
        move(name + "d", side, y, slot0 + 1, 1, ydown)
        move(late, side, y, slot0 + 1, 1, yup)
        move(late, side, y, slot0, 1, ydown)

    def ring_on(name, side, slot0, late):
        sent[name + "u"].wait()
        move(late, side, below, slot0, 1, yup)
        sent[name + "d"].wait()
        move(late, side, above, slot0 + 1, 1, ydown)

    def spread_start():
        back.wait()
        for q in range(8):
            fin[pi, y, :, q // 4, q % 4] = seen[0, q // 4, q % 4] + seen[1, q // 4, q % 4]
        sent["c1"] = wires.group(fin.at[0, 0, pl.ds(0, 2)])
        sent["c2"] = wires.group(fin.at[0, 0, pl.ds(0, 2)])
        move("px", pi, y, 0, 2, place.x_pair())
        ring("c", pi, 2, "c1")
        ring("a", pi, 0, "")
        move("", pi, y, 2, 2, place.x_pair())

    def spread_on():
        ring_on("c", pi, 2, "c2")

    def spread_middle():
        sent["px"].wait()
        ring("b", 1 - pi, 0, "")
        sent["c1"].wait()
        move("", pi, below, 2, 2, place.x_pair())
        move("", pi, above, 2, 2, place.x_pair())
        ring_on("a", pi, 0, "")

    def spread_late():
        sent["c2"].wait()
        move("", pi, across, 2, 2, place.x_pair())
        ring_on("b", 1 - pi, 0, "")

    def spread_end():
        last.wait()

        @pl.loop(0, 32)
        def _(t):
            i, r = lax.div(t, 8), lax.rem(t, 8)
            for q in range(8):
                side = lax.rem(lax.div(r, 4) + q // 4, 2)
                slab_out[i, r, :, q * 128:(q + 1) * 128] = fin[side, lax.rem(r, 4), i, q // 4, q % 4].astype(F32)

    for i in range(3): norm(i)
    wait_greet()
    trade_weights()
    for i in range(3, 6): norm(i)
    cots.wait()
    partial(0, False)
    far.append(swap(0, 2))
    partial(1, False)
    far.append(swap(1, 2))
    partial(2, False)
    far.append(swap(2, 2))
    near.extend(swap_rest(p) for p in range(3))
    partial(0, True)
    pick()
    each(gather.start, 0)
    merge_far(0)
    scatter.start(0, 0, 0)
    partial(1, True)
    merge_far(1)
    scatter.start(1, 0, 0)
    partial(2, True)
    each(gather.finish, 0)
    each(gather.start, 1)
    merge_far(2)
    scatter.start(2, 0, 0)
    for p in range(3): merge_near(p); scatter.start(p, 0, 1)
    for p in (1, 2): gather.forward(p, 1)
    scatter.forward(0, 0)
    gather.forward(0, 1)
    scatter.forward(1, 0)
    bias_sum()
    invert()
    scatter.forward(2, 0)
    for p in (2, 0, 1): gather.finish(p, 1); gather.start(p, 2, 0, 0)
    for p in range(3): scatter.finish(p, 0); scatter.start(p, 1)
    each(gather.start, 2, 0, 1)
    each(scatter.forward, 1)
    each(gather.forward, 2, 0)
    each(gather.start, 2, 1, 0)
    each(scatter.finish, 1)
    each(scatter.start, 2)
    each(gather.start, 2, 1, 1)
    each(gather.arrive, 2, 0)
    each(gather.finish, 2, 0)
    backward_early(True)
    each(gather.forward, 2, 1)
    each(scatter.finish, 2)
    trade_grads()
    each(gather.arrive, 2, 1)
    backward_early(False)
    each(gather.finish, 2, 1)
    backward_late(True)
    spread_start()
    backward_late(False)
    small.start(0, small_v[...])
    forward(0, 0, 2)
    small_next(0)
    spread_on()
    forward(0, 2, 4)
    spread_middle()
    forward(1, 0, 2)
    small_next(1)
    spread_late()
    forward(1, 2, 4)
    small_next(2)
    project_out(0, 20)
    spread_end()
    small_end()
    wires.drain()


def emit_kernel(*refs):
    sem = refs[-1]
    copies = [pltpu.make_async_copy(refs[i], refs[5 + i], sem.at[i]) for i in range(5)]
    for copy in copies:
        copy.start()
    for copy in copies:
        copy.wait()


VM = pl.BlockSpec(memory_space=pltpu.VMEM)
SM = pl.BlockSpec(memory_space=pltpu.SMEM)
ANY = pl.BlockSpec(memory_space=pl.ANY)
LIMIT = 56 * 1024 * 1024


SEMS = 77
LANES = 24
OUTS = (
    ((ROWS, KEYS), BF),
    ((ROWS, WIDTH), BF),
    ((4, 8, 16, KEYS), F32),
    ((40, 128), F32),
    ((8, 128), F32),
)


def fused(block_slot, tokens, gain, bias, key_weight, cotangent):
    outs = pl.pallas_call(
        fused_kernel,
        out_shape=tuple(pltpu.VMEM(*out) for out in OUTS),
        in_specs=[ANY] * 6,
        out_specs=(VM,) * 5,
        scratch_shapes=[
            pltpu.VMEM((4, 4, 4, 40, 16, 128), BF),
            pltpu.VMEM((2, 4, 4, 16, 128), BF),
            pltpu.VMEM((64, 16, 128), BF),
            pltpu.VMEM((4, 4, 4, 40, 16, 128), BF),
            pltpu.VMEM((4, 4, 4, 20, 16, 128), BF),
            pltpu.VMEM((64, 16, 128), BF),
            pltpu.VMEM((2, 2, 4, 4, 16, 128), BF),
            pltpu.VMEM((2, 4, 4, 2, 4, 16, 128), BF),
            pltpu.VMEM((2, 48, 128), F32),
            pltpu.VMEM((3, 4, 48, 128), F32),
            pltpu.VMEM((ROWS, WIDTH), BF),
            pltpu.VMEM((ROWS, WIDTH), BF),
            pltpu.VMEM((ROWS, KEYS), BF),
            pltpu.VMEM((ROWS, 128), F32),
            pltpu.VMEM((ROWS, 128), F32),
            pltpu.VMEM((48, 128), F32),
            pltpu.VMEM((ROWS, 256), F32),
            pltpu.VMEM((ROWS, 256), F32),
            pltpu.VMEM((ROWS, KEYS), F32),
            pltpu.SMEM((64,), jnp.int32),
            pltpu.SMEM((40,), jnp.int32),
            pltpu.VMEM((1, WIDTH), F32),
            pltpu.VMEM((1, KEYS), F32),
            pltpu.SemaphoreType.DMA((LANES,)),
            pltpu.SemaphoreType.DMA((SEMS,)),
            pltpu.SemaphoreType.DMA((11,)),
        ] + scatter_scratch(),
        compiler_params=pltpu.CompilerParams(collective_id=0, has_side_effects=True, vmem_limit_bytes=LIMIT),
        name="fused",
    )(block_slot, tokens, gain, bias, key_weight, cotangent)
    return pl.pallas_call(
        emit_kernel,
        out_shape=tuple(jax.ShapeDtypeStruct(*out) for out in OUTS),
        in_specs=[VM] * 5,
        out_specs=(ANY,) * 5,
        scratch_shapes=[pltpu.SemaphoreType.DMA((5,))],
        compiler_params=pltpu.CompilerParams(vmem_limit_bytes=1024 * 1024),
        name="emit",
    )(*(pltpu.with_memory_space_constraint(out, pltpu.VMEM) for out in outs))


def local(tokens, norm_gain, key_bias, key_weight, cotangent, block_slot):
    projected, token_grad, slab, gain, bias = fused(
        block_slot, tokens, norm_gain.reshape(1, WIDTH), key_bias.reshape(1, KEYS),
        key_weight.reshape(4, 8, 16, KEYS), cotangent)
    return (projected, token_grad, slab.reshape(512, KEYS), gain.reshape(-1), bias.reshape(-1))


def solution(mesh):
    return jax.shard_map(
        local,
        mesh=mesh,
        in_specs=(
            P(("shard", "rep"), None),
            P(),
            P(),
            P("shard", None),
            P(("shard", "rep"), None),
            P(),
        ),
        out_specs=(
            P(("shard", "rep"), None),
            P(("shard", "rep"), None),
            P("shard", None),
            P(),
            P(),
        ),
        check_vma=False,
    )
```
